8 devices in a mesh: pz: 2 (over z, y), py: 2 (over x), px: 2 (over core).
Axes of the slice: x: 2, y: 2, z: 1, core: 2. Of those that a mesh axis runs over, the one named last changes fastest.
Arguments:
- shift_diag: float32 [2, 128, 128, 128], P(None, 'px', 'py', 'pz')
- rhs_field: float32 [2, 128, 128, 128], P(None, 'px', 'py', 'pz')
- x_start: float32 [2, 128, 128, 128], P(None, 'px', 'py', 'pz')
- cond_x: float32 [2, 128, 128, 128], P(None, 'px', 'py', 'pz')
- cond_y: float32 [2, 128, 128, 128], P(None, 'px', 'py', 'pz')
- cond_z: float32 [2, 128, 128, 128], P(None, 'px', 'py', 'pz')
Outputs:
- output 1: float32 [2, 128, 128, 128], P(None, 'px', 'py', 'pz')
- output 2: float32 [2, 21], replicated
All inputs are finite; a program needn't handle non-finite values.
Results may differ from the reference program's by a relative error of at most 0.001.
Values sent between devices are 32-bit elements.
A program may use at most 1 GiB of HBM per device.

```python
import jax
import jax.numpy as jnp
from jax import lax

GRID_X = 128
GRID_Y = 128
GRID_Z = 128
ITERS = 20


def setup_inputs(seed: int = 0) -> dict:
    base_key = jax.random.key(seed)
    sub_keys = jax.random.split(base_key, 6)
    field_shape = (2, GRID_X, GRID_Y, GRID_Z)
    shift_diag = 0.05 + 0.3 * jax.random.uniform(sub_keys[0], field_shape, jnp.float32)
    rhs_field = jax.random.normal(sub_keys[1], field_shape, jnp.float32)
    x_start = 0.5 * jax.random.normal(sub_keys[2], field_shape, jnp.float32)
    cond_x = 0.1 + 1.8 * jax.random.uniform(sub_keys[3], field_shape, jnp.float32)
    cond_y = 0.1 + 1.8 * jax.random.uniform(sub_keys[4], field_shape, jnp.float32)
    cond_z = 0.1 + 1.8 * jax.random.uniform(sub_keys[5], field_shape, jnp.float32)
    return {'shift_diag': shift_diag, 'rhs_field': rhs_field, 'x_start': x_start, 'cond_x': cond_x, 'cond_y': cond_y, 'cond_z': cond_z}


def face_term(field, conduct, axis_dim):
    planes = field.shape[axis_dim]
    face_flux = lax.slice_in_dim(conduct, 0, planes - 1, axis=axis_dim) * (lax.slice_in_dim(field, 0, planes - 1, axis=axis_dim) - lax.slice_in_dim(field, 1, planes, axis=axis_dim))
    widths = [(1, 1) if pos_dim == axis_dim else (0, 0) for pos_dim in range(field.ndim)]
    padded = jnp.pad(face_flux, widths)
    return lax.slice_in_dim(padded, 1, planes + 1, axis=axis_dim) - lax.slice_in_dim(padded, 0, planes, axis=axis_dim)


def apply_operator(field, shift_diag, cond_x, cond_y, cond_z):
    return shift_diag * field + face_term(field, cond_x, 0) + face_term(field, cond_y, 1) + face_term(field, cond_z, 2)


def solve_one(fields):
    shift_diag, rhs_field, x_start, cond_x, cond_y, cond_z = fields
    cell_count = GRID_X * GRID_Y * GRID_Z
    residual = rhs_field - apply_operator(x_start, shift_diag, cond_x, cond_y, cond_z)
    rho_start = jnp.sum(residual * residual)

    def cg_step(loop_state, unused):
        x_cur, res_cur, direction, rho_old, beta_coef = loop_state
        direction = res_cur + beta_coef * direction
        q_vec = apply_operator(direction, shift_diag, cond_x, cond_y, cond_z)
        alpha_step = rho_old / jnp.sum(direction * q_vec)
        x_cur = x_cur + alpha_step * direction
        res_cur = res_cur - alpha_step * q_vec
        rho_new = jnp.sum(res_cur * res_cur)
        return (x_cur, res_cur, direction, rho_new, rho_new / rho_old), jnp.sqrt(rho_new / cell_count)

    init_state = (x_start, residual, jnp.zeros_like(residual), rho_start, jnp.zeros_like(rho_start))
    final_state, res_tail = lax.scan(cg_step, init_state, None, length=ITERS)
    res_hist = jnp.concatenate([jnp.sqrt(rho_start / cell_count)[None], res_tail])
    return final_state[0], res_hist


def reference(shift_diag, rhs_field, x_start, cond_x, cond_y, cond_z):
    x_final, res_hist = lax.map(solve_one, (shift_diag, rhs_field, x_start, cond_x, cond_y, cond_z))
    return x_final, res_hist
```

```python
import jax
import jax.numpy as jnp
from jax import lax
from jax.experimental import pallas as pl
from jax.experimental.pallas import tpu as pltpu
from jax.sharding import PartitionSpec as P

ITERS = 20
F32 = jnp.float32
MESH = pl.DeviceIdType.MESH

NP = 32
NR = 64
LN = 128
PR = 80
KR = 72
SYS = NP * NR
PSYS = (NP + 1) * PR
KSYS = NP * KR


def roll(val, shift):
    if isinstance(shift, int):
        shift = shift % LN
    return pltpu.roll(val, shift, 1)


def kernel(s_hbm, b_hbm, x0_hbm, kx_hbm, ky_hbm, kz_hbm, x_out, hist_out,
           st_s, st_b, st_x, st_kx, st_ky, st_kz,
           R, Q, PB, KX, KXM, KY, KZ, D, KF,
           ix, iy, iz, jx, jy, jz, sxy, sxz, sky, skz, sy, sz,
           rhx, rhy, rhz, phx, phy, phz, qhx, qhy, qhz,
           red, rho_s, alpha_s, hist_s,
           ld_sem, isend, irecv, rsend, rrecv, qsend, qrecv, dsend, drecv):
    X = x_out
    pz, py, px = lax.axis_index('pz'), lax.axis_index('py'), lax.axis_index('px')
    nbr = {'x': (pz, py, 1 - px), 'y': (pz, 1 - py, px), 'z': (1 - pz, py, px)}
    others = {}
    for m in range(1, 8):
        others[m] = (1 - pz if m & 4 else pz, 1 - py if m & 2 else py, 1 - px if m & 1 else px)

    lane = lax.broadcasted_iota(jnp.int32, (8, LN), 1)
    row8 = lax.broadcasted_iota(jnp.int32, (8, LN), 0)

    def lanes(n):
        return lax.broadcasted_iota(jnp.int32, (n, LN), 1)

    zf = 63 * (1 - pz)
    xf = 31 * (1 - px)
    yf = 63 * (1 - py)
    hrow = 72 - 65 * py
    to_z = 127 - 126 * pz
    fro_z = 1 + 126 * pz

    def face_mask(n):
        return (lanes(n) % 64) == zf

    def splits(n):
        return lanes(n) < 64

    loads = []
    for num, (src, dst) in enumerate(((x0_hbm, st_x), (kz_hbm, st_kz), (kx_hbm, st_kx), (ky_hbm, st_ky), (s_hbm, st_s), (b_hbm, st_b))):
        pair = [pltpu.make_async_copy(src.at[c], dst.at[c], ld_sem.at[num, c]) for c in range(2)]
        for cp in pair:
            cp.start()
        loads.append(pair)

    barrier = pltpu.get_barrier_semaphore()
    for m in range(1, 8):
        pl.semaphore_signal(barrier, inc=1, device_id=others[m], device_id_type=MESH)

    def packed(st, c, x):
        return jnp.concatenate([st[c, x], st[c, x + NP]], axis=1)

    def pick(T, val, x, f):
        l64 = lanes(32) % 64
        T = jnp.where(l64 == x, roll(val[:32], (x - f + LN) % LN), T)
        return jnp.where(l64 == x + 32, roll(val[32:], (x + 32 - f + LN) % LN), T)

    def spread(G, x, f):
        return jnp.concatenate([roll(G, (f - x + LN) % LN), roll(G, (f - x - 32 + LN) % LN)], axis=0)

    zero32 = jnp.zeros((32, LN), F32)

    for c in range(2):
        loads[0][c].wait()

        def pack_x(x, T):
            u = packed(st_x, c, x)
            X[pl.ds(pl.multiple_of(c * SYS + x * NR, 8), NR)] = u
            base = pl.multiple_of(c * PSYS + x * PR, 8)
            PB[pl.ds(base, 8)] = jnp.zeros((8, LN), F32)
            PB[pl.ds(base + 72, 8)] = jnp.zeros((8, LN), F32)
            PB[pl.ds(base + 8, NR)] = u
            return pick(T, u, x, zf)
        sxz[c] = lax.fori_loop(0, NP, pack_x, zero32, unroll=4)
        sxy[c] = X[pl.ds(c * SYS + yf, 32, stride=NR)]
    for c in range(2):
        loads[1][c].wait()

        def pack_z(x, T):
            u = packed(st_kz, c, x)
            inner = jnp.where(lanes(NR) % 64 == 63, 0.0, u)
            KZ[pl.ds(pl.multiple_of(c * SYS + x * NR, 8), NR)] = jnp.where(pz == 1, roll(inner, 1), inner)
            return pick(T, u, x, 63)
        skz[c] = lax.fori_loop(0, NP, pack_z, zero32, unroll=4)
    for c in range(2):
        loads[2][c].wait()

        def pack_kx(x, carry):
            u = packed(st_kx, c, x)
            KX[pl.ds(pl.multiple_of(c * SYS + x * NR, 8), NR)] = u
            return carry
        lax.fori_loop(0, NP, pack_kx, 0, unroll=4)
        last = KX[pl.ds(c * SYS + 31 * NR, NR)]
        edge = jnp.logical_and(lanes(NR) >= 64, px == 1)
        KX[pl.ds(c * SYS + 31 * NR, NR)] = jnp.where(edge, 0.0, last)
    for c in range(2):
        loads[3][c].wait()

        def pack_ky(x, carry):
            u = packed(st_ky, c, x)
            rows = lax.broadcasted_iota(jnp.int32, (NR, LN), 0)
            u = jnp.where(jnp.logical_and(rows == NR - 1, py == 1), 0.0, u)
            KY[pl.ds(pl.multiple_of(c * KSYS + x * KR + 8, 8), NR)] = u
            return carry
        lax.fori_loop(0, NP, pack_ky, 0, unroll=4)
        sky[c] = KY[pl.ds(c * KSYS + 71, 32, stride=KR)]

    def remote(src, dst, send_sem, recv_sem, dev):
        return pltpu.make_async_remote_copy(src_ref=src, dst_ref=dst, send_sem=send_sem, recv_sem=recv_sem, device_id=dev, device_id_type=MESH)

    pl.semaphore_wait(barrier, 7)

    def x_plane(ref, c):
        return ref.at[pl.ds(pl.multiple_of(c * SYS + xf * NR, 8), NR)]

    first = []
    for c in range(2):
        first.append([
            remote(sxz.at[c], iz.at[c], isend.at[c, 0], irecv.at[c, 0], nbr['z']),
            remote(sxy.at[c], iy.at[c], isend.at[c, 1], irecv.at[c, 1], nbr['y']),
            remote(x_plane(X, c), ix.at[c], isend.at[c, 2], irecv.at[c, 2], nbr['x']),
            remote(skz.at[c], jz.at[c], isend.at[c, 3], irecv.at[c, 3], nbr['z']),
            remote(sky.at[c], jy.at[c], isend.at[c, 4], irecv.at[c, 4], nbr['y']),
            remote(KX.at[pl.ds(c * SYS + 31 * NR, NR)], jx.at[c], isend.at[c, 5], irecv.at[c, 5], nbr['x'])])
        for cp in first[c]:
            cp.start()

    def reduce_copies(kind, c):
        return [remote(red.at[kind, c, 0], red.at[kind, c, m], dsend.at[kind, c, m], drecv.at[kind, c, m], others[m]) for m in (7, 6, 5, 4, 3, 2, 1)]

    def reduce_start(kind, c, part):
        red[kind, c, 0] = jnp.sum(part, axis=0, keepdims=True)
        for cp in reduce_copies(kind, c):
            cp.start()

    def reduce_end(kind, c):
        for cp in reduce_copies(kind, c):
            cp.wait()
        v = [red[kind, c, m] for m in range(8)]
        total = ((v[0] + v[1]) + (v[2] + v[3])) + ((v[4] + v[5]) + (v[6] + v[7]))
        total = jnp.broadcast_to(total, (8, LN))
        return jnp.broadcast_to(jnp.sum(total, axis=1, keepdims=True), (8, LN))

    def fold(val):
        return jnp.sum(val.reshape(-1, 8, LN), axis=0)

    def wide(vec, n):
        return jnp.broadcast_to(vec[None], (n // 8, 8, LN)).reshape(n, LN)

    def r_copies(c):
        return [
            remote(sz.at[c], rhz.at[c], rsend.at[c, 0], rrecv.at[c, 0], nbr['z']),
            remote(sy.at[c], rhy.at[c], rsend.at[c, 1], rrecv.at[c, 1], nbr['y']),
            remote(x_plane(R, c), rhx.at[c], rsend.at[c, 2], rrecv.at[c, 2], nbr['x'])]

    for c in range(2):
        loads[4][c].wait()
        loads[5][c].wait()
        for cp in first[c]:
            cp.wait()
        lo = splits(NR)
        kx_last = KX[pl.ds(c * SYS + 31 * NR, NR)]
        KXM[c] = roll(jnp.where(lo, kx_last, jnp.where(px == 1, jx[c], 0.0)), 64)
        KY[pl.ds(c * KSYS + 7, 32, stride=KR)] = jnp.where(py == 1, jy[c], 0.0)
        KF[c] = jnp.where(pz == 1, jz[c], skz[c])
        PB[pl.ds(c * PSYS + hrow, 32, stride=PR)] = iy[c]
        u_first = PB[pl.ds(c * PSYS + 8, NR)]
        u_last = PB[pl.ds(c * PSYS + 31 * PR + 8, NR)]
        PB[pl.ds(c * PSYS + 32 * PR + 8, NR)] = roll(jnp.where(lo, ix[c], u_first), 64)
        low = roll(jnp.where(lo, u_last, ix[c]), 64)
        z_flux = KF[c] * (sxz[c] - iz[c])
        kf = KF[c]
        mask = face_mask(NR)

        def start_plane(x, carry):
            T, acc, fx_prev, kx_prev, u = carry
            base = pl.multiple_of(c * PSYS + x * PR, 8)
            at = pl.ds(pl.multiple_of(c * SYS + x * NR, 8), NR)
            kbase = pl.multiple_of(c * KSYS + x * KR, 8)
            nxt = PB[pl.ds(base + PR + 8, NR)]
            yu = PB[pl.ds(base + 9, NR)]
            yl = PB[pl.ds(base + 7, NR)]
            s = packed(st_s, c, x)
            kxv = KX[at]
            kyv = KY[pl.ds(kbase + 8, NR)]
            kyl = KY[pl.ds(kbase + 7, NR)]
            kzv = KZ[at]
            D[at] = s + (kxv + kx_prev) + (kyv + kyl) + (kzv + roll(kzv, fro_z) + jnp.where(mask, spread(kf, x, zf), 0.0))
            fx = kxv * (u - nxt)
            fz = kzv * (u - roll(u, to_z))
            au = s * u + (fx - fx_prev) + (kyv * (u - yu) - kyl * (yl - u)) + (fz - roll(fz, fro_z) + jnp.where(mask, spread(z_flux, x, zf), 0.0))
            r = packed(st_b, c, x) - au
            R[at] = r
            return pick(T, r, x, zf), acc + fold(r * r), fx, kxv, nxt
        T, acc, _, _, _ = lax.fori_loop(0, NP, start_plane, (zero32, jnp.zeros((8, LN), F32), KXM[c] * (low - u_first), KXM[c], u_first), unroll=2)
        reduce_start(0, c, acc)
        sz[c] = T
        sy[c] = R[pl.ds(c * SYS + yf, 32, stride=NR)]
        for cp in r_copies(c):
            cp.start()
        phx[c] = jnp.zeros((NR, LN), F32)
        phy[c] = zero32
        phz[c] = zero32
    hist_s[...] = jnp.zeros((8, LN), F32)
    for c in range(2):
        for cp in r_copies(c):
            cp.wait()

    def q_copies(c, par):
        return [
            remote(sz.at[c], qhz.at[par, c], qsend.at[c, 0], qrecv.at[par, c, 0], nbr['z']),
            remote(sy.at[c], qhy.at[par, c], qsend.at[c, 1], qrecv.at[par, c, 1], nbr['y']),
            remote(x_plane(Q, c), qhx.at[par, c], qsend.at[c, 2], qrecv.at[par, c, 2], nbr['x'])]

    def note(c, k, rho):
        hist_s[...] = jnp.where(jnp.logical_and(lane == k, row8 == c), rho, hist_s[...])

    def product(c, beta):
        b64, b32 = wide(beta, NR), wide(beta, 32)
        hx = rhx[c] + b64 * phx[c]
        hy = rhy[c] + b32 * phy[c]
        hz = rhz[c] + b32 * phz[c]
        phx[c] = hx
        phy[c] = hy
        phz[c] = hz
        PB[pl.ds(c * PSYS + hrow, 32, stride=PR)] = hy
        G = KF[c] * hz
        lo = splits(NR)
        mask = face_mask(NR)

        def direction(x):
            at = pl.ds(c * PSYS + x * PR + 8, NR)
            val = R[pl.ds(c * SYS + x * NR, NR)] + b64 * PB[at]
            PB[at] = val
            return val

        p_first = direction(0)
        p_last = direction(NP - 1)
        above = roll(jnp.where(lo, hx, p_first), 64)
        below = roll(jnp.where(lo, p_last, hx), 64)
        cur, kxp_prev = p_first, KXM[c] * below
        acc, T = jnp.zeros((8, LN), F32), zero32
        for x in range(NP):
            if x + 1 < NP - 1:
                nxt = direction(x + 1)
            elif x + 1 == NP - 1:
                nxt = PB[pl.ds(c * PSYS + (NP - 1) * PR + 8, NR)]
            else:
                nxt = above
            base = c * PSYS + x * PR
            at = pl.ds(c * SYS + x * NR, NR)
            kbase = c * KSYS + x * KR
            kxv, kzv = KX[at], KZ[at]
            kxp = kxv * cur
            zu = jnp.where(mask, spread(G, x, zf), kzv * roll(cur, to_z))
            zl = roll(kzv * cur, fro_z)
            q = D[at] * cur - kxp_prev - kxv * nxt
            q = q - KY[pl.ds(kbase + 8, NR)] * PB[pl.ds(base + 9, NR)]
            q = q - KY[pl.ds(kbase + 7, NR)] * PB[pl.ds(base + 7, NR)]
            q = q - zu - zl
            Q[at] = q
            acc = acc + fold(cur * q)
            T = pick(T, q, x, zf)
            cur, kxp_prev = nxt, kxp
        return acc, T

    CH = 256

    def body(k, carry):
        par = k % 2
        for c in range(2):
            rho = reduce_end(0, c)
            note(c, k, rho)
            beta = jnp.where(k == 0, 0.0, rho / rho_s[c])
            rho_s[c] = rho
            acc, T = product(c, beta)
            reduce_start(1, c, acc)
            sz[c] = T
            sy[c] = Q[pl.ds(c * SYS + yf, 32, stride=NR)]
            for cp in q_copies(c, par):
                cp.start()
        for c in range(2):
            alpha = rho_s[c] / reduce_end(1, c)
            a_ch = wide(alpha, CH)

            def step_r(i, acc):
                at = pl.ds(pl.multiple_of(c * SYS + i * CH, 8), CH)
                r = R[at] - a_ch * Q[at]
                R[at] = r
                return acc + fold(r * r)
            acc = lax.fori_loop(0, SYS // CH, step_r, jnp.zeros((8, LN), F32))
            reduce_start(0, c, acc)

            def step_x(x, carry):
                at = pl.ds(pl.multiple_of(c * SYS + x * NR, 8), NR)
                X[at] = X[at] + wide(alpha, NR) * PB[pl.ds(pl.multiple_of(c * PSYS + x * PR + 8, 8), NR)]
                return carry
            lax.fori_loop(0, NP, step_x, 0, unroll=4)
            for cp in q_copies(c, par):
                cp.wait()
            rhx[c] = rhx[c] - wide(alpha, NR) * qhx[par, c]
            rhy[c] = rhy[c] - wide(alpha, 32) * qhy[par, c]
            rhz[c] = rhz[c] - wide(alpha, 32) * qhz[par, c]
        return carry

    lax.fori_loop(0, ITERS, body, 0)
    for c in range(2):
        note(c, ITERS, reduce_end(0, c))
    hist_out[...] = jnp.sqrt(hist_s[...] * (1.0 / (128 * 128 * 128)))


def run(s, b, x0, kx, ky, kz):
    v = lambda *shape: pltpu.VMEM(shape, F32)
    sem = lambda *shape: pltpu.SemaphoreType.DMA(shape)
    scratch = [v(2, 64, 64, 64)] * 6
    scratch += [v(2 * SYS, LN), v(2 * SYS, LN), v(2 * PSYS, LN), v(2 * SYS, LN), v(2, NR, LN), v(2 * KSYS, LN), v(2 * SYS, LN), v(2 * SYS, LN), v(2, 32, LN)]
    scratch += [v(2, NR, LN), v(2, 32, LN), v(2, 32, LN)] * 2
    scratch += [v(2, 32, LN)] * 6
    scratch += [v(2, NR, LN), v(2, 32, LN), v(2, 32, LN)] * 2
    scratch += [v(2, 2, NR, LN), v(2, 2, 32, LN), v(2, 2, 32, LN)]
    scratch += [v(2, 2, 8, 1, LN), v(2, 8, LN), v(2, 8, LN), v(8, LN)]
    scratch += [sem(6, 2), sem(2, 6), sem(2, 6), sem(2, 3), sem(2, 3), sem(2, 3), sem(2, 2, 3), sem(2, 2, 8), sem(2, 2, 8)]
    xp, hist = pl.pallas_call(
        kernel,
        out_shape=(jax.ShapeDtypeStruct((2 * SYS, LN), F32), jax.ShapeDtypeStruct((8, LN), F32)),
        in_specs=[pl.BlockSpec(memory_space=pl.ANY)] * 6,
        out_specs=(pl.BlockSpec(memory_space=pltpu.VMEM), pl.BlockSpec(memory_space=pltpu.VMEM)),
        scratch_shapes=scratch,
        compiler_params=pltpu.CompilerParams(collective_id=0, has_side_effects=True, vmem_limit_bytes=60 * 1024 * 1024),
        name='cg',
    )(s, b, x0, kx, ky, kz)
    xp = xp.reshape(2, NP, NR, LN)
    x = jnp.concatenate([xp[..., :64], xp[..., 64:]], axis=1)
    return x, hist[:2, :ITERS + 1]


def solution(mesh):
    field = P(None, 'px', 'py', 'pz')
    return jax.shard_map(run, mesh=mesh, in_specs=(field,) * 6, out_specs=(field, P(None, None)), check_vma=False)
```

```python
import jax
import jax.numpy as jnp
from jax import lax
from jax.experimental import pallas as pl
from jax.experimental.pallas import tpu as pltpu
from jax.sharding import PartitionSpec as P

ITERS = 20
F32 = jnp.float32
MESH = pl.DeviceIdType.MESH

NP = 32
NR = 64
LN = 128
PR = 80
KR = 72
SYS = NP * NR
PSYS = (NP + 1) * PR
KSYS = NP * KR
AHEAD = 3


def roll(val, shift):
    if isinstance(shift, int):
        shift = shift % LN
    return pltpu.roll(val, shift, 1)


def kernel(s_hbm, b_hbm, x0_hbm, kx_hbm, ky_hbm, kz_hbm, x_out, hist_out,
           st_s, st_b, st_x, st_kx, st_ky, st_kz,
           R, Q, PB, KX, KXM, KY, KZ, KZB, D, KF,
           ix, iy, iz, jx, jy, jz, sxy, sxz, sky, skz, sy, sz,
           rhx, rhy, rhz, phx, phy, phz, qhx, qhy, qhz,
           red, rho_s, alpha_s, hist_s,
           ld_sem, isend, irecv, rsend, rrecv, qsend, qrecv, dsend, drecv):
    X = x_out
    pz, py, px = lax.axis_index('pz'), lax.axis_index('py'), lax.axis_index('px')
    nbr = {'x': (pz, py, 1 - px), 'y': (pz, 1 - py, px), 'z': (1 - pz, py, px)}
    others = {}
    for m in range(1, 8):
        others[m] = (1 - pz if m & 4 else pz, 1 - py if m & 2 else py, 1 - px if m & 1 else px)

    lane = lax.broadcasted_iota(jnp.int32, (8, LN), 1)
    row8 = lax.broadcasted_iota(jnp.int32, (8, LN), 0)

    def lanes(n):
        return lax.broadcasted_iota(jnp.int32, (n, LN), 1)

    zf = 63 * (1 - pz)
    xf = 31 * (1 - px)
    yf = 63 * (1 - py)
    hrow = 72 - 65 * py
    to_z = 127 - 126 * pz
    fro_z = 1 + 126 * pz

    def face_mask(n):
        return (lanes(n) % 64) == zf

    def splits(n):
        return lanes(n) < 64

    loads = []
    for num, (src, dst) in enumerate(((x0_hbm, st_x), (kz_hbm, st_kz), (kx_hbm, st_kx), (ky_hbm, st_ky), (s_hbm, st_s), (b_hbm, st_b))):
        pair = [pltpu.make_async_copy(src.at[c], dst.at[c], ld_sem.at[num, c]) for c in range(2)]
        for cp in pair:
            cp.start()
        loads.append(pair)

    barrier = pltpu.get_barrier_semaphore()
    for m in range(1, 8):
        pl.semaphore_signal(barrier, inc=1, device_id=others[m], device_id_type=MESH)

    def packed(st, c, x):
        return jnp.concatenate([st[c, x], st[c, x + NP]], axis=1)

    def pick(T, val, x, f):
        l64 = lanes(32) % 64
        T = jnp.where(l64 == x, roll(val[:32], (x - f + LN) % LN), T)
        return jnp.where(l64 == x + 32, roll(val[32:], (x + 32 - f + LN) % LN), T)

    def spread(G, x, f):
        return jnp.concatenate([roll(G, (f - x + LN) % LN), roll(G, (f - x - 32 + LN) % LN)], axis=0)

    zero32 = jnp.zeros((32, LN), F32)

    for c in range(2):
        loads[0][c].wait()

        def pack_x(x, T):
            u = packed(st_x, c, x)
            X[pl.ds(pl.multiple_of(c * SYS + x * NR, 8), NR)] = u
            base = pl.multiple_of(c * PSYS + x * PR, 8)
            PB[pl.ds(base, 8)] = jnp.zeros((8, LN), F32)
            PB[pl.ds(base + 72, 8)] = jnp.zeros((8, LN), F32)
            PB[pl.ds(base + 8, NR)] = u
            return pick(T, u, x, zf)
        sxz[c] = lax.fori_loop(0, NP, pack_x, zero32, unroll=4)
        sxy[c] = X[pl.ds(c * SYS + yf, 32, stride=NR)]
    for c in range(2):
        loads[1][c].wait()

        def pack_z(x, T):
            u = packed(st_kz, c, x)
            inner = jnp.where(lanes(NR) % 64 == 63, 0.0, u)
            moved = roll(inner, 1)
            at = pl.ds(pl.multiple_of(c * SYS + x * NR, 8), NR)
            KZ[at] = jnp.where(pz == 1, moved, inner)
            KZB[at] = jnp.where(pz == 1, inner, moved)
            return pick(T, u, x, 63)
        skz[c] = lax.fori_loop(0, NP, pack_z, zero32, unroll=4)
    for c in range(2):
        loads[2][c].wait()

        def pack_kx(x, carry):
            u = packed(st_kx, c, x)
            KX[pl.ds(pl.multiple_of(c * SYS + x * NR, 8), NR)] = u
            return carry
        lax.fori_loop(0, NP, pack_kx, 0, unroll=4)
        last = KX[pl.ds(c * SYS + 31 * NR, NR)]
        edge = jnp.logical_and(lanes(NR) >= 64, px == 1)
        KX[pl.ds(c * SYS + 31 * NR, NR)] = jnp.where(edge, 0.0, last)
    for c in range(2):
        loads[3][c].wait()

        def pack_ky(x, carry):
            u = packed(st_ky, c, x)
            rows = lax.broadcasted_iota(jnp.int32, (NR, LN), 0)
            u = jnp.where(jnp.logical_and(rows == NR - 1, py == 1), 0.0, u)
            KY[pl.ds(pl.multiple_of(c * KSYS + x * KR + 8, 8), NR)] = u
            return carry
        lax.fori_loop(0, NP, pack_ky, 0, unroll=4)
        sky[c] = KY[pl.ds(c * KSYS + 71, 32, stride=KR)]

    def remote(src, dst, send_sem, recv_sem, dev):
        return pltpu.make_async_remote_copy(src_ref=src, dst_ref=dst, send_sem=send_sem, recv_sem=recv_sem, device_id=dev, device_id_type=MESH)

    pl.semaphore_wait(barrier, 7)

    def x_plane(ref, c):
        return ref.at[pl.ds(pl.multiple_of(c * SYS + xf * NR, 8), NR)]

    first = []
    for c in range(2):
        first.append([
            remote(sxz.at[c], iz.at[c], isend.at[c, 0], irecv.at[c, 0], nbr['z']),
            remote(sxy.at[c], iy.at[c], isend.at[c, 1], irecv.at[c, 1], nbr['y']),
            remote(x_plane(X, c), ix.at[c], isend.at[c, 2], irecv.at[c, 2], nbr['x']),
            remote(skz.at[c], jz.at[c], isend.at[c, 3], irecv.at[c, 3], nbr['z']),
            remote(sky.at[c], jy.at[c], isend.at[c, 4], irecv.at[c, 4], nbr['y']),
            remote(KX.at[pl.ds(c * SYS + 31 * NR, NR)], jx.at[c], isend.at[c, 5], irecv.at[c, 5], nbr['x'])])
        for cp in first[c]:
            cp.start()

    def reduce_copies(kind, c):
        return [remote(red.at[kind, c, 0], red.at[kind, c, m], dsend.at[kind, c, m], drecv.at[kind, c, m], others[m]) for m in (7, 6, 5, 4, 3, 2, 1)]

    def reduce_start(kind, c, part):
        red[kind, c, 0] = jnp.sum(part, axis=0, keepdims=True)
        for cp in reduce_copies(kind, c):
            cp.start()

    def reduce_end(kind, c):
        for cp in reduce_copies(kind, c):
            cp.wait_recv()
        v = [red[kind, c, m] for m in range(8)]
        total = ((v[0] + v[1]) + (v[2] + v[3])) + ((v[4] + v[5]) + (v[6] + v[7]))
        total = jnp.broadcast_to(total, (8, LN))
        return jnp.broadcast_to(jnp.sum(total, axis=1, keepdims=True), (8, LN))

    def reduce_sent(kind, c):
        for cp in reduce_copies(kind, c):
            cp.wait_send()

    def fold(val):
        return jnp.sum(val.reshape(-1, 8, LN), axis=0)

    def wide(vec, n):
        return jnp.broadcast_to(vec[None], (n // 8, 8, LN)).reshape(n, LN)

    def r_copies(c):
        return [
            remote(sz.at[c], rhz.at[c], rsend.at[c, 0], rrecv.at[c, 0], nbr['z']),
            remote(sy.at[c], rhy.at[c], rsend.at[c, 1], rrecv.at[c, 1], nbr['y']),
            remote(x_plane(R, c), rhx.at[c], rsend.at[c, 2], rrecv.at[c, 2], nbr['x'])]

    for c in range(2):
        loads[4][c].wait()
        loads[5][c].wait()
        for cp in first[c]:
            cp.wait()
        lo = splits(NR)
        kx_last = KX[pl.ds(c * SYS + 31 * NR, NR)]
        KXM[c] = roll(jnp.where(lo, kx_last, jnp.where(px == 1, jx[c], 0.0)), 64)
        KY[pl.ds(c * KSYS + 7, 32, stride=KR)] = jnp.where(py == 1, jy[c], 0.0)
        KF[c] = jnp.where(pz == 1, jz[c], skz[c])
        PB[pl.ds(c * PSYS + hrow, 32, stride=PR)] = iy[c]
        u_first = PB[pl.ds(c * PSYS + 8, NR)]
        u_last = PB[pl.ds(c * PSYS + 31 * PR + 8, NR)]
        PB[pl.ds(c * PSYS + 32 * PR + 8, NR)] = roll(jnp.where(lo, ix[c], u_first), 64)
        low = roll(jnp.where(lo, u_last, ix[c]), 64)
        z_flux = KF[c] * (sxz[c] - iz[c])
        kf = KF[c]
        mask = face_mask(NR)

        def start_plane(x, carry):
            T, acc, fx_prev, kx_prev, u = carry
            base = pl.multiple_of(c * PSYS + x * PR, 8)
            at = pl.ds(pl.multiple_of(c * SYS + x * NR, 8), NR)
            kbase = pl.multiple_of(c * KSYS + x * KR, 8)
            nxt = PB[pl.ds(base + PR + 8, NR)]
            yu = PB[pl.ds(base + 9, NR)]
            yl = PB[pl.ds(base + 7, NR)]
            s = packed(st_s, c, x)
            kxv = KX[at]
            kyv = KY[pl.ds(kbase + 8, NR)]
            kyl = KY[pl.ds(kbase + 7, NR)]
            kzv = KZ[at]
            D[at] = s + (kxv + kx_prev) + (kyv + kyl) + (kzv + KZB[at] + jnp.where(mask, spread(kf, x, zf), 0.0))
            fx = kxv * (u - nxt)
            fz = kzv * (u - roll(u, to_z))
            au = s * u + (fx - fx_prev) + (kyv * (u - yu) - kyl * (yl - u)) + (fz - roll(fz, fro_z) + jnp.where(mask, spread(z_flux, x, zf), 0.0))
            r = packed(st_b, c, x) - au
            R[at] = r
            return pick(T, r, x, zf), acc + fold(r * r), fx, kxv, nxt
        T, acc, _, _, _ = lax.fori_loop(0, NP, start_plane, (zero32, jnp.zeros((8, LN), F32), KXM[c] * (low - u_first), KXM[c], u_first), unroll=2)
        reduce_start(0, c, acc)
        sz[c] = T
        sy[c] = R[pl.ds(c * SYS + yf, 32, stride=NR)]
        for cp in r_copies(c):
            cp.start()
        phx[c] = jnp.zeros((NR, LN), F32)
        phy[c] = zero32
        phz[c] = zero32
    hist_s[...] = jnp.zeros((8, LN), F32)
    for c in range(2):
        for cp in r_copies(c):
            cp.wait()

    def q_copies(c, par):
        return [
            remote(sz.at[c], qhz.at[par, c], qsend.at[c, 0], qrecv.at[par, c, 0], nbr['z']),
            remote(sy.at[c], qhy.at[par, c], qsend.at[c, 1], qrecv.at[par, c, 1], nbr['y']),
            remote(x_plane(Q, c), qhx.at[par, c], qsend.at[c, 2], qrecv.at[par, c, 2], nbr['x'])]

    def note(c, k, rho):
        hist_s[...] = jnp.where(jnp.logical_and(lane == k, row8 == c), rho, hist_s[...])

    def product(c, beta):
        b64, b32 = wide(beta, NR), wide(beta, 32)
        hx = rhx[c] + b64 * phx[c]
        hy = rhy[c] + b32 * phy[c]
        hz = rhz[c] + b32 * phz[c]
        phx[c] = hx
        phy[c] = hy
        phz[c] = hz
        PB[pl.ds(c * PSYS + hrow, 32, stride=PR)] = hy
        G = KF[c] * hz
        lo = splits(NR)
        mask = face_mask(NR)

        def direction(x):
            at = pl.ds(c * PSYS + x * PR + 8, NR)
            val = R[pl.ds(c * SYS + x * NR, NR)] + b64 * PB[at]
            PB[at] = val
            return val

        def turn(x, p):
            at = pl.ds(c * SYS + x * NR, NR)
            return roll(KZB[at] * p, to_z), roll(KZ[at] * p, fro_z), spread(G, x, zf)

        def load_p(x):
            return PB[pl.ds(c * PSYS + x * PR + 8, NR)]

        p_last = direction(NP - 1)
        p_first = direction(0)
        above = roll(jnp.where(lo, hx, p_first), 64)
        below = roll(jnp.where(lo, p_last, hx), 64)
        turned = {0: turn(0, p_first)}
        for x in range(1, AHEAD):
            turned[x] = turn(x, direction(x))
        cur, kxp_prev = p_first, KXM[c] * below
        acc = jnp.zeros((8, LN), F32)
        for x in range(NP):
            w = x + AHEAD
            if w < NP:
                turned[w] = turn(w, direction(w) if w < NP - 1 else load_p(w))
            nxt = load_p(x + 1) if x + 1 < NP else above
            base = c * PSYS + x * PR
            at = pl.ds(c * SYS + x * NR, NR)
            kbase = c * KSYS + x * KR
            kxv = KX[at]
            kxp = kxv * cur
            q = D[at] * cur - kxp_prev - kxv * nxt
            q = q - KY[pl.ds(kbase + 8, NR)] * PB[pl.ds(base + 9, NR)]
            q = q - KY[pl.ds(kbase + 7, NR)] * PB[pl.ds(base + 7, NR)]
            zu, zl, e = turned.pop(x)
            q = q - (jnp.where(mask, e, zu) + zl)
            Q[at] = q
            acc = acc + fold(cur * q)
            cur, kxp_prev = nxt, kxp
        return acc

    CH = 256

    def body(k, carry):
        par = k % 2
        for c in range(2):
            rho = reduce_end(0, c)
            note(c, k, rho)
            beta = jnp.where(k == 0, 0.0, rho / rho_s[c])
            rho_s[c] = rho
            reduce_start(1, c, product(c, beta))
        for c in range(2):
            reduce_sent(0, c)

            def z_face(x, T):
                return pick(T, Q[pl.ds(pl.multiple_of(c * SYS + x * NR, 8), NR)], x, zf)
            sz[c] = lax.fori_loop(0, NP, z_face, zero32, unroll=8)
            sy[c] = Q[pl.ds(c * SYS + yf, 32, stride=NR)]
            for cp in q_copies(c, par):
                cp.start()
        for c in range(2):
            alpha = rho_s[c] / reduce_end(1, c)
            alpha_s[c] = alpha
            a_ch = wide(alpha, CH)

            def step_r(i, acc):
                at = pl.ds(pl.multiple_of(c * SYS + i * CH, 8), CH)
                r = R[at] - a_ch * Q[at]
                R[at] = r
                return acc + fold(r * r)
            acc = lax.fori_loop(0, SYS // CH, step_r, jnp.zeros((8, LN), F32))
            reduce_start(0, c, acc)

            def step_x(x, carry):
                at = pl.ds(pl.multiple_of(c * SYS + x * NR, 8), NR)
                X[at] = X[at] + wide(alpha, NR) * PB[pl.ds(pl.multiple_of(c * PSYS + x * PR + 8, 8), NR)]
                return carry
            lax.fori_loop(0, NP, step_x, 0, unroll=4)
        for c in range(2):
            reduce_sent(1, c)
            for cp in q_copies(c, par):
                cp.wait()
            alpha = alpha_s[c]
            rhx[c] = rhx[c] - wide(alpha, NR) * qhx[par, c]
            rhy[c] = rhy[c] - wide(alpha, 32) * qhy[par, c]
            rhz[c] = rhz[c] - wide(alpha, 32) * qhz[par, c]
        return carry

    lax.fori_loop(0, ITERS, body, 0)
    for c in range(2):
        note(c, ITERS, reduce_end(0, c))
        reduce_sent(0, c)
    hist_out[...] = jnp.sqrt(hist_s[...] * (1.0 / (128 * 128 * 128)))


def run(s, b, x0, kx, ky, kz):
    v = lambda *shape: pltpu.VMEM(shape, F32)
    sem = lambda *shape: pltpu.SemaphoreType.DMA(shape)
    scratch = [v(2, 64, 64, 64)] * 6
    scratch += [v(2 * SYS, LN), v(2 * SYS, LN), v(2 * PSYS, LN), v(2 * SYS, LN), v(2, NR, LN), v(2 * KSYS, LN), v(2 * SYS, LN), v(2 * SYS, LN), v(2 * SYS, LN), v(2, 32, LN)]
    scratch += [v(2, NR, LN), v(2, 32, LN), v(2, 32, LN)] * 2
    scratch += [v(2, 32, LN)] * 6
    scratch += [v(2, NR, LN), v(2, 32, LN), v(2, 32, LN)] * 2
    scratch += [v(2, 2, NR, LN), v(2, 2, 32, LN), v(2, 2, 32, LN)]
    scratch += [v(2, 2, 8, 1, LN), v(2, 8, LN), v(2, 8, LN), v(8, LN)]
    scratch += [sem(6, 2), sem(2, 6), sem(2, 6), sem(2, 3), sem(2, 3), sem(2, 3), sem(2, 2, 3), sem(2, 2, 8), sem(2, 2, 8)]
    xp, hist = pl.pallas_call(
        kernel,
        out_shape=(jax.ShapeDtypeStruct((2 * SYS, LN), F32), jax.ShapeDtypeStruct((8, LN), F32)),
        in_specs=[pl.BlockSpec(memory_space=pl.ANY)] * 6,
        out_specs=(pl.BlockSpec(memory_space=pltpu.VMEM), pl.BlockSpec(memory_space=pltpu.VMEM)),
        scratch_shapes=scratch,
        compiler_params=pltpu.CompilerParams(collective_id=0, has_side_effects=True, vmem_limit_bytes=60 * 1024 * 1024),
        name='cg',
    )(s, b, x0, kx, ky, kz)
    xp = xp.reshape(2, NP, NR, LN)
    x = jnp.concatenate([xp[..., :64], xp[..., 64:]], axis=1)
    return x, hist[:2, :ITERS + 1]


def solution(mesh):
    field = P(None, 'px', 'py', 'pz')
    return jax.shard_map(run, mesh=mesh, in_specs=(field,) * 6, out_specs=(field, P(None, None)), check_vma=False)
```

```python
import jax
import jax.numpy as jnp
from jax import lax
from jax.experimental import pallas as pl
from jax.experimental.pallas import tpu as pltpu
from jax.sharding import PartitionSpec as P

ITERS = 20
F32 = jnp.float32
MESH = pl.DeviceIdType.MESH

NP = 32
NR = 64
LN = 128
PR = 80
KR = 72
SYS = NP * NR
PSYS = (NP + 1) * PR
KSYS = NP * KR
AHEAD = 3


def roll(val, shift):
    if isinstance(shift, int):
        shift = shift % LN
    return pltpu.roll(val, shift, 1)


def kernel(s_hbm, b_hbm, x0_hbm, kx_hbm, ky_hbm, kz_hbm, x_out, hist_out,
           st_s, st_b, st_x, st_kx, st_ky, st_kz,
           R, Q, PB, KX, KXM, KY, KZ, KZB, D, KF,
           ix, iy, iz, jx, jy, jz, sxy, sxz, sky, skz, sy, sz,
           rhx, rhy, rhz, phx, phy, phz, qhx, qhy, qhz,
           red, rho_s, alpha_s, hist_s,
           ld_sem, isend, irecv, rsend, rrecv, qsend, qrecv, dsend, drecv):
    X = x_out
    pz, py, px = lax.axis_index('pz'), lax.axis_index('py'), lax.axis_index('px')
    nbr = {'x': (pz, py, 1 - px), 'y': (pz, 1 - py, px), 'z': (1 - pz, py, px)}
    others = {}
    for m in range(1, 8):
        others[m] = (1 - pz if m & 4 else pz, 1 - py if m & 2 else py, 1 - px if m & 1 else px)

    lane = lax.broadcasted_iota(jnp.int32, (8, LN), 1)
    row8 = lax.broadcasted_iota(jnp.int32, (8, LN), 0)

    def lanes(n):
        return lax.broadcasted_iota(jnp.int32, (n, LN), 1)

    zf = 63 * (1 - pz)
    xf = 31 * (1 - px)
    yf = 63 * (1 - py)
    hrow = 72 - 65 * py
    to_z = 127 - 126 * pz
    fro_z = 1 + 126 * pz
    zturn = 63 + 65 * pz

    def face_mask(n):
        return (lanes(n) % 64) == zf

    def splits(n):
        return lanes(n) < 64

    loads = []
    for num, (src, dst) in enumerate(((x0_hbm, st_x), (kz_hbm, st_kz), (kx_hbm, st_kx), (ky_hbm, st_ky), (s_hbm, st_s), (b_hbm, st_b))):
        pair = [pltpu.make_async_copy(src.at[c], dst.at[c], ld_sem.at[num, c]) for c in range(2)]
        loads.append(pair)
    for num in range(2):
        for cp in loads[num]:
            cp.start()

    barrier = pltpu.get_barrier_semaphore()
    for m in range(1, 8):
        pl.semaphore_signal(barrier, inc=1, device_id=others[m], device_id_type=MESH)

    def packed(st, c, x):
        return jnp.concatenate([st[c, x], st[c, x + NP]], axis=1)

    def pick(T, val, x, f):
        l64 = lanes(32) % 64
        T = jnp.where(l64 == x, roll(val[:32], lax.rem(x - f + LN, LN)), T)
        return jnp.where(l64 == x + 32, roll(val[32:], lax.rem(x + 32 - f + LN, LN)), T)

    def spread(G, x, f):
        return jnp.concatenate([roll(G, lax.rem(f - x + LN, LN)), roll(G, lax.rem(f - x - 32 + LN, LN))], axis=0)

    zero32 = jnp.zeros((32, LN), F32)

    for c in range(2):
        loads[0][c].wait()
        for num in ((2,), (3, 4, 5))[c]:
            for cp in loads[num]:
                cp.start()

        def pack_x(x, T):
            u = packed(st_x, c, x)
            X[pl.ds(pl.multiple_of(c * SYS + x * NR, 8), NR)] = u
            base = pl.multiple_of(c * PSYS + x * PR, 8)
            PB[pl.ds(base, 8)] = jnp.zeros((8, LN), F32)
            PB[pl.ds(base + 72, 8)] = jnp.zeros((8, LN), F32)
            PB[pl.ds(base + 8, NR)] = u
            return pick(T, u, x, zf)
        sxz[c] = lax.fori_loop(0, NP, pack_x, zero32, unroll=8)
        sxy[c] = X[pl.ds(c * SYS + yf, 32, stride=NR)]
    for c in range(2):
        loads[1][c].wait()

        def pack_z(x, T):
            u = packed(st_kz, c, x)
            inner = jnp.where(lanes(NR) % 64 == 63, 0.0, u)
            moved = roll(inner, 1)
            at = pl.ds(pl.multiple_of(c * SYS + x * NR, 8), NR)
            KZ[at] = jnp.where(pz == 1, moved, inner)
            KZB[at] = jnp.where(pz == 1, inner, moved)
            return pick(T, u, x, 63)
        skz[c] = lax.fori_loop(0, NP, pack_z, zero32, unroll=8)
    for c in range(2):
        loads[2][c].wait()

        def pack_kx(x, carry):
            u = packed(st_kx, c, x)
            KX[pl.ds(pl.multiple_of(c * SYS + x * NR, 8), NR)] = u
            return carry
        lax.fori_loop(0, NP, pack_kx, 0, unroll=8)
        last = KX[pl.ds(c * SYS + 31 * NR, NR)]
        edge = jnp.logical_and(lanes(NR) >= 64, px == 1)
        KX[pl.ds(c * SYS + 31 * NR, NR)] = jnp.where(edge, 0.0, last)
    for c in range(2):
        loads[3][c].wait()

        def pack_ky(x, carry):
            u = packed(st_ky, c, x)
            rows = lax.broadcasted_iota(jnp.int32, (NR, LN), 0)
            u = jnp.where(jnp.logical_and(rows == NR - 1, py == 1), 0.0, u)
            KY[pl.ds(pl.multiple_of(c * KSYS + x * KR + 8, 8), NR)] = u
            return carry
        lax.fori_loop(0, NP, pack_ky, 0, unroll=8)
        sky[c] = KY[pl.ds(c * KSYS + 71, 32, stride=KR)]

    def remote(src, dst, send_sem, recv_sem, dev):
        return pltpu.make_async_remote_copy(src_ref=src, dst_ref=dst, send_sem=send_sem, recv_sem=recv_sem, device_id=dev, device_id_type=MESH)

    pl.semaphore_wait(barrier, 7)

    def x_plane(ref, c):
        return ref.at[pl.ds(pl.multiple_of(c * SYS + xf * NR, 8), NR)]

    first = []
    for c in range(2):
        first.append([
            remote(sxz.at[c], iz.at[c], isend.at[c, 0], irecv.at[c, 0], nbr['z']),
            remote(sxy.at[c], iy.at[c], isend.at[c, 1], irecv.at[c, 1], nbr['y']),
            remote(x_plane(X, c), ix.at[c], isend.at[c, 2], irecv.at[c, 2], nbr['x']),
            remote(skz.at[c], jz.at[c], isend.at[c, 3], irecv.at[c, 3], nbr['z']),
            remote(sky.at[c], jy.at[c], isend.at[c, 4], irecv.at[c, 4], nbr['y']),
            remote(KX.at[pl.ds(c * SYS + 31 * NR, NR)], jx.at[c], isend.at[c, 5], irecv.at[c, 5], nbr['x'])])
        for cp in first[c]:
            cp.start()

    def reduce_copies(kind, c):
        return [remote(red.at[kind, c, 0], red.at[kind, c, m], dsend.at[kind, c, m], drecv.at[kind, c, m], others[m]) for m in (7, 6, 5, 4, 3, 2, 1)]

    def reduce_start(kind, c, part):
        red[kind, c, 0] = jnp.sum(part, axis=0, keepdims=True)
        for cp in reduce_copies(kind, c):
            cp.start()

    def reduce_end(kind, c):
        for cp in reduce_copies(kind, c):
            cp.wait_recv()
        v = [red[kind, c, m] for m in range(8)]
        total = ((v[0] + v[1]) + (v[2] + v[3])) + ((v[4] + v[5]) + (v[6] + v[7]))
        total = jnp.broadcast_to(total, (8, LN))
        return jnp.broadcast_to(jnp.sum(total, axis=1, keepdims=True), (8, LN))

    def reduce_sent(kind, c):
        for cp in reduce_copies(kind, c):
            cp.wait_send()

    def fold(val):
        return jnp.sum(val.reshape(-1, 8, LN), axis=0)

    def wide(vec, n):
        return jnp.broadcast_to(vec[None], (n // 8, 8, LN)).reshape(n, LN)

    def r_copies(c):
        return [
            remote(sz.at[c], rhz.at[c], rsend.at[c, 0], rrecv.at[c, 0], nbr['z']),
            remote(sy.at[c], rhy.at[c], rsend.at[c, 1], rrecv.at[c, 1], nbr['y']),
            remote(x_plane(R, c), rhx.at[c], rsend.at[c, 2], rrecv.at[c, 2], nbr['x'])]

    for c in range(2):
        loads[4][c].wait()
        loads[5][c].wait()
        for cp in first[c]:
            cp.wait()
        lo = splits(NR)
        kx_last = KX[pl.ds(c * SYS + 31 * NR, NR)]
        KXM[c] = roll(jnp.where(lo, kx_last, jnp.where(px == 1, jx[c], 0.0)), 64)
        KY[pl.ds(c * KSYS + 7, 32, stride=KR)] = jnp.where(py == 1, jy[c], 0.0)
        KF[c] = jnp.where(pz == 1, jz[c], skz[c])
        PB[pl.ds(c * PSYS + hrow, 32, stride=PR)] = iy[c]
        u_first = PB[pl.ds(c * PSYS + 8, NR)]
        u_last = PB[pl.ds(c * PSYS + 31 * PR + 8, NR)]
        PB[pl.ds(c * PSYS + 32 * PR + 8, NR)] = roll(jnp.where(lo, ix[c], u_first), 64)
        low = roll(jnp.where(lo, u_last, ix[c]), 64)
        z_flux = KF[c] * (sxz[c] - iz[c])
        kf = KF[c]
        mask = face_mask(NR)

        def start_plane(x, carry):
            T, acc, fx_prev, kx_prev, u = carry
            base = pl.multiple_of(c * PSYS + x * PR, 8)
            at = pl.ds(pl.multiple_of(c * SYS + x * NR, 8), NR)
            kbase = pl.multiple_of(c * KSYS + x * KR, 8)
            nxt = PB[pl.ds(base + PR + 8, NR)]
            yu = PB[pl.ds(base + 9, NR)]
            yl = PB[pl.ds(base + 7, NR)]
            s = packed(st_s, c, x)
            kxv = KX[at]
            kyv = KY[pl.ds(kbase + 8, NR)]
            kyl = KY[pl.ds(kbase + 7, NR)]
            kzv = KZ[at]
            D[at] = s + (kxv + kx_prev) + (kyv + kyl) + (kzv + KZB[at] + jnp.where(mask, spread(kf, x, zf), 0.0))
            fx = kxv * (u - nxt)
            fz = kzv * (u - roll(u, to_z))
            au = s * u + (fx - fx_prev) + (kyv * (u - yu) - kyl * (yl - u)) + (fz - roll(fz, fro_z) + jnp.where(mask, spread(z_flux, x, zf), 0.0))
            r = packed(st_b, c, x) - au
            R[at] = r
            return pick(T, r, x, zf), acc + fold(r * r), fx, kxv, nxt
        T, acc, _, _, _ = lax.fori_loop(0, NP, start_plane, (zero32, jnp.zeros((8, LN), F32), KXM[c] * (low - u_first), KXM[c], u_first), unroll=4)
        reduce_start(0, c, acc)
        sz[c] = T
        sy[c] = R[pl.ds(c * SYS + yf, 32, stride=NR)]
        for cp in r_copies(c):
            cp.start()
        phx[c] = jnp.zeros((NR, LN), F32)
        phy[c] = zero32
        phz[c] = zero32
    hist_s[...] = jnp.zeros((8, LN), F32)
    for c in range(2):
        for cp in r_copies(c):
            cp.wait()

    def q_copies(c, par):
        return [
            remote(sz.at[c], qhz.at[par, c], qsend.at[c, 0], qrecv.at[par, c, 0], nbr['z']),
            remote(sy.at[c], qhy.at[par, c], qsend.at[c, 1], qrecv.at[par, c, 1], nbr['y']),
            remote(x_plane(Q, c), qhx.at[par, c], qsend.at[c, 2], qrecv.at[par, c, 2], nbr['x'])]

    def note(c, k, rho):
        hist_s[...] = jnp.where(jnp.logical_and(lane == k, row8 == c), rho, hist_s[...])

    def product(c, beta):
        b64, b32 = wide(beta, NR), wide(beta, 32)
        hx = rhx[c] + b64 * phx[c]
        hy = rhy[c] + b32 * phy[c]
        hz = rhz[c] + b32 * phz[c]
        phx[c] = hx
        phy[c] = hy
        phz[c] = hz
        PB[pl.ds(c * PSYS + hrow, 32, stride=PR)] = hy
        G = KF[c] * hz
        lo = splits(NR)
        mask = face_mask(NR)

        def direction(x):
            at = pl.ds(c * PSYS + x * PR + 8, NR)
            val = R[pl.ds(c * SYS + x * NR, NR)] + b64 * PB[at]
            PB[at] = val
            return val

        def turn(x, p):
            at = pl.ds(c * SYS + x * NR, NR)
            e = jnp.concatenate([roll(G, zf if x == 0 else zturn - x), roll(G, zturn - x - 32)], axis=0)
            return roll(KZB[at] * p, to_z), roll(KZ[at] * p, fro_z), e

        def load_p(x):
            return PB[pl.ds(c * PSYS + x * PR + 8, NR)]

        p_last = direction(NP - 1)
        p_first = direction(0)
        above = roll(jnp.where(lo, hx, p_first), 64)
        below = roll(jnp.where(lo, p_last, hx), 64)
        turned = {0: turn(0, p_first)}
        for x in range(1, AHEAD):
            turned[x] = turn(x, direction(x))
        cur, kxp_prev = p_first, KXM[c] * below
        acc = jnp.zeros((8, LN), F32)
        for x in range(NP):
            w = x + AHEAD
            if w < NP:
                turned[w] = turn(w, direction(w) if w < NP - 1 else load_p(w))
            nxt = load_p(x + 1) if x + 1 < NP else above
            base = c * PSYS + x * PR
            at = pl.ds(c * SYS + x * NR, NR)
            kbase = c * KSYS + x * KR
            kxv = KX[at]
            kxp = kxv * cur
            q = D[at] * cur - kxp_prev - kxv * nxt
            q = q - KY[pl.ds(kbase + 8, NR)] * PB[pl.ds(base + 9, NR)]
            q = q - KY[pl.ds(kbase + 7, NR)] * PB[pl.ds(base + 7, NR)]
            zu, zl, e = turned.pop(x)
            q = q - (jnp.where(mask, e, zu) + zl)
            Q[at] = q
            acc = acc + fold(cur * q)
            cur, kxp_prev = nxt, kxp
        return acc

    CH = 256

    def body(k, carry):
        par = k % 2
        for c in range(2):
            rho = reduce_end(0, c)
            note(c, k, rho)
            beta = jnp.where(k == 0, 0.0, rho / rho_s[c])
            rho_s[c] = rho
            reduce_start(1, c, product(c, beta))
        for c in range(2):
            reduce_sent(0, c)

            def z_face(x, T):
                return pick(T, Q[pl.ds(pl.multiple_of(c * SYS + x * NR, 8), NR)], x, zf)
            sz[c] = lax.fori_loop(0, NP, z_face, zero32, unroll=8)
            sy[c] = Q[pl.ds(c * SYS + yf, 32, stride=NR)]
            for cp in q_copies(c, par):
                cp.start()
        for c in range(2):
            alpha = rho_s[c] / reduce_end(1, c)
            alpha_s[c] = alpha
            a_ch = wide(alpha, CH)

            def step_r(i, acc):
                at = pl.ds(pl.multiple_of(c * SYS + i * CH, 8), CH)
                r = R[at] - a_ch * Q[at]
                R[at] = r
                return acc + fold(r * r)
            acc = lax.fori_loop(0, SYS // CH, step_r, jnp.zeros((8, LN), F32))
            reduce_start(0, c, acc)

            def step_x(x, carry):
                at = pl.ds(pl.multiple_of(c * SYS + x * NR, 8), NR)
                X[at] = X[at] + wide(alpha, NR) * PB[pl.ds(pl.multiple_of(c * PSYS + x * PR + 8, 8), NR)]
                return carry
            lax.fori_loop(0, NP, step_x, 0, unroll=4)
        for c in range(2):
            reduce_sent(1, c)
            for cp in q_copies(c, par):
                cp.wait()
            alpha = alpha_s[c]
            rhx[c] = rhx[c] - wide(alpha, NR) * qhx[par, c]
            rhy[c] = rhy[c] - wide(alpha, 32) * qhy[par, c]
            rhz[c] = rhz[c] - wide(alpha, 32) * qhz[par, c]
        return carry

    lax.fori_loop(0, ITERS, body, 0)
    for c in range(2):
        note(c, ITERS, reduce_end(0, c))
        reduce_sent(0, c)
    hist_out[...] = jnp.sqrt(hist_s[...] * (1.0 / (128 * 128 * 128)))


CHUNKS = 2
VMEM_MAIN = 60 * 1024 * 1024


def unpack(xp, hist, x_out, hist_out, buf, st, in_sem, out_sem):
    planes = NP // CHUNKS
    loads = []
    for n in range(2 * CHUNKS):
        at = pl.ds(n * planes * NR, planes * NR)
        loads.append(pltpu.make_async_copy(xp.at[at], buf.at[at], in_sem.at[n]))
        loads[n].start()
    hist_out[...] = hist[:2, :ITERS + 1]
    stores = []
    for n in range(2 * CHUNKS):
        c, x0 = n // CHUNKS, n % CHUNKS * planes
        loads[n].wait()

        def plane(x, carry):
            val = buf[pl.ds(pl.multiple_of(n * planes * NR + x * NR, 8), NR)]
            st[c, x0 + x] = val[:, :64]
            st[c, x0 + x + NP] = roll(val, 64)[:, :64]
            return carry
        lax.fori_loop(0, planes, plane, 0, unroll=8)
        for h in range(2):
            at = pl.ds(x0 + NP * h, planes)
            stores.append(pltpu.make_async_copy(st.at[c, at], x_out.at[c, at], out_sem.at[n, h]))
            stores[-1].start()
    for cp in stores:
        cp.wait()


def run(s, b, x0, kx, ky, kz):
    v = lambda *shape: pltpu.VMEM(shape, F32)
    sem = lambda *shape: pltpu.SemaphoreType.DMA(shape)
    scratch = [v(2, 64, 64, 64)] * 6
    scratch += [v(2 * SYS, LN), v(2 * SYS, LN), v(2 * PSYS, LN), v(2 * SYS, LN), v(2, NR, LN), v(2 * KSYS, LN), v(2 * SYS, LN), v(2 * SYS, LN), v(2 * SYS, LN), v(2, 32, LN)]
    scratch += [v(2, NR, LN), v(2, 32, LN), v(2, 32, LN)] * 2
    scratch += [v(2, 32, LN)] * 6
    scratch += [v(2, NR, LN), v(2, 32, LN), v(2, 32, LN)] * 2
    scratch += [v(2, 2, NR, LN), v(2, 2, 32, LN), v(2, 2, 32, LN)]
    scratch += [v(2, 2, 8, 1, LN), v(2, 8, LN), v(2, 8, LN), v(8, LN)]
    scratch += [sem(6, 2), sem(2, 6), sem(2, 6), sem(2, 3), sem(2, 3), sem(2, 3), sem(2, 2, 3), sem(2, 2, 8), sem(2, 2, 8)]
    xp, hist = pl.pallas_call(
        kernel,
        out_shape=(jax.ShapeDtypeStruct((2 * SYS, LN), F32), jax.ShapeDtypeStruct((8, LN), F32)),
        in_specs=[pl.BlockSpec(memory_space=pl.ANY)] * 6,
        out_specs=(pl.BlockSpec(memory_space=pltpu.VMEM), pl.BlockSpec(memory_space=pltpu.VMEM)),
        scratch_shapes=scratch,
        compiler_params=pltpu.CompilerParams(collective_id=0, has_side_effects=True, vmem_limit_bytes=VMEM_MAIN),
        name='cg',
    )(s, b, x0, kx, ky, kz)
    return pl.pallas_call(
        unpack,
        out_shape=(jax.ShapeDtypeStruct((2, 64, 64, 64), F32), jax.ShapeDtypeStruct((2, ITERS + 1), F32)),
        in_specs=[pl.BlockSpec(memory_space=pl.ANY), pl.BlockSpec(memory_space=pltpu.VMEM)],
        out_specs=(pl.BlockSpec(memory_space=pl.ANY), pl.BlockSpec(memory_space=pltpu.VMEM)),
        scratch_shapes=[v(2 * SYS, LN), v(2, 64, 64, 64), sem(2 * CHUNKS), sem(2 * CHUNKS, 2)],
        compiler_params=pltpu.CompilerParams(vmem_limit_bytes=60 * 1024 * 1024),
        name='unpack',
    )(xp, hist)


def solution(mesh):
    field = P(None, 'px', 'py', 'pz')
    return jax.shard_map(run, mesh=mesh, in_specs=(field,) * 6, out_specs=(field, P(None, None)), check_vma=False)
```

```python
import jax
import jax.numpy as jnp
from jax import lax
from jax.experimental import pallas as pl
from jax.experimental.pallas import tpu as pltpu
from jax.sharding import PartitionSpec as P

ITERS = 20
F32 = jnp.float32
MESH = pl.DeviceIdType.MESH

NP = 32
NR = 64
LN = 128
PR = 80
KR = 72
SYS = NP * NR
PSYS = (NP + 1) * PR
KSYS = NP * KR
AHEAD = 3


def roll(val, shift):
    if isinstance(shift, int):
        shift = shift % LN
    return pltpu.roll(val, shift, 1)


def kernel(s_hbm, b_hbm, x0_hbm, kx_hbm, ky_hbm, kz_hbm, x_out, hist_out,
           st_s, st_b, st_x, st_kx, st_ky, st_kz,
           X, R, Q, PB, PZ, RZ, KX, KXM, KY, KZ, KZF, D, KF,
           ix, iy, iz, jx, jy, jz, sxy, sxz, sky, skz, sy, sz,
           rhx, rhy, rhz, phx, phy, qhx, qhy, qhz,
           red, rho_s, alpha_s, hist_s,
           ld_sem, isend, irecv, rsend, rrecv, qsend, qrecv, dsend, drecv, out_sem):
    pz, py, px = lax.axis_index('pz'), lax.axis_index('py'), lax.axis_index('px')
    nbr = {'x': (pz, py, 1 - px), 'y': (pz, 1 - py, px), 'z': (1 - pz, py, px)}
    others = {}
    for m in range(1, 8):
        others[m] = (1 - pz if m & 4 else pz, 1 - py if m & 2 else py, 1 - px if m & 1 else px)

    lane = lax.broadcasted_iota(jnp.int32, (8, LN), 1)
    row8 = lax.broadcasted_iota(jnp.int32, (8, LN), 0)

    def lanes(n):
        return lax.broadcasted_iota(jnp.int32, (n, LN), 1)

    zf = 63 * (1 - pz)
    xf = 31 * (1 - px)
    yf = 63 * (1 - py)
    hrow = 72 - 65 * py
    to_z = 127 - 126 * pz
    fro_z = 1 + 126 * pz

    def face_mask(n):
        return (lanes(n) % 64) == zf

    def splits(n):
        return lanes(n) < 64

    loads = []
    for num, (src, dst) in enumerate(((x0_hbm, st_x), (kz_hbm, st_kz), (kx_hbm, st_kx), (ky_hbm, st_ky), (s_hbm, st_s), (b_hbm, st_b))):
        pair = [pltpu.make_async_copy(src.at[c], dst.at[c], ld_sem.at[num, c]) for c in range(2)]
        loads.append(pair)
    for num in range(1):
        for cp in loads[num]:
            cp.start()

    barrier = pltpu.get_barrier_semaphore()
    for m in range(1, 8):
        pl.semaphore_signal(barrier, inc=1, device_id=others[m], device_id_type=MESH)

    def packed(st, c, x):
        return jnp.concatenate([st[c, x], st[c, x + NP]], axis=1)

    def pick(T, val, x, f):
        l64 = lanes(32) % 64
        T = jnp.where(l64 == x, roll(val[:32], lax.rem(x - f + LN, LN)), T)
        return jnp.where(l64 == x + 32, roll(val[32:], lax.rem(x + 32 - f + LN, LN)), T)

    def spread(G, x, f):
        return jnp.concatenate([roll(G, lax.rem(f - x + LN, LN)), roll(G, lax.rem(f - x - 32 + LN, LN))], axis=0)

    zero32 = jnp.zeros((32, LN), F32)

    def remote(src, dst, send_sem, recv_sem, dev):
        return pltpu.make_async_remote_copy(src_ref=src, dst_ref=dst, send_sem=send_sem, recv_sem=recv_sem, device_id=dev, device_id_type=MESH)

    def x_plane(ref, c):
        return ref.at[pl.ds(pl.multiple_of(c * SYS + xf * NR, 8), NR)]

    def rows(x, c):
        return pl.ds(pl.multiple_of(c * SYS + x * NR, 8), NR)

    first = []
    for c in range(2):
        first.append([
            remote(sxz.at[c], iz.at[c], isend.at[c, 0], irecv.at[c, 0], nbr['z']),
            remote(sxy.at[c], iy.at[c], isend.at[c, 1], irecv.at[c, 1], nbr['y']),
            remote(x_plane(X, c), ix.at[c], isend.at[c, 2], irecv.at[c, 2], nbr['x']),
            remote(skz.at[c], jz.at[c], isend.at[c, 3], irecv.at[c, 3], nbr['z']),
            remote(sky.at[c], jy.at[c], isend.at[c, 4], irecv.at[c, 4], nbr['y']),
            remote(KX.at[pl.ds(c * SYS + 31 * NR, NR)], jx.at[c], isend.at[c, 5], irecv.at[c, 5], nbr['x'])])

    for c in range(2):
        loads[0][c].wait()
        for num in ((1, 2), (3, 4, 5))[c]:
            for cp in loads[num]:
                cp.start()

        def pack_x(x, T):
            u = packed(st_x, c, x)
            X[rows(x, c)] = u
            base = pl.multiple_of(c * PSYS + x * PR, 8)
            PB[pl.ds(base, 8)] = jnp.zeros((8, LN), F32)
            PB[pl.ds(base + 72, 8)] = jnp.zeros((8, LN), F32)
            PB[pl.ds(base + 8, NR)] = u
            return pick(T, u, x, zf)
        sxz[c] = lax.fori_loop(0, NP, pack_x, zero32, unroll=8)
        sxy[c] = X[pl.ds(c * SYS + yf, 32, stride=NR)]
    pl.semaphore_wait(barrier, 7)
    for c in range(2):
        for cp in first[c][:3]:
            cp.start()
    for c in range(2):
        loads[1][c].wait()

        def pack_z(x, T):
            u = packed(st_kz, c, x)
            inner = jnp.where(lanes(NR) % 64 == 63, 0.0, u)
            moved = roll(inner, 1)
            KZ[rows(x, c)] = jnp.where(pz == 1, moved, inner)
            KZF[rows(x, c)] = jnp.where(pz == 1, inner, moved)
            return pick(T, u, x, 63)
        skz[c] = lax.fori_loop(0, NP, pack_z, zero32, unroll=8)
    for c in range(2):
        loads[2][c].wait()

        def pack_kx(x, carry):
            KX[rows(x, c)] = packed(st_kx, c, x)
            return carry
        lax.fori_loop(0, NP, pack_kx, 0, unroll=8)
        last = KX[pl.ds(c * SYS + 31 * NR, NR)]
        edge = jnp.logical_and(lanes(NR) >= 64, px == 1)
        KX[pl.ds(c * SYS + 31 * NR, NR)] = jnp.where(edge, 0.0, last)
        first[c][3].start()
    for c in range(2):
        loads[3][c].wait()

        def pack_ky(x, carry):
            u = packed(st_ky, c, x)
            row = lax.broadcasted_iota(jnp.int32, (NR, LN), 0)
            u = jnp.where(jnp.logical_and(row == NR - 1, py == 1), 0.0, u)
            KY[pl.ds(pl.multiple_of(c * KSYS + x * KR + 8, 8), NR)] = u
            return carry
        lax.fori_loop(0, NP, pack_ky, 0, unroll=8)
        sky[c] = KY[pl.ds(c * KSYS + 71, 32, stride=KR)]
        first[c][5].start()
    for c in range(2):
        loads[4][c].wait()
        loads[5][c].wait()
        if c == 0:
            for cp in (first[0][4], first[1][4]):
                cp.start()

        def pack_sb(x, carry):
            D[rows(x, c)] = packed(st_s, c, x)
            R[rows(x, c)] = packed(st_b, c, x)
            return carry
        lax.fori_loop(0, NP, pack_sb, 0, unroll=8)

    def reduce_copies(kind, c):
        return [remote(red.at[kind, c, 0], red.at[kind, c, m], dsend.at[kind, c, m], drecv.at[kind, c, m], others[m]) for m in (7, 6, 5, 4, 3, 2, 1)]

    def reduce_start(kind, c, part):
        red[kind, c, 0] = jnp.sum(part, axis=0, keepdims=True)
        for cp in reduce_copies(kind, c):
            cp.start()

    def reduce_end(kind, c):
        for cp in reduce_copies(kind, c):
            cp.wait_recv()
        v = [red[kind, c, m] for m in range(8)]
        total = ((v[0] + v[1]) + (v[2] + v[3])) + ((v[4] + v[5]) + (v[6] + v[7]))
        total = jnp.broadcast_to(total, (8, LN))
        return jnp.broadcast_to(jnp.sum(total, axis=1, keepdims=True), (8, LN))

    def reduce_sent(kind, c):
        for cp in reduce_copies(kind, c):
            cp.wait_send()

    def fold(val):
        return jnp.sum(val.reshape(-1, 8, LN), axis=0)

    def wide(vec, n):
        return jnp.broadcast_to(vec[None], (n // 8, 8, LN)).reshape(n, LN)

    def r_copies(c):
        return [
            remote(sz.at[c], rhz.at[c], rsend.at[c, 0], rrecv.at[c, 0], nbr['z']),
            remote(sy.at[c], rhy.at[c], rsend.at[c, 1], rrecv.at[c, 1], nbr['y']),
            remote(x_plane(R, c), rhx.at[c], rsend.at[c, 2], rrecv.at[c, 2], nbr['x'])]

    for c in range(2):
        for cp in first[c]:
            cp.wait()
        lo = splits(NR)
        kx_last = KX[pl.ds(c * SYS + 31 * NR, NR)]
        KXM[c] = roll(jnp.where(lo, kx_last, jnp.where(px == 1, jx[c], 0.0)), 64)
        KY[pl.ds(c * KSYS + 7, 32, stride=KR)] = jnp.where(py == 1, jy[c], 0.0)
        KF[c] = jnp.where(pz == 1, jz[c], skz[c])
        PB[pl.ds(c * PSYS + hrow, 32, stride=PR)] = iy[c]
        u_first = PB[pl.ds(c * PSYS + 8, NR)]
        u_last = PB[pl.ds(c * PSYS + 31 * PR + 8, NR)]
        PB[pl.ds(c * PSYS + 32 * PR + 8, NR)] = roll(jnp.where(lo, ix[c], u_first), 64)
        low = roll(jnp.where(lo, u_last, ix[c]), 64)
        kf, uf = KF[c], iz[c]
        mask = face_mask(NR)

        def start_plane(x, carry):
            acc, fx_prev, kx_prev, u = carry
            base = pl.multiple_of(c * PSYS + x * PR, 8)
            at = rows(x, c)
            kbase = pl.multiple_of(c * KSYS + x * KR, 8)
            nxt = PB[pl.ds(base + PR + 8, NR)]
            yu = PB[pl.ds(base + 9, NR)]
            yl = PB[pl.ds(base + 7, NR)]
            s = D[at]
            kxv = KX[at]
            kyv = KY[pl.ds(kbase + 8, NR)]
            kyl = KY[pl.ds(kbase + 7, NR)]
            kzf = jnp.where(mask, spread(kf, x, zf), KZ[at])
            uz = jnp.where(mask, spread(uf, x, zf), roll(u, to_z))
            fx = kxv * (u - nxt)
            fz = kzf * (u - uz)
            fz_away = roll(jnp.where(mask, 0.0, fz), fro_z)
            D[at] = s + (kxv + kx_prev) + (kyv + kyl) + (kzf + KZF[at])
            KZF[at] = kzf
            PZ[at] = uz
            r = R[at] - (s * u + (fx - fx_prev) + (kyv * (u - yu) - kyl * (yl - u)) + (fz - fz_away))
            R[at] = r
            return acc + fold(r * r), fx, kxv, nxt
        acc, _, _, _ = lax.fori_loop(0, NP, start_plane, (jnp.zeros((8, LN), F32), KXM[c] * (low - u_first), KXM[c], u_first), unroll=4)
        reduce_start(0, c, acc)

    def z_face(ref, c):
        def plane(x, T):
            return pick(T, ref[rows(x, c)], x, zf)
        sz[c] = lax.fori_loop(0, NP, plane, zero32, unroll=8)
        sy[c] = ref[pl.ds(c * SYS + yf, 32, stride=NR)]

    def turn_r(c):
        G = rhz[c]
        mask = face_mask(NR)

        def plane(x, carry):
            RZ[rows(x, c)] = jnp.where(mask, spread(G, x, zf), roll(R[rows(x, c)], to_z))
            return carry
        lax.fori_loop(0, NP, plane, 0, unroll=8)

    for c in range(2):
        z_face(R, c)
        for cp in r_copies(c):
            cp.start()
        phx[c] = jnp.zeros((NR, LN), F32)
        phy[c] = zero32
    hist_s[...] = jnp.zeros((8, LN), F32)
    for c in range(2):
        for cp in r_copies(c):
            cp.wait()
        turn_r(c)

    def q_copies(c, par):
        return [
            remote(sz.at[c], qhz.at[par, c], qsend.at[c, 0], qrecv.at[par, c, 0], nbr['z']),
            remote(sy.at[c], qhy.at[par, c], qsend.at[c, 1], qrecv.at[par, c, 1], nbr['y']),
            remote(x_plane(Q, c), qhx.at[par, c], qsend.at[c, 2], qrecv.at[par, c, 2], nbr['x'])]

    def note(c, k, rho):
        hist_s[...] = jnp.where(jnp.logical_and(lane == k, row8 == c), rho, hist_s[...])

    def product(c, beta):
        b64 = wide(beta, NR)
        hx = rhx[c] + b64 * phx[c]
        hy = rhy[c] + wide(beta, 32) * phy[c]
        phx[c] = hx
        phy[c] = hy
        PB[pl.ds(c * PSYS + hrow, 32, stride=PR)] = hy
        lo = splits(NR)

        def direction(x):
            at = pl.ds(c * PSYS + x * PR + 8, NR)
            val = R[pl.ds(c * SYS + x * NR, NR)] + b64 * PB[at]
            PB[at] = val
            return val

        def turn(x, p):
            return roll(KZ[pl.ds(c * SYS + x * NR, NR)] * p, fro_z)

        def load_p(x):
            return PB[pl.ds(c * PSYS + x * PR + 8, NR)]

        p_last = direction(NP - 1)
        p_first = direction(0)
        above = roll(jnp.where(lo, hx, p_first), 64)
        below = roll(jnp.where(lo, p_last, hx), 64)
        turned = {0: turn(0, p_first)}
        for x in range(1, AHEAD):
            turned[x] = turn(x, direction(x))
        cur, kxp_prev = p_first, KXM[c] * below
        acc = jnp.zeros((8, LN), F32)
        for x in range(NP):
            w = x + AHEAD
            if w < NP:
                turned[w] = turn(w, direction(w) if w < NP - 1 else load_p(w))
            nxt = load_p(x + 1) if x + 1 < NP else above
            base = c * PSYS + x * PR
            at = pl.ds(c * SYS + x * NR, NR)
            kbase = c * KSYS + x * KR
            kxv = KX[at]
            kxp = kxv * cur
            q = D[at] * cur - kxp_prev - kxv * nxt
            q = q - KY[pl.ds(kbase + 8, NR)] * PB[pl.ds(base + 9, NR)]
            q = q - KY[pl.ds(kbase + 7, NR)] * PB[pl.ds(base + 7, NR)]
            pz_new = RZ[at] + b64 * PZ[at]
            PZ[at] = pz_new
            q = q - KZF[at] * pz_new - turned.pop(x)
            Q[at] = q
            acc = acc + fold(cur * q)
            cur, kxp_prev = nxt, kxp
        return acc

    CH = 512

    def body(k, carry):
        par = k % 2
        for c in range(2):
            rho = reduce_end(0, c)
            note(c, k, rho)
            beta = jnp.where(k == 0, 0.0, rho / rho_s[c])
            rho_s[c] = rho
            reduce_start(1, c, product(c, beta))
        for c in range(2):
            reduce_sent(0, c)

            z_face(Q, c)
            for cp in q_copies(c, par):
                cp.start()
        for c in range(2):
            alpha = rho_s[c] / reduce_end(1, c)
            alpha_s[c] = alpha
            a_ch = wide(alpha, CH)

            def step_r(i, acc):
                at = pl.ds(pl.multiple_of(c * SYS + i * CH, 8), CH)
                r = R[at] - a_ch * Q[at]
                R[at] = r
                return acc + fold(r * r)
            acc = lax.fori_loop(0, SYS // CH, step_r, jnp.zeros((8, LN), F32))
            reduce_start(0, c, acc)

            def step_x(x, carry):
                at = pl.ds(pl.multiple_of(c * SYS + x * NR, 8), NR)
                X[at] = X[at] + wide(alpha, NR) * PB[pl.ds(pl.multiple_of(c * PSYS + x * PR + 8, 8), NR)]
                return carry
            lax.fori_loop(0, NP, step_x, 0, unroll=4)
        for c in range(2):
            reduce_sent(1, c)
            for cp in q_copies(c, par):
                cp.wait()
            alpha = alpha_s[c]
            rhx[c] = rhx[c] - wide(alpha, NR) * qhx[par, c]
            rhy[c] = rhy[c] - wide(alpha, 32) * qhy[par, c]
            rhz[c] = rhz[c] - wide(alpha, 32) * qhz[par, c]
            turn_r(c)
        return carry

    lax.fori_loop(0, ITERS, body, 0)
    outs = [pltpu.make_async_copy(X.at[pl.ds(c * SYS, SYS)], x_out.at[pl.ds(c * SYS, SYS)], out_sem.at[c]) for c in range(2)]
    for cp in outs:
        cp.start()
    for c in range(2):
        note(c, ITERS, reduce_end(0, c))
        reduce_sent(0, c)
    hist_out[...] = jnp.sqrt(hist_s[...] * (1.0 / (128 * 128 * 128)))
    for cp in outs:
        cp.wait()


CHUNKS = 2
VMEM_MAIN = 60 * 1024 * 1024


def unpack(xp, hist, x_out, hist_out, buf, st, hs, ho, in_sem, out_sem, h_sem):
    planes = NP // CHUNKS
    hist_in = pltpu.make_async_copy(hist, hs, h_sem.at[0])
    hist_in.start()
    loads = []
    for n in range(2 * CHUNKS):
        at = pl.ds(n * planes * NR, planes * NR)
        loads.append(pltpu.make_async_copy(xp.at[at], buf.at[at], in_sem.at[n]))
        loads[n].start()
    stores = []
    for n in range(2 * CHUNKS):
        c, x0 = n // CHUNKS, n % CHUNKS * planes
        loads[n].wait()

        def plane(x, carry):
            val = buf[pl.ds(pl.multiple_of(n * planes * NR + x * NR, 8), NR)]
            st[c, x0 + x] = val[:, :64]
            st[c, x0 + x + NP] = roll(val, 64)[:, :64]
            return carry
        lax.fori_loop(0, planes, plane, 0, unroll=16)
        for h in range(2):
            at = pl.ds(x0 + NP * h, planes)
            stores.append(pltpu.make_async_copy(st.at[c, at], x_out.at[c, at], out_sem.at[n, h]))
            stores[-1].start()
    hist_in.wait()
    ho[...] = hs[:2, :ITERS + 1]
    stores.append(pltpu.make_async_copy(ho, hist_out, h_sem.at[1]))
    stores[-1].start()
    for cp in stores:
        cp.wait()


def run(s, b, x0, kx, ky, kz):
    v = lambda *shape: pltpu.VMEM(shape, F32)
    sem = lambda *shape: pltpu.SemaphoreType.DMA(shape)
    scratch = [v(2, 64, 64, 64)] * 6
    full = v(2 * SYS, LN)
    scratch += [full, full, full, v(2 * PSYS, LN), full, full, full, v(2, NR, LN), v(2 * KSYS, LN), full, full, full, v(2, 32, LN)]
    scratch += [v(2, NR, LN), v(2, 32, LN), v(2, 32, LN)] * 2
    scratch += [v(2, 32, LN)] * 6
    scratch += [v(2, NR, LN), v(2, 32, LN), v(2, 32, LN), v(2, NR, LN), v(2, 32, LN)]
    scratch += [v(2, 2, NR, LN), v(2, 2, 32, LN), v(2, 2, 32, LN)]
    scratch += [v(2, 2, 8, 1, LN), v(2, 8, LN), v(2, 8, LN), v(8, LN)]
    scratch += [sem(6, 2), sem(2, 6), sem(2, 6), sem(2, 3), sem(2, 3), sem(2, 3), sem(2, 2, 3), sem(2, 2, 8), sem(2, 2, 8), sem(2)]
    xp, hist = pl.pallas_call(
        kernel,
        out_shape=(jax.ShapeDtypeStruct((2 * SYS, LN), F32), jax.ShapeDtypeStruct((8, LN), F32)),
        in_specs=[pl.BlockSpec(memory_space=pl.ANY)] * 6,
        out_specs=(pl.BlockSpec(memory_space=pl.ANY), pl.BlockSpec(memory_space=pltpu.VMEM)),
        scratch_shapes=scratch,
        compiler_params=pltpu.CompilerParams(collective_id=0, has_side_effects=True, vmem_limit_bytes=VMEM_MAIN),
        name='cg',
    )(s, b, x0, kx, ky, kz)
    return pl.pallas_call(
        unpack,
        out_shape=(jax.ShapeDtypeStruct((2, 64, 64, 64), F32), jax.ShapeDtypeStruct((2, ITERS + 1), F32)),
        in_specs=[pl.BlockSpec(memory_space=pl.ANY)] * 2,
        out_specs=[pl.BlockSpec(memory_space=pl.ANY)] * 2,
        scratch_shapes=[v(2 * SYS, LN), v(2, 64, 64, 64), v(8, LN), v(2, ITERS + 1), sem(2 * CHUNKS), sem(2 * CHUNKS, 2), sem(2)],
        compiler_params=pltpu.CompilerParams(vmem_limit_bytes=60 * 1024 * 1024),
        name='unpack',
    )(xp, hist)


def solution(mesh):
    field = P(None, 'px', 'py', 'pz')
    return jax.shard_map(run, mesh=mesh, in_specs=(field,) * 6, out_specs=(field, P(None, None)), check_vma=False)
```

```python
import jax
import jax.numpy as jnp
from jax import lax
from jax.experimental import pallas as pl
from jax.experimental.pallas import tpu as pltpu
from jax.sharding import PartitionSpec as P

ITERS = 20
F32 = jnp.float32
MESH = pl.DeviceIdType.MESH

NP = 32
NR = 64
LN = 128
PR = 80
KR = 72
SYS = NP * NR
PSYS = (NP + 1) * PR
KSYS = NP * KR
AHEAD = 3


def roll(val, shift):
    if isinstance(shift, int):
        shift = shift % LN
    return pltpu.roll(val, shift, 1)


def kernel(s_hbm, b_hbm, x0_hbm, kx_hbm, ky_hbm, kz_hbm, x_out, hist_out,
           st_s, st_b, st_x, st_kx, st_ky, st_kz,
           X, R, Q, PB, PZ, RZ, KX, KXM, KY, KZ, KZF, D, KF,
           ix, iy, iz, jx, jy, jz, sxy, sxz, sky, skz, sy, sz,
           rhx, rhy, rhz, phx, phy, qhx, qhy, qhz,
           red, rho_s, alpha_s, hist_s,
           ld_sem, isend, irecv, rsend, rrecv, qsend, qrecv, dsend, drecv, out_sem):
    pz, py, px = lax.axis_index('pz'), lax.axis_index('py'), lax.axis_index('px')
    nbr = {'x': (pz, py, 1 - px), 'y': (pz, 1 - py, px), 'z': (1 - pz, py, px)}
    others = {}
    for m in range(1, 8):
        others[m] = (1 - pz if m & 4 else pz, 1 - py if m & 2 else py, 1 - px if m & 1 else px)

    lane = lax.broadcasted_iota(jnp.int32, (8, LN), 1)
    row8 = lax.broadcasted_iota(jnp.int32, (8, LN), 0)

    def lanes(n):
        return lax.broadcasted_iota(jnp.int32, (n, LN), 1)

    zf = 63 * (1 - pz)
    xf = 31 * (1 - px)
    yf = 63 * (1 - py)
    hrow = 72 - 65 * py
    to_z = 127 - 126 * pz
    fro_z = 1 + 126 * pz

    def face_mask(n):
        return (lanes(n) % 64) == zf

    def splits(n):
        return lanes(n) < 64

    loads = []
    for num, (src, dst) in enumerate(((x0_hbm, st_x), (kz_hbm, st_kz), (kx_hbm, st_kx), (ky_hbm, st_ky), (s_hbm, st_s), (b_hbm, st_b))):
        pair = [pltpu.make_async_copy(src.at[c], dst.at[c], ld_sem.at[num, c]) for c in range(2)]
        loads.append(pair)
    for num in range(1):
        for cp in loads[num]:
            cp.start()

    barrier = pltpu.get_barrier_semaphore()
    for m in range(1, 8):
        pl.semaphore_signal(barrier, inc=1, device_id=others[m], device_id_type=MESH)

    def packed(st, c, x):
        return jnp.concatenate([st[c, x], st[c, x + NP]], axis=1)

    def pick(T, val, x, f):
        l64 = lanes(32) % 64
        T = jnp.where(l64 == x, roll(val[:32], lax.rem(x - f + LN, LN)), T)
        return jnp.where(l64 == x + 32, roll(val[32:], lax.rem(x + 32 - f + LN, LN)), T)

    def spread(G, x, f):
        return jnp.concatenate([roll(G, lax.rem(f - x + LN, LN)), roll(G, lax.rem(f - x - 32 + LN, LN))], axis=0)

    zero32 = jnp.zeros((32, LN), F32)

    def remote(src, dst, send_sem, recv_sem, dev):
        return pltpu.make_async_remote_copy(src_ref=src, dst_ref=dst, send_sem=send_sem, recv_sem=recv_sem, device_id=dev, device_id_type=MESH)

    def x_plane(ref, c):
        return ref.at[pl.ds(pl.multiple_of(c * SYS + xf * NR, 8), NR)]

    def rows(x, c):
        return pl.ds(pl.multiple_of(c * SYS + x * NR, 8), NR)

    first = []
    for c in range(2):
        first.append([
            remote(sxz.at[c], iz.at[c], isend.at[c, 0], irecv.at[c, 0], nbr['z']),
            remote(sxy.at[c], iy.at[c], isend.at[c, 1], irecv.at[c, 1], nbr['y']),
            remote(x_plane(X, c), ix.at[c], isend.at[c, 2], irecv.at[c, 2], nbr['x']),
            remote(skz.at[c], jz.at[c], isend.at[c, 3], irecv.at[c, 3], nbr['z']),
            remote(sky.at[c], jy.at[c], isend.at[c, 4], irecv.at[c, 4], nbr['y']),
            remote(KX.at[pl.ds(c * SYS + 31 * NR, NR)], jx.at[c], isend.at[c, 5], irecv.at[c, 5], nbr['x'])])

    for c in range(2):
        loads[0][c].wait()
        for num in ((1, 2), (3, 4, 5))[c]:
            for cp in loads[num]:
                cp.start()

        def pack_x(x, T):
            u = packed(st_x, c, x)
            X[rows(x, c)] = u
            base = pl.multiple_of(c * PSYS + x * PR, 8)
            PB[pl.ds(base, 8)] = jnp.zeros((8, LN), F32)
            PB[pl.ds(base + 72, 8)] = jnp.zeros((8, LN), F32)
            PB[pl.ds(base + 8, NR)] = u
            return pick(T, u, x, zf)
        sxz[c] = lax.fori_loop(0, NP, pack_x, zero32, unroll=8)
        sxy[c] = X[pl.ds(c * SYS + yf, 32, stride=NR)]
    pl.semaphore_wait(barrier, 7)
    for c in range(2):
        for cp in first[c][:3]:
            cp.start()
    for c in range(2):
        loads[1][c].wait()

        def pack_z(x, T):
            u = packed(st_kz, c, x)
            inner = jnp.where(lanes(NR) % 64 == 63, 0.0, u)
            moved = roll(inner, 1)
            KZ[rows(x, c)] = jnp.where(pz == 1, moved, inner)
            KZF[rows(x, c)] = jnp.where(pz == 1, inner, moved)
            return pick(T, u, x, 63)
        skz[c] = lax.fori_loop(0, NP, pack_z, zero32, unroll=8)
    for c in range(2):
        loads[2][c].wait()

        def pack_kx(x, carry):
            KX[rows(x, c)] = packed(st_kx, c, x)
            return carry
        lax.fori_loop(0, NP, pack_kx, 0, unroll=8)
        last = KX[pl.ds(c * SYS + 31 * NR, NR)]
        edge = jnp.logical_and(lanes(NR) >= 64, px == 1)
        KX[pl.ds(c * SYS + 31 * NR, NR)] = jnp.where(edge, 0.0, last)
        first[c][3].start()
    for c in range(2):
        loads[3][c].wait()

        def pack_ky(x, carry):
            u = packed(st_ky, c, x)
            row = lax.broadcasted_iota(jnp.int32, (NR, LN), 0)
            u = jnp.where(jnp.logical_and(row == NR - 1, py == 1), 0.0, u)
            KY[pl.ds(pl.multiple_of(c * KSYS + x * KR + 8, 8), NR)] = u
            return carry
        lax.fori_loop(0, NP, pack_ky, 0, unroll=8)
        sky[c] = KY[pl.ds(c * KSYS + 71, 32, stride=KR)]
        first[c][5].start()
    for c in range(2):
        loads[4][c].wait()
        loads[5][c].wait()
        if c == 0:
            for cp in (first[0][4], first[1][4]):
                cp.start()

        def pack_sb(x, carry):
            D[rows(x, c)] = packed(st_s, c, x)
            R[rows(x, c)] = packed(st_b, c, x)
            return carry
        lax.fori_loop(0, NP, pack_sb, 0, unroll=8)

    def reduce_copies(kind, c):
        return [remote(red.at[kind, c, 0], red.at[kind, c, m], dsend.at[kind, c, m], drecv.at[kind, c, m], others[m]) for m in (7, 6, 5, 4, 3, 2, 1)]

    def reduce_start(kind, c, part):
        red[kind, c, 0] = jnp.sum(part, axis=0, keepdims=True)
        for cp in reduce_copies(kind, c):
            cp.start()

    def reduce_end(kind, c):
        for cp in reduce_copies(kind, c):
            cp.wait_recv()
        v = [red[kind, c, m] for m in range(8)]
        total = ((v[0] + v[1]) + (v[2] + v[3])) + ((v[4] + v[5]) + (v[6] + v[7]))
        total = jnp.broadcast_to(total, (8, LN))
        return jnp.broadcast_to(jnp.sum(total, axis=1, keepdims=True), (8, LN))

    def reduce_sent(kind, c):
        for cp in reduce_copies(kind, c):
            cp.wait_send()

    def fold(val):
        return jnp.sum(val.reshape(-1, 8, LN), axis=0)

    def wide(vec, n):
        return jnp.broadcast_to(vec[None], (n // 8, 8, LN)).reshape(n, LN)

    def z_face(ref, c):
        def plane(x, T):
            return pick(T, ref[rows(x, c)], x, zf)
        sz[c] = lax.fori_loop(0, NP, plane, zero32, unroll=8)
        sy[c] = ref[pl.ds(c * SYS + yf, 32, stride=NR)]

    def turn_r(c):
        G = rhz[c]
        mask = face_mask(NR)

        def plane(x, carry):
            RZ[rows(x, c)] = jnp.where(mask, spread(G, x, zf), roll(R[rows(x, c)], to_z))
            return carry
        lax.fori_loop(0, NP, plane, 0, unroll=8)

    def r_copies(c):
        return [
            remote(sz.at[c], rhz.at[c], rsend.at[c, 0], rrecv.at[c, 0], nbr['z']),
            remote(sy.at[c], rhy.at[c], rsend.at[c, 1], rrecv.at[c, 1], nbr['y']),
            remote(x_plane(R, c), rhx.at[c], rsend.at[c, 2], rrecv.at[c, 2], nbr['x'])]

    for c in range(2):
        for cp in first[c]:
            cp.wait()
        lo = splits(NR)
        kx_last = KX[pl.ds(c * SYS + 31 * NR, NR)]
        KXM[c] = roll(jnp.where(lo, kx_last, jnp.where(px == 1, jx[c], 0.0)), 64)
        KY[pl.ds(c * KSYS + 7, 32, stride=KR)] = jnp.where(py == 1, jy[c], 0.0)
        KF[c] = jnp.where(pz == 1, jz[c], skz[c])
        PB[pl.ds(c * PSYS + hrow, 32, stride=PR)] = iy[c]
        u_first = PB[pl.ds(c * PSYS + 8, NR)]
        u_last = PB[pl.ds(c * PSYS + 31 * PR + 8, NR)]
        PB[pl.ds(c * PSYS + 32 * PR + 8, NR)] = roll(jnp.where(lo, ix[c], u_first), 64)
        low = roll(jnp.where(lo, u_last, ix[c]), 64)
        kf, uf = KF[c], iz[c]
        mask = face_mask(NR)

        def start_plane(x, carry):
            acc, fx_prev, kx_prev, u = carry
            base = pl.multiple_of(c * PSYS + x * PR, 8)
            at = rows(x, c)
            kbase = pl.multiple_of(c * KSYS + x * KR, 8)
            nxt = PB[pl.ds(base + PR + 8, NR)]
            yu = PB[pl.ds(base + 9, NR)]
            yl = PB[pl.ds(base + 7, NR)]
            s = D[at]
            kxv = KX[at]
            kyv = KY[pl.ds(kbase + 8, NR)]
            kyl = KY[pl.ds(kbase + 7, NR)]
            kzf = jnp.where(mask, spread(kf, x, zf), KZ[at])
            uz = jnp.where(mask, spread(uf, x, zf), roll(u, to_z))
            fx = kxv * (u - nxt)
            fz = kzf * (u - uz)
            fz_away = roll(jnp.where(mask, 0.0, fz), fro_z)
            D[at] = s + (kxv + kx_prev) + (kyv + kyl) + (kzf + KZF[at])
            KZF[at] = kzf
            PZ[at] = uz
            r = R[at] - (s * u + (fx - fx_prev) + (kyv * (u - yu) - kyl * (yl - u)) + (fz - fz_away))
            R[at] = r
            return acc + fold(r * r), fx, kxv, nxt
        acc, _, _, _ = lax.fori_loop(0, NP, start_plane, (jnp.zeros((8, LN), F32), KXM[c] * (low - u_first), KXM[c], u_first), unroll=4)
        reduce_start(0, c, acc)
        z_face(R, c)
        for cp in r_copies(c):
            cp.start()

    hist_s[...] = jnp.zeros((8, LN), F32)
    for c in range(2):
        phx[c] = jnp.zeros((NR, LN), F32)
        phy[c] = zero32
        for cp in r_copies(c):
            cp.wait_send()

    def q_copies(c, par):
        return [
            remote(sz.at[c], qhz.at[par, c], qsend.at[c, 0], qrecv.at[par, c, 0], nbr['z']),
            remote(sy.at[c], qhy.at[par, c], qsend.at[c, 1], qrecv.at[par, c, 1], nbr['y']),
            remote(x_plane(Q, c), qhx.at[par, c], qsend.at[c, 2], qrecv.at[par, c, 2], nbr['x'])]

    def note(c, k, rho):
        hist_s[...] = jnp.where(jnp.logical_and(lane == k, row8 == c), rho, hist_s[...])

    def product(c, beta):
        b64 = wide(beta, NR)
        hx = rhx[c] + b64 * phx[c]
        hy = rhy[c] + wide(beta, 32) * phy[c]
        phx[c] = hx
        phy[c] = hy
        PB[pl.ds(c * PSYS + hrow, 32, stride=PR)] = hy
        lo = splits(NR)

        def direction(x):
            at = pl.ds(c * PSYS + x * PR + 8, NR)
            val = R[pl.ds(c * SYS + x * NR, NR)] + b64 * PB[at]
            PB[at] = val
            return val

        def turn(x, p):
            return roll(KZ[pl.ds(c * SYS + x * NR, NR)] * p, fro_z)

        def load_p(x):
            return PB[pl.ds(c * PSYS + x * PR + 8, NR)]

        p_last = direction(NP - 1)
        p_first = direction(0)
        above = roll(jnp.where(lo, hx, p_first), 64)
        below = roll(jnp.where(lo, p_last, hx), 64)
        turned = {0: turn(0, p_first)}
        for x in range(1, AHEAD):
            turned[x] = turn(x, direction(x))
        cur, kxp_prev = p_first, KXM[c] * below
        acc = jnp.zeros((8, LN), F32)
        for x in range(NP):
            w = x + AHEAD
            if w < NP:
                turned[w] = turn(w, direction(w) if w < NP - 1 else load_p(w))
            nxt = load_p(x + 1) if x + 1 < NP else above
            base = c * PSYS + x * PR
            at = pl.ds(c * SYS + x * NR, NR)
            kbase = c * KSYS + x * KR
            kxv = KX[at]
            kxp = kxv * cur
            q = D[at] * cur - kxp_prev - kxv * nxt
            q = q - KY[pl.ds(kbase + 8, NR)] * PB[pl.ds(base + 9, NR)]
            q = q - KY[pl.ds(kbase + 7, NR)] * PB[pl.ds(base + 7, NR)]
            pz_new = RZ[at] + b64 * PZ[at]
            PZ[at] = pz_new
            q = q - KZF[at] * pz_new - turned.pop(x)
            Q[at] = q
            acc = acc + fold(cur * q)
            cur, kxp_prev = nxt, kxp
        return acc

    def body(k, carry):
        par = k % 2
        for c in range(2):
            @pl.when(k == 0)
            def _():
                for cp in r_copies(c):
                    cp.wait_recv()
            turn_r(c)
            rho = reduce_end(0, c)
            note(c, k, rho)
            beta = jnp.where(k == 0, 0.0, rho / rho_s[c])
            rho_s[c] = rho
            reduce_start(1, c, product(c, beta))
        for c in range(2):
            reduce_sent(0, c)

            z_face(Q, c)
            for cp in q_copies(c, par):
                cp.start()
        for c in range(2):
            alpha = rho_s[c] / reduce_end(1, c)
            alpha_s[c] = alpha
            a_ch = wide(alpha, NR)
            acc = jnp.zeros((8, LN), F32)
            for x in range(NP):
                at = pl.ds(c * SYS + x * NR, NR)
                r = R[at] - a_ch * Q[at]
                R[at] = r
                acc = acc + fold(r * r)
            reduce_start(0, c, acc)

            def step_x(x, carry):
                at = pl.ds(pl.multiple_of(c * SYS + x * NR, 8), NR)
                X[at] = X[at] + wide(alpha, NR) * PB[pl.ds(pl.multiple_of(c * PSYS + x * PR + 8, 8), NR)]
                return carry
            lax.fori_loop(0, NP, step_x, 0, unroll=4)
        for c in range(2):
            reduce_sent(1, c)
            for cp in q_copies(c, par):
                cp.wait()
            alpha = alpha_s[c]
            rhx[c] = rhx[c] - wide(alpha, NR) * qhx[par, c]
            rhy[c] = rhy[c] - wide(alpha, 32) * qhy[par, c]
            rhz[c] = rhz[c] - wide(alpha, 32) * qhz[par, c]
        return carry

    lax.fori_loop(0, ITERS, body, 0)
    outs = [pltpu.make_async_copy(X.at[pl.ds(c * SYS, SYS)], x_out.at[pl.ds(c * SYS, SYS)], out_sem.at[c]) for c in range(2)]
    for cp in outs:
        cp.start()
    for c in range(2):
        note(c, ITERS, reduce_end(0, c))
        reduce_sent(0, c)
    hist_out[...] = jnp.sqrt(hist_s[...] * (1.0 / (128 * 128 * 128)))
    for cp in outs:
        cp.wait()


CHUNKS = 2
VMEM_MAIN = 60 * 1024 * 1024


def unpack(xp, hist, x_out, hist_out, buf, st, hs, ho, in_sem, out_sem, h_sem):
    planes = NP // CHUNKS
    hist_in = pltpu.make_async_copy(hist, hs, h_sem.at[0])
    hist_in.start()
    loads = []
    for n in range(2 * CHUNKS):
        at = pl.ds(n * planes * NR, planes * NR)
        loads.append(pltpu.make_async_copy(xp.at[at], buf.at[at], in_sem.at[n]))
        loads[n].start()
    stores = []
    for n in range(2 * CHUNKS):
        c, x0 = n // CHUNKS, n % CHUNKS * planes
        loads[n].wait()

        def plane(x, carry):
            val = buf[pl.ds(pl.multiple_of(n * planes * NR + x * NR, 8), NR)]
            st[c, x0 + x] = val[:, :64]
            st[c, x0 + x + NP] = roll(val, 64)[:, :64]
            return carry
        lax.fori_loop(0, planes, plane, 0, unroll=16)
        for h in range(2):
            at = pl.ds(x0 + NP * h, planes)
            stores.append(pltpu.make_async_copy(st.at[c, at], x_out.at[c, at], out_sem.at[n, h]))
            stores[-1].start()
    hist_in.wait()
    ho[...] = hs[:2, :ITERS + 1]
    stores.append(pltpu.make_async_copy(ho, hist_out, h_sem.at[1]))
    stores[-1].start()
    for cp in stores:
        cp.wait()


def run(s, b, x0, kx, ky, kz):
    v = lambda *shape: pltpu.VMEM(shape, F32)
    sem = lambda *shape: pltpu.SemaphoreType.DMA(shape)
    scratch = [v(2, 64, 64, 64)] * 6
    full = v(2 * SYS, LN)
    scratch += [full, full, full, v(2 * PSYS, LN), full, full, full, v(2, NR, LN), v(2 * KSYS, LN), full, full, full, v(2, 32, LN)]
    scratch += [v(2, NR, LN), v(2, 32, LN), v(2, 32, LN)] * 2
    scratch += [v(2, 32, LN)] * 6
    scratch += [v(2, NR, LN), v(2, 32, LN), v(2, 32, LN), v(2, NR, LN), v(2, 32, LN)]
    scratch += [v(2, 2, NR, LN), v(2, 2, 32, LN), v(2, 2, 32, LN)]
    scratch += [v(2, 2, 8, 1, LN), v(2, 8, LN), v(2, 8, LN), v(8, LN)]
    scratch += [sem(6, 2), sem(2, 6), sem(2, 6), sem(2, 3), sem(2, 3), sem(2, 3), sem(2, 2, 3), sem(2, 2, 8), sem(2, 2, 8), sem(2)]
    xp, hist = pl.pallas_call(
        kernel,
        out_shape=(jax.ShapeDtypeStruct((2 * SYS, LN), F32), jax.ShapeDtypeStruct((8, LN), F32)),
        in_specs=[pl.BlockSpec(memory_space=pl.ANY)] * 6,
        out_specs=(pl.BlockSpec(memory_space=pl.ANY), pl.BlockSpec(memory_space=pltpu.VMEM)),
        scratch_shapes=scratch,
        compiler_params=pltpu.CompilerParams(collective_id=0, has_side_effects=True, vmem_limit_bytes=VMEM_MAIN),
        name='cg',
    )(s, b, x0, kx, ky, kz)
    return pl.pallas_call(
        unpack,
        out_shape=(jax.ShapeDtypeStruct((2, 64, 64, 64), F32), jax.ShapeDtypeStruct((2, ITERS + 1), F32)),
        in_specs=[pl.BlockSpec(memory_space=pl.ANY)] * 2,
        out_specs=[pl.BlockSpec(memory_space=pl.ANY)] * 2,
        scratch_shapes=[v(2 * SYS, LN), v(2, 64, 64, 64), v(8, LN), v(2, ITERS + 1), sem(2 * CHUNKS), sem(2 * CHUNKS, 2), sem(2)],
        compiler_params=pltpu.CompilerParams(vmem_limit_bytes=60 * 1024 * 1024),
        name='unpack',
    )(xp, hist)


def solution(mesh):
    field = P(None, 'px', 'py', 'pz')
    return jax.shard_map(run, mesh=mesh, in_specs=(field,) * 6, out_specs=(field, P(None, None)), check_vma=False)
```

```python
import jax
import jax.numpy as jnp
from jax import lax
from jax.experimental import pallas as pl
from jax.experimental.pallas import tpu as pltpu
from jax.sharding import PartitionSpec as P

ITERS = 20
F32 = jnp.float32
MESH = pl.DeviceIdType.MESH

NP = 32
NR = 64
LN = 128
PR = 80
KR = 72
SYS = NP * NR
PSYS = (NP + 1) * PR
KSYS = NP * KR
AHEAD = 3


def roll(val, shift):
    if isinstance(shift, int):
        shift = shift % LN
    return pltpu.roll(val, shift, 1)


def kernel(s_hbm, b_hbm, x0_hbm, kx_hbm, ky_hbm, kz_hbm, x_out, hist_out,
           st_s, st_b, st_x, st_kx, st_ky, st_kz,
           X, R, Q, PB, PZ, RZ, KX, KXM, KY, KZ, KZF, D, KF,
           ix, iy, iz, jx, jy, jz, sxy, sxz, sky, skz, sy, sz,
           rhx, rhy, rhz, phx, phy, qhx, qhy, qhz,
           red, rho_s, alpha_s, hist_s,
           ld_sem, isend, irecv, rsend, rrecv, qsend, qrecv, dsend, drecv, out_sem):
    pz, py, px = lax.axis_index('pz'), lax.axis_index('py'), lax.axis_index('px')
    nbr = {'x': (pz, py, 1 - px), 'y': (pz, 1 - py, px), 'z': (1 - pz, py, px)}
    others = {}
    for m in range(1, 8):
        others[m] = (1 - pz if m & 4 else pz, 1 - py if m & 2 else py, 1 - px if m & 1 else px)

    lane = lax.broadcasted_iota(jnp.int32, (8, LN), 1)
    row8 = lax.broadcasted_iota(jnp.int32, (8, LN), 0)

    def lanes(n):
        return lax.broadcasted_iota(jnp.int32, (n, LN), 1)

    zf = 63 * (1 - pz)
    xf = 31 * (1 - px)
    yf = 63 * (1 - py)
    hrow = 72 - 65 * py
    to_z = 127 - 126 * pz
    fro_z = 1 + 126 * pz

    def face_mask(n):
        return (lanes(n) % 64) == zf

    def splits(n):
        return lanes(n) < 64

    loads = []
    for num, (src, dst) in enumerate(((x0_hbm, st_x), (kz_hbm, st_kz), (kx_hbm, st_kx), (ky_hbm, st_ky), (s_hbm, st_s), (b_hbm, st_b))):
        pair = [pltpu.make_async_copy(src.at[c], dst.at[c], ld_sem.at[num, c]) for c in range(2)]
        loads.append(pair)
    for num in range(1):
        for cp in loads[num]:
            cp.start()

    barrier = pltpu.get_barrier_semaphore()
    for m in range(1, 8):
        pl.semaphore_signal(barrier, inc=1, device_id=others[m], device_id_type=MESH)

    def packed(st, c, x):
        return jnp.concatenate([st[c, x], st[c, x + NP]], axis=1)

    def pick(T, val, x, f):
        l64 = lanes(32) % 64
        T = jnp.where(l64 == x, roll(val[:32], lax.rem(x - f + LN, LN)), T)
        return jnp.where(l64 == x + 32, roll(val[32:], lax.rem(x + 32 - f + LN, LN)), T)

    def spread(G, x, f):
        return jnp.concatenate([roll(G, lax.rem(f - x + LN, LN)), roll(G, lax.rem(f - x - 32 + LN, LN))], axis=0)

    zero32 = jnp.zeros((32, LN), F32)

    def remote(src, dst, send_sem, recv_sem, dev):
        return pltpu.make_async_remote_copy(src_ref=src, dst_ref=dst, send_sem=send_sem, recv_sem=recv_sem, device_id=dev, device_id_type=MESH)

    def x_plane(ref, c):
        return ref.at[pl.ds(pl.multiple_of(c * SYS + xf * NR, 8), NR)]

    def rows(x, c):
        return pl.ds(pl.multiple_of(c * SYS + x * NR, 8), NR)

    first = []
    for c in range(2):
        first.append([
            remote(sxz.at[c], iz.at[c], isend.at[c, 0], irecv.at[c, 0], nbr['z']),
            remote(sxy.at[c], iy.at[c], isend.at[c, 1], irecv.at[c, 1], nbr['y']),
            remote(x_plane(X, c), ix.at[c], isend.at[c, 2], irecv.at[c, 2], nbr['x']),
            remote(skz.at[c], jz.at[c], isend.at[c, 3], irecv.at[c, 3], nbr['z']),
            remote(sky.at[c], jy.at[c], isend.at[c, 4], irecv.at[c, 4], nbr['y']),
            remote(KX.at[pl.ds(c * SYS + 31 * NR, NR)], jx.at[c], isend.at[c, 5], irecv.at[c, 5], nbr['x'])])

    for c in range(2):
        loads[0][c].wait()
        for num in ((1, 2), (3, 4, 5))[c]:
            for cp in loads[num]:
                cp.start()

        def pack_x(x, T):
            u = packed(st_x, c, x)
            X[rows(x, c)] = u
            base = pl.multiple_of(c * PSYS + x * PR, 8)
            PB[pl.ds(base, 8)] = jnp.zeros((8, LN), F32)
            PB[pl.ds(base + 72, 8)] = jnp.zeros((8, LN), F32)
            PB[pl.ds(base + 8, NR)] = u
            return pick(T, u, x, zf)
        sxz[c] = lax.fori_loop(0, NP, pack_x, zero32, unroll=8)
        sxy[c] = X[pl.ds(c * SYS + yf, 32, stride=NR)]
    pl.semaphore_wait(barrier, 7)
    for c in range(2):
        for cp in first[c][:3]:
            cp.start()
    for c in range(2):
        loads[1][c].wait()

        def pack_z(x, T):
            u = packed(st_kz, c, x)
            inner = jnp.where(lanes(NR) % 64 == 63, 0.0, u)
            moved = roll(inner, 1)
            KZ[rows(x, c)] = jnp.where(pz == 1, moved, inner)
            KZF[rows(x, c)] = jnp.where(pz == 1, inner, moved)
            return pick(T, u, x, 63)
        skz[c] = lax.fori_loop(0, NP, pack_z, zero32, unroll=8)
    for c in range(2):
        loads[2][c].wait()

        def pack_kx(x, carry):
            KX[rows(x, c)] = packed(st_kx, c, x)
            return carry
        lax.fori_loop(0, NP, pack_kx, 0, unroll=8)
        last = KX[pl.ds(c * SYS + 31 * NR, NR)]
        edge = jnp.logical_and(lanes(NR) >= 64, px == 1)
        KX[pl.ds(c * SYS + 31 * NR, NR)] = jnp.where(edge, 0.0, last)
        first[c][3].start()
    for c in range(2):
        loads[3][c].wait()

        def pack_ky(x, carry):
            u = packed(st_ky, c, x)
            row = lax.broadcasted_iota(jnp.int32, (NR, LN), 0)
            u = jnp.where(jnp.logical_and(row == NR - 1, py == 1), 0.0, u)
            KY[pl.ds(pl.multiple_of(c * KSYS + x * KR + 8, 8), NR)] = u
            return carry
        lax.fori_loop(0, NP, pack_ky, 0, unroll=8)
        sky[c] = KY[pl.ds(c * KSYS + 71, 32, stride=KR)]
        first[c][5].start()
    for c in range(2):
        loads[4][c].wait()
        loads[5][c].wait()
        if c == 0:
            for cp in (first[0][4], first[1][4]):
                cp.start()

        def pack_sb(x, carry):
            D[rows(x, c)] = packed(st_s, c, x)
            R[rows(x, c)] = packed(st_b, c, x)
            return carry
        lax.fori_loop(0, NP, pack_sb, 0, unroll=8)

    def reduce_copies(kind, c):
        return [remote(red.at[kind, c, 0], red.at[kind, c, m], dsend.at[kind, c, m], drecv.at[kind, c, m], others[m]) for m in (7, 6, 5, 4, 3, 2, 1)]

    def reduce_start(kind, c, part):
        red[kind, c, 0] = jnp.sum(part, axis=0, keepdims=True)
        for cp in reduce_copies(kind, c):
            cp.start()

    def reduce_end(kind, c):
        for cp in reduce_copies(kind, c):
            cp.wait_recv()
        v = [red[kind, c, m] for m in range(8)]
        total = ((v[0] + v[1]) + (v[2] + v[3])) + ((v[4] + v[5]) + (v[6] + v[7]))
        total = jnp.broadcast_to(total, (8, LN))
        return jnp.broadcast_to(jnp.sum(total, axis=1, keepdims=True), (8, LN))

    def reduce_sent(kind, c):
        for cp in reduce_copies(kind, c):
            cp.wait_send()

    def fold(val):
        return jnp.sum(val.reshape(-1, 8, LN), axis=0)

    def wide(vec, n):
        return jnp.broadcast_to(vec[None], (n // 8, 8, LN)).reshape(n, LN)

    def z_face(ref, c):
        def plane(x, T):
            return pick(T, ref[rows(x, c)], x, zf)
        sz[c] = lax.fori_loop(0, NP, plane, zero32, unroll=8)
        sy[c] = ref[pl.ds(c * SYS + yf, 32, stride=NR)]

    def turn_r(c):
        G = rhz[c]
        mask = face_mask(NR)

        def plane(x, carry):
            RZ[rows(x, c)] = jnp.where(mask, spread(G, x, zf), roll(R[rows(x, c)], to_z))
            return carry
        lax.fori_loop(0, NP, plane, 0, unroll=8)

    def r_copies(c):
        return [
            remote(sz.at[c], rhz.at[c], rsend.at[c, 0], rrecv.at[c, 0], nbr['z']),
            remote(sy.at[c], rhy.at[c], rsend.at[c, 1], rrecv.at[c, 1], nbr['y']),
            remote(x_plane(R, c), rhx.at[c], rsend.at[c, 2], rrecv.at[c, 2], nbr['x'])]

    for c in range(2):
        for cp in first[c]:
            cp.wait()
        lo = splits(NR)
        kx_last = KX[pl.ds(c * SYS + 31 * NR, NR)]
        KXM[c] = roll(jnp.where(lo, kx_last, jnp.where(px == 1, jx[c], 0.0)), 64)
        KY[pl.ds(c * KSYS + 7, 32, stride=KR)] = jnp.where(py == 1, jy[c], 0.0)
        KF[c] = jnp.where(pz == 1, jz[c], skz[c])
        PB[pl.ds(c * PSYS + hrow, 32, stride=PR)] = iy[c]
        u_first = PB[pl.ds(c * PSYS + 8, NR)]
        u_last = PB[pl.ds(c * PSYS + 31 * PR + 8, NR)]
        PB[pl.ds(c * PSYS + 32 * PR + 8, NR)] = roll(jnp.where(lo, ix[c], u_first), 64)
        low = roll(jnp.where(lo, u_last, ix[c]), 64)
        kf, uf = KF[c], iz[c]
        mask = face_mask(NR)

        def start_plane(x, carry):
            acc, fx_prev, kx_prev, u = carry
            base = pl.multiple_of(c * PSYS + x * PR, 8)
            at = rows(x, c)
            kbase = pl.multiple_of(c * KSYS + x * KR, 8)
            nxt = PB[pl.ds(base + PR + 8, NR)]
            yu = PB[pl.ds(base + 9, NR)]
            yl = PB[pl.ds(base + 7, NR)]
            s = D[at]
            kxv = KX[at]
            kyv = KY[pl.ds(kbase + 8, NR)]
            kyl = KY[pl.ds(kbase + 7, NR)]
            kzf = jnp.where(mask, spread(kf, x, zf), KZ[at])
            uz = jnp.where(mask, spread(uf, x, zf), roll(u, to_z))
            fx = kxv * (u - nxt)
            fz = kzf * (u - uz)
            fz_away = roll(jnp.where(mask, 0.0, fz), fro_z)
            D[at] = s + (kxv + kx_prev) + (kyv + kyl) + (kzf + KZF[at])
            KZF[at] = kzf
            PZ[at] = uz
            r = R[at] - (s * u + (fx - fx_prev) + (kyv * (u - yu) - kyl * (yl - u)) + (fz - fz_away))
            R[at] = r
            return acc + fold(r * r), fx, kxv, nxt
        acc, _, _, _ = lax.fori_loop(0, NP, start_plane, (jnp.zeros((8, LN), F32), KXM[c] * (low - u_first), KXM[c], u_first), unroll=4)
        reduce_start(0, c, acc)
        z_face(R, c)
        for cp in r_copies(c):
            cp.start()

    hist_s[...] = jnp.zeros((8, LN), F32)
    for c in range(2):
        phx[c] = jnp.zeros((NR, LN), F32)
        phy[c] = zero32
        for cp in r_copies(c):
            cp.wait_send()

    def q_copies(c, par):
        return [
            remote(sz.at[c], qhz.at[par, c], qsend.at[c, 0], qrecv.at[par, c, 0], nbr['z']),
            remote(sy.at[c], qhy.at[par, c], qsend.at[c, 1], qrecv.at[par, c, 1], nbr['y']),
            remote(x_plane(Q, c), qhx.at[par, c], qsend.at[c, 2], qrecv.at[par, c, 2], nbr['x'])]

    def note(c, k, rho):
        hist_s[...] = jnp.where(jnp.logical_and(lane == k, row8 == c), rho, hist_s[...])

    def product(c, beta):
        b64 = wide(beta, NR)
        hx = rhx[c] + b64 * phx[c]
        hy = rhy[c] + wide(beta, 32) * phy[c]
        phx[c] = hx
        phy[c] = hy
        PB[pl.ds(c * PSYS + hrow, 32, stride=PR)] = hy
        lo = splits(NR)

        def direction(x):
            at = pl.ds(c * PSYS + x * PR + 8, NR)
            val = R[pl.ds(c * SYS + x * NR, NR)] + b64 * PB[at]
            PB[at] = val
            return val

        def turn(x, p):
            return roll(KZ[pl.ds(c * SYS + x * NR, NR)] * p, fro_z)

        def load_p(x):
            return PB[pl.ds(c * PSYS + x * PR + 8, NR)]

        p_last = direction(NP - 1)
        p_first = direction(0)
        above = roll(jnp.where(lo, hx, p_first), 64)
        below = roll(jnp.where(lo, p_last, hx), 64)
        turned = {0: turn(0, p_first)}
        for x in range(1, AHEAD):
            turned[x] = turn(x, direction(x))
        cur, kxp_prev = p_first, KXM[c] * below
        acc = jnp.zeros((8, LN), F32)
        for x in range(NP):
            w = x + AHEAD
            if w < NP:
                turned[w] = turn(w, direction(w) if w < NP - 1 else load_p(w))
            nxt = load_p(x + 1) if x + 1 < NP else above
            base = c * PSYS + x * PR
            at = pl.ds(c * SYS + x * NR, NR)
            kbase = c * KSYS + x * KR
            kxv = KX[at]
            kxp = kxv * cur
            q = D[at] * cur - kxp_prev - kxv * nxt
            q = q - KY[pl.ds(kbase + 8, NR)] * PB[pl.ds(base + 9, NR)]
            q = q - KY[pl.ds(kbase + 7, NR)] * PB[pl.ds(base + 7, NR)]
            pz_new = RZ[at] + b64 * PZ[at]
            PZ[at] = pz_new
            q = q - KZF[at] * pz_new - turned.pop(x)
            Q[at] = q
            acc = acc + fold(cur * q)
            cur, kxp_prev = nxt, kxp
        return acc

    outs = [pltpu.make_async_copy(X.at[pl.ds(c * SYS, SYS)], x_out.at[pl.ds(c * SYS, SYS)], out_sem.at[c]) for c in range(2)]

    def body(k, carry):
        par = k % 2
        for c in range(2):
            @pl.when(k == 0)
            def _():
                for cp in r_copies(c):
                    cp.wait_recv()
                turn_r(c)
            rho = reduce_end(0, c)
            note(c, k, rho)
            beta = jnp.where(k == 0, 0.0, rho / rho_s[c])
            rho_s[c] = rho
            reduce_start(1, c, product(c, beta))
            reduce_sent(0, c)
            z_face(Q, c)
            for cp in q_copies(c, par):
                cp.start()
        for c in range(2):
            alpha = rho_s[c] / reduce_end(1, c)
            alpha_s[c] = alpha
            a_ch = wide(alpha, NR)
            acc = jnp.zeros((8, LN), F32)
            for x in range(NP):
                at = pl.ds(c * SYS + x * NR, NR)
                r = R[at] - a_ch * Q[at]
                R[at] = r
                acc = acc + fold(r * r)
            reduce_start(0, c, acc)

            def step_x(x, carry):
                at = pl.ds(pl.multiple_of(c * SYS + x * NR, 8), NR)
                X[at] = X[at] + wide(alpha, NR) * PB[pl.ds(pl.multiple_of(c * PSYS + x * PR + 8, 8), NR)]
                return carry
            lax.fori_loop(0, NP, step_x, 0, unroll=4)

            @pl.when(k == ITERS - 1)
            def _():
                outs[c].start()
        for c in range(2):
            reduce_sent(1, c)
            for cp in q_copies(c, par):
                cp.wait()

            @pl.when(k < ITERS - 1)
            def _():
                alpha = alpha_s[c]
                rhx[c] = rhx[c] - wide(alpha, NR) * qhx[par, c]
                rhy[c] = rhy[c] - wide(alpha, 32) * qhy[par, c]
                rhz[c] = rhz[c] - wide(alpha, 32) * qhz[par, c]
                turn_r(c)
        return carry

    lax.fori_loop(0, ITERS, body, 0)
    for c in range(2):
        note(c, ITERS, reduce_end(0, c))
        reduce_sent(0, c)
    hist_out[...] = jnp.sqrt(hist_s[...] * (1.0 / (128 * 128 * 128)))
    for cp in outs:
        cp.wait()


CHUNKS = 2
VMEM_MAIN = 60 * 1024 * 1024


def unpack(xp, hist, x_out, hist_out, buf, st, hs, ho, in_sem, out_sem, h_sem):
    planes = NP // CHUNKS
    hist_in = pltpu.make_async_copy(hist, hs, h_sem.at[0])
    hist_in.start()
    loads = []
    for n in range(2 * CHUNKS):
        at = pl.ds(n * planes * NR, planes * NR)
        loads.append(pltpu.make_async_copy(xp.at[at], buf.at[at], in_sem.at[n]))
        loads[n].start()
    stores = []
    for n in range(2 * CHUNKS):
        c, x0 = n // CHUNKS, n % CHUNKS * planes
        loads[n].wait()

        def plane(x, carry):
            val = buf[pl.ds(pl.multiple_of(n * planes * NR + x * NR, 8), NR)]
            st[c, x0 + x] = val[:, :64]
            st[c, x0 + x + NP] = roll(val, 64)[:, :64]
            return carry
        lax.fori_loop(0, planes, plane, 0, unroll=16)
        for h in range(2):
            at = pl.ds(x0 + NP * h, planes)
            stores.append(pltpu.make_async_copy(st.at[c, at], x_out.at[c, at], out_sem.at[n, h]))
            stores[-1].start()
    hist_in.wait()
    ho[...] = hs[:2, :ITERS + 1]
    stores.append(pltpu.make_async_copy(ho, hist_out, h_sem.at[1]))
    stores[-1].start()
    for cp in stores:
        cp.wait()


def run(s, b, x0, kx, ky, kz):
    v = lambda *shape: pltpu.VMEM(shape, F32)
    sem = lambda *shape: pltpu.SemaphoreType.DMA(shape)
    scratch = [v(2, 64, 64, 64)] * 6
    full = v(2 * SYS, LN)
    scratch += [full, full, full, v(2 * PSYS, LN), full, full, full, v(2, NR, LN), v(2 * KSYS, LN), full, full, full, v(2, 32, LN)]
    scratch += [v(2, NR, LN), v(2, 32, LN), v(2, 32, LN)] * 2
    scratch += [v(2, 32, LN)] * 6
    scratch += [v(2, NR, LN), v(2, 32, LN), v(2, 32, LN), v(2, NR, LN), v(2, 32, LN)]
    scratch += [v(2, 2, NR, LN), v(2, 2, 32, LN), v(2, 2, 32, LN)]
    scratch += [v(2, 2, 8, 1, LN), v(2, 8, LN), v(2, 8, LN), v(8, LN)]
    scratch += [sem(6, 2), sem(2, 6), sem(2, 6), sem(2, 3), sem(2, 3), sem(2, 3), sem(2, 2, 3), sem(2, 2, 8), sem(2, 2, 8), sem(2)]
    xp, hist = pl.pallas_call(
        kernel,
        out_shape=(jax.ShapeDtypeStruct((2 * SYS, LN), F32), jax.ShapeDtypeStruct((8, LN), F32)),
        in_specs=[pl.BlockSpec(memory_space=pl.ANY)] * 6,
        out_specs=(pl.BlockSpec(memory_space=pl.ANY), pl.BlockSpec(memory_space=pltpu.VMEM)),
        scratch_shapes=scratch,
        compiler_params=pltpu.CompilerParams(collective_id=0, has_side_effects=True, vmem_limit_bytes=VMEM_MAIN),
        name='cg',
    )(s, b, x0, kx, ky, kz)
    return pl.pallas_call(
        unpack,
        out_shape=(jax.ShapeDtypeStruct((2, 64, 64, 64), F32), jax.ShapeDtypeStruct((2, ITERS + 1), F32)),
        in_specs=[pl.BlockSpec(memory_space=pl.ANY)] * 2,
        out_specs=[pl.BlockSpec(memory_space=pl.ANY)] * 2,
        scratch_shapes=[v(2 * SYS, LN), v(2, 64, 64, 64), v(8, LN), v(2, ITERS + 1), sem(2 * CHUNKS), sem(2 * CHUNKS, 2), sem(2)],
        compiler_params=pltpu.CompilerParams(vmem_limit_bytes=60 * 1024 * 1024),
        name='unpack',
    )(xp, hist)


def solution(mesh):
    field = P(None, 'px', 'py', 'pz')
    return jax.shard_map(run, mesh=mesh, in_specs=(field,) * 6, out_specs=(field, P(None, None)), check_vma=False)
```

```python
import jax
import jax.numpy as jnp
from jax import lax
from jax.experimental import pallas as pl
from jax.experimental.pallas import tpu as pltpu
from jax.sharding import PartitionSpec as P

ITERS = 20
F32 = jnp.float32
MESH = pl.DeviceIdType.MESH

NP = 32
NR = 64
LN = 128
PR = 80
KR = 72
SYS = NP * NR
PSYS = (NP + 1) * PR
KSYS = NP * KR
AHEAD = 3


def roll(val, shift):
    if isinstance(shift, int):
        shift = shift % LN
    return pltpu.roll(val, shift, 1)


def kernel(s_hbm, b_hbm, x0_hbm, kx_hbm, ky_hbm, kz_hbm, x_out, hist_out,
           st_s, st_b, st_x, st_kx, st_ky, st_kz,
           X, R, Q, PB, PZ, RZ, KX, KXM, KY, KZ, KZF, D, KF,
           ix, iy, iz, jx, jy, jz, sxy, sxz, sky, skz, sy, sz,
           rhx, rhy, rhz, phx, phy, qhx, qhy, qhz,
           red, rho_s, alpha_s, hist_s,
           ld_sem, isend, irecv, rsend, rrecv, qsend, qrecv, dsend, drecv, out_sem):
    pz, py, px = lax.axis_index('pz'), lax.axis_index('py'), lax.axis_index('px')
    nbr = {'x': (pz, py, 1 - px), 'y': (pz, 1 - py, px), 'z': (1 - pz, py, px)}
    others = {}
    for m in range(1, 8):
        others[m] = (1 - pz if m & 4 else pz, 1 - py if m & 2 else py, 1 - px if m & 1 else px)

    lane = lax.broadcasted_iota(jnp.int32, (8, LN), 1)
    row8 = lax.broadcasted_iota(jnp.int32, (8, LN), 0)

    def lanes(n):
        return lax.broadcasted_iota(jnp.int32, (n, LN), 1)

    zf = 63 * (1 - pz)
    xf = 31 * (1 - px)
    yf = 63 * (1 - py)
    hrow = 72 - 65 * py
    to_z = 127 - 126 * pz
    fro_z = 1 + 126 * pz

    def face_mask(n):
        return (lanes(n) % 64) == zf

    def splits(n):
        return lanes(n) < 64

    loads = []
    for num, (src, dst) in enumerate(((x0_hbm, st_x), (kz_hbm, st_kz), (kx_hbm, st_kx), (ky_hbm, st_ky), (s_hbm, st_s), (b_hbm, st_b))):
        pair = [pltpu.make_async_copy(src.at[c], dst.at[c], ld_sem.at[num, c]) for c in range(2)]
        loads.append(pair)
    for num in range(1):
        for cp in loads[num]:
            cp.start()

    barrier = pltpu.get_barrier_semaphore()
    for m in range(1, 8):
        pl.semaphore_signal(barrier, inc=1, device_id=others[m], device_id_type=MESH)

    def packed(st, c, x):
        return jnp.concatenate([st[c, x], st[c, x + NP]], axis=1)

    def pick(T, val, x, f):
        l64 = lanes(32) % 64
        T = jnp.where(l64 == x, roll(val[:32], lax.rem(x - f + LN, LN)), T)
        return jnp.where(l64 == x + 32, roll(val[32:], lax.rem(x + 32 - f + LN, LN)), T)

    def spread(G, x, f):
        return jnp.concatenate([roll(G, lax.rem(f - x + LN, LN)), roll(G, lax.rem(f - x - 32 + LN, LN))], axis=0)

    zero32 = jnp.zeros((32, LN), F32)

    def remote(src, dst, send_sem, recv_sem, dev):
        return pltpu.make_async_remote_copy(src_ref=src, dst_ref=dst, send_sem=send_sem, recv_sem=recv_sem, device_id=dev, device_id_type=MESH)

    def x_plane(ref, c):
        return ref.at[pl.ds(pl.multiple_of(c * SYS + xf * NR, 8), NR)]

    def rows(x, c):
        return pl.ds(pl.multiple_of(c * SYS + x * NR, 8), NR)

    first = []
    for c in range(2):
        first.append([
            remote(sxz.at[c], iz.at[c], isend.at[c, 0], irecv.at[c, 0], nbr['z']),
            remote(sxy.at[c], iy.at[c], isend.at[c, 1], irecv.at[c, 1], nbr['y']),
            remote(x_plane(X, c), ix.at[c], isend.at[c, 2], irecv.at[c, 2], nbr['x']),
            remote(skz.at[c], jz.at[c], isend.at[c, 3], irecv.at[c, 3], nbr['z']),
            remote(sky.at[c], jy.at[c], isend.at[c, 4], irecv.at[c, 4], nbr['y']),
            remote(KX.at[pl.ds(c * SYS + 31 * NR, NR)], jx.at[c], isend.at[c, 5], irecv.at[c, 5], nbr['x'])])

    for c in range(2):
        loads[0][c].wait()
        for num in ((1, 2), (3, 4, 5))[c]:
            for cp in loads[num]:
                cp.start()

        def pack_x(x, T):
            u = packed(st_x, c, x)
            X[rows(x, c)] = u
            base = pl.multiple_of(c * PSYS + x * PR, 8)
            PB[pl.ds(base, 8)] = jnp.zeros((8, LN), F32)
            PB[pl.ds(base + 72, 8)] = jnp.zeros((8, LN), F32)
            PB[pl.ds(base + 8, NR)] = u
            return pick(T, u, x, zf)
        sxz[c] = lax.fori_loop(0, NP, pack_x, zero32, unroll=8)
        sxy[c] = X[pl.ds(c * SYS + yf, 32, stride=NR)]
    pl.semaphore_wait(barrier, 7)
    for c in range(2):
        for cp in first[c][:3]:
            cp.start()
    for c in range(2):
        loads[1][c].wait()

        def pack_z(x, T):
            u = packed(st_kz, c, x)
            inner = jnp.where(lanes(NR) % 64 == 63, 0.0, u)
            moved = roll(inner, 1)
            KZ[rows(x, c)] = jnp.where(pz == 1, moved, inner)
            KZF[rows(x, c)] = jnp.where(pz == 1, inner, moved)
            return pick(T, u, x, 63)
        skz[c] = lax.fori_loop(0, NP, pack_z, zero32, unroll=8)
    for c in range(2):
        loads[2][c].wait()

        def pack_kx(x, carry):
            KX[rows(x, c)] = packed(st_kx, c, x)
            return carry
        lax.fori_loop(0, NP, pack_kx, 0, unroll=8)
        last = KX[pl.ds(c * SYS + 31 * NR, NR)]
        edge = jnp.logical_and(lanes(NR) >= 64, px == 1)
        KX[pl.ds(c * SYS + 31 * NR, NR)] = jnp.where(edge, 0.0, last)
        first[c][3].start()
    for c in range(2):
        loads[3][c].wait()

        def pack_ky(x, carry):
            u = packed(st_ky, c, x)
            row = lax.broadcasted_iota(jnp.int32, (NR, LN), 0)
            u = jnp.where(jnp.logical_and(row == NR - 1, py == 1), 0.0, u)
            KY[pl.ds(pl.multiple_of(c * KSYS + x * KR + 8, 8), NR)] = u
            return carry
        lax.fori_loop(0, NP, pack_ky, 0, unroll=8)
        sky[c] = KY[pl.ds(c * KSYS + 71, 32, stride=KR)]
        first[c][5].start()
    for c in range(2):
        loads[4][c].wait()
        loads[5][c].wait()
        if c == 0:
            for cp in (first[0][4], first[1][4]):
                cp.start()

        def pack_sb(x, carry):
            D[rows(x, c)] = packed(st_s, c, x)
            R[rows(x, c)] = packed(st_b, c, x)
            return carry
        lax.fori_loop(0, NP, pack_sb, 0, unroll=8)

    def reduce_copies(kind, c):
        return [remote(red.at[kind, c, 0], red.at[kind, c, m], dsend.at[kind, c, m], drecv.at[kind, c, m], others[m]) for m in (7, 6, 5, 4, 3, 2, 1)]

    def reduce_start(kind, c, part):
        red[kind, c, 0] = jnp.sum(part, axis=0, keepdims=True)
        for cp in reduce_copies(kind, c):
            cp.start()

    def reduce_end(kind, c):
        for cp in reduce_copies(kind, c):
            cp.wait_recv()
        v = [red[kind, c, m] for m in range(8)]
        total = ((v[0] + v[1]) + (v[2] + v[3])) + ((v[4] + v[5]) + (v[6] + v[7]))
        total = jnp.broadcast_to(total, (8, LN))
        return jnp.broadcast_to(jnp.sum(total, axis=1, keepdims=True), (8, LN))

    def reduce_sent(kind, c):
        for cp in reduce_copies(kind, c):
            cp.wait_send()

    def fold(val):
        return jnp.sum(val.reshape(-1, 8, LN), axis=0)

    def wide(vec, n):
        return jnp.broadcast_to(vec[None], (n // 8, 8, LN)).reshape(n, LN)

    def z_face(ref, c):
        def plane(x, T):
            return pick(T, ref[rows(x, c)], x, zf)
        sz[c] = lax.fori_loop(0, NP, plane, zero32, unroll=8)
        sy[c] = ref[pl.ds(c * SYS + yf, 32, stride=NR)]

    def turn_r(c):
        G = rhz[c]
        mask = face_mask(NR)

        def plane(x, carry):
            RZ[rows(x, c)] = jnp.where(mask, spread(G, x, zf), roll(R[rows(x, c)], to_z))
            return carry
        lax.fori_loop(0, NP, plane, 0, unroll=8)

    def r_copies(c):
        return [
            remote(sz.at[c], rhz.at[c], rsend.at[c, 0], rrecv.at[c, 0], nbr['z']),
            remote(sy.at[c], rhy.at[c], rsend.at[c, 1], rrecv.at[c, 1], nbr['y']),
            remote(x_plane(R, c), rhx.at[c], rsend.at[c, 2], rrecv.at[c, 2], nbr['x'])]

    for c in range(2):
        for cp in first[c]:
            cp.wait()
        lo = splits(NR)
        kx_last = KX[pl.ds(c * SYS + 31 * NR, NR)]
        KXM[c] = roll(jnp.where(lo, kx_last, jnp.where(px == 1, jx[c], 0.0)), 64)
        KY[pl.ds(c * KSYS + 7, 32, stride=KR)] = jnp.where(py == 1, jy[c], 0.0)
        KF[c] = jnp.where(pz == 1, jz[c], skz[c])
        PB[pl.ds(c * PSYS + hrow, 32, stride=PR)] = iy[c]
        u_first = PB[pl.ds(c * PSYS + 8, NR)]
        u_last = PB[pl.ds(c * PSYS + 31 * PR + 8, NR)]
        PB[pl.ds(c * PSYS + 32 * PR + 8, NR)] = roll(jnp.where(lo, ix[c], u_first), 64)
        low = roll(jnp.where(lo, u_last, ix[c]), 64)
        kf, uf = KF[c], iz[c]
        mask = face_mask(NR)

        def start_plane(x, carry):
            acc, fx_prev, kx_prev, u = carry
            base = pl.multiple_of(c * PSYS + x * PR, 8)
            at = rows(x, c)
            kbase = pl.multiple_of(c * KSYS + x * KR, 8)
            nxt = PB[pl.ds(base + PR + 8, NR)]
            yu = PB[pl.ds(base + 9, NR)]
            yl = PB[pl.ds(base + 7, NR)]
            s = D[at]
            kxv = KX[at]
            kyv = KY[pl.ds(kbase + 8, NR)]
            kyl = KY[pl.ds(kbase + 7, NR)]
            kzf = jnp.where(mask, spread(kf, x, zf), KZ[at])
            uz = jnp.where(mask, spread(uf, x, zf), roll(u, to_z))
            fx = kxv * (u - nxt)
            fz = kzf * (u - uz)
            fz_away = roll(jnp.where(mask, 0.0, fz), fro_z)
            D[at] = s + (kxv + kx_prev) + (kyv + kyl) + (kzf + KZF[at])
            KZF[at] = kzf
            PZ[at] = uz
            r = R[at] - (s * u + (fx - fx_prev) + (kyv * (u - yu) - kyl * (yl - u)) + (fz - fz_away))
            R[at] = r
            return acc + fold(r * r), fx, kxv, nxt
        acc, _, _, _ = lax.fori_loop(0, NP, start_plane, (jnp.zeros((8, LN), F32), KXM[c] * (low - u_first), KXM[c], u_first), unroll=4)
        reduce_start(0, c, acc)
        z_face(R, c)
        for cp in r_copies(c):
            cp.start()

    hist_s[...] = jnp.zeros((8, LN), F32)
    for c in range(2):
        phx[c] = jnp.zeros((NR, LN), F32)
        phy[c] = zero32
        for cp in r_copies(c):
            cp.wait_send()
    for cp in r_copies(0):
        cp.wait_recv()
    turn_r(0)

    def q_copies(c, par):
        return [
            remote(sz.at[c], qhz.at[par, c], qsend.at[c, 0], qrecv.at[par, c, 0], nbr['z']),
            remote(sy.at[c], qhy.at[par, c], qsend.at[c, 1], qrecv.at[par, c, 1], nbr['y']),
            remote(x_plane(Q, c), qhx.at[par, c], qsend.at[c, 2], qrecv.at[par, c, 2], nbr['x'])]

    def note(c, k, rho):
        hist_s[...] = jnp.where(jnp.logical_and(lane == k, row8 == c), rho, hist_s[...])

    def product(c, beta):
        b64 = wide(beta, NR)
        hx = rhx[c] + b64 * phx[c]
        hy = rhy[c] + wide(beta, 32) * phy[c]
        phx[c] = hx
        phy[c] = hy
        PB[pl.ds(c * PSYS + hrow, 32, stride=PR)] = hy
        lo = splits(NR)

        def direction(x):
            at = pl.ds(c * PSYS + x * PR + 8, NR)
            val = R[pl.ds(c * SYS + x * NR, NR)] + b64 * PB[at]
            PB[at] = val
            return val

        def turn(x, p):
            return roll(KZ[pl.ds(c * SYS + x * NR, NR)] * p, fro_z)

        def load_p(x):
            return PB[pl.ds(c * PSYS + x * PR + 8, NR)]

        p_last = direction(NP - 1)
        p_first = direction(0)
        above = roll(jnp.where(lo, hx, p_first), 64)
        below = roll(jnp.where(lo, p_last, hx), 64)
        turned = {0: turn(0, p_first)}
        for x in range(1, AHEAD):
            turned[x] = turn(x, direction(x))
        cur, kxp_prev = p_first, KXM[c] * below
        acc = jnp.zeros((8, LN), F32)
        for x in range(NP):
            w = x + AHEAD
            if w < NP:
                turned[w] = turn(w, direction(w) if w < NP - 1 else load_p(w))
            nxt = load_p(x + 1) if x + 1 < NP else above
            base = c * PSYS + x * PR
            at = pl.ds(c * SYS + x * NR, NR)
            kbase = c * KSYS + x * KR
            kxv = KX[at]
            kxp = kxv * cur
            q = D[at] * cur - kxp_prev - kxv * nxt
            q = q - KY[pl.ds(kbase + 8, NR)] * PB[pl.ds(base + 9, NR)]
            q = q - KY[pl.ds(kbase + 7, NR)] * PB[pl.ds(base + 7, NR)]
            pz_new = RZ[at] + b64 * PZ[at]
            PZ[at] = pz_new
            q = q - KZF[at] * pz_new - turned.pop(x)
            Q[at] = q
            acc = acc + fold(cur * q)
            cur, kxp_prev = nxt, kxp
        return acc

    outs = [pltpu.make_async_copy(X.at[pl.ds(c * SYS, SYS)], x_out.at[pl.ds(c * SYS, SYS)], out_sem.at[c]) for c in range(2)]

    def halo_r(c, par):
        for cp in q_copies(c, par):
            cp.wait_recv()
        alpha = alpha_s[c]
        rhx[c] = rhx[c] - wide(alpha, NR) * qhx[par, c]
        rhy[c] = rhy[c] - wide(alpha, 32) * qhy[par, c]
        rhz[c] = rhz[c] - wide(alpha, 32) * qhz[par, c]

    def q_sent(c, par):
        for cp in q_copies(c, par):
            cp.wait_send()

    def first_half(c, k, par):
        rho = reduce_end(0, c)
        note(c, k, rho)
        beta = jnp.where(k == 0, 0.0, rho / rho_s[c])
        rho_s[c] = rho
        reduce_start(1, c, product(c, beta))
        reduce_sent(0, c)
        z_face(Q, c)
        for cp in q_copies(c, par):
            cp.start()

    def second_half(c, k):
        alpha = rho_s[c] / reduce_end(1, c)
        alpha_s[c] = alpha
        a_pl = wide(alpha, NR)
        acc = jnp.zeros((8, LN), F32)
        for x in range(NP):
            at = pl.ds(c * SYS + x * NR, NR)
            r = R[at] - a_pl * Q[at]
            R[at] = r
            acc = acc + fold(r * r)
        reduce_start(0, c, acc)

        def step_x(x, carry):
            X[rows(x, c)] = X[rows(x, c)] + a_pl * PB[pl.ds(pl.multiple_of(c * PSYS + x * PR + 8, 8), NR)]
            return carry
        lax.fori_loop(0, NP, step_x, 0, unroll=4)

        @pl.when(k == ITERS - 1)
        def _():
            outs[c].start()
        reduce_sent(1, c)

    def body(k, carry):
        par = k % 2
        first_half(0, k, par)

        @pl.when(k == 0)
        def _():
            for cp in r_copies(1):
                cp.wait_recv()

        @pl.when(k > 0)
        def _():
            halo_r(1, 1 - par)
            q_sent(1, 1 - par)
        turn_r(1)
        first_half(1, k, par)
        second_half(0, k)
        halo_r(0, par)
        turn_r(0)
        second_half(1, k)
        q_sent(0, par)
        return carry

    lax.fori_loop(0, ITERS, body, 0)
    for c in range(2):
        note(c, ITERS, reduce_end(0, c))
        reduce_sent(0, c)
    for cp in q_copies(1, (ITERS - 1) % 2):
        cp.wait()
    hist_out[...] = jnp.sqrt(hist_s[...] * (1.0 / (128 * 128 * 128)))
    for cp in outs:
        cp.wait()


CHUNKS = 2
VMEM_MAIN = 60 * 1024 * 1024


def unpack(xp, hist, x_out, hist_out, buf, st, hs, ho, in_sem, out_sem, h_sem):
    planes = NP // CHUNKS
    hist_in = pltpu.make_async_copy(hist, hs, h_sem.at[0])
    hist_in.start()
    loads = []
    for n in range(2 * CHUNKS):
        at = pl.ds(n * planes * NR, planes * NR)
        loads.append(pltpu.make_async_copy(xp.at[at], buf.at[at], in_sem.at[n]))
        loads[n].start()
    stores = []
    for n in range(2 * CHUNKS):
        c, x0 = n // CHUNKS, n % CHUNKS * planes
        loads[n].wait()

        def plane(x, carry):
            val = buf[pl.ds(pl.multiple_of(n * planes * NR + x * NR, 8), NR)]
            st[c, x0 + x] = val[:, :64]
            st[c, x0 + x + NP] = roll(val, 64)[:, :64]
            return carry
        lax.fori_loop(0, planes, plane, 0, unroll=16)
        for h in range(2):
            at = pl.ds(x0 + NP * h, planes)
            stores.append(pltpu.make_async_copy(st.at[c, at], x_out.at[c, at], out_sem.at[n, h]))
            stores[-1].start()
    hist_in.wait()
    ho[...] = hs[:2, :ITERS + 1]
    stores.append(pltpu.make_async_copy(ho, hist_out, h_sem.at[1]))
    stores[-1].start()
    for cp in stores:
        cp.wait()


def run(s, b, x0, kx, ky, kz):
    v = lambda *shape: pltpu.VMEM(shape, F32)
    sem = lambda *shape: pltpu.SemaphoreType.DMA(shape)
    scratch = [v(2, 64, 64, 64)] * 6
    full = v(2 * SYS, LN)
    scratch += [full, full, full, v(2 * PSYS, LN), full, full, full, v(2, NR, LN), v(2 * KSYS, LN), full, full, full, v(2, 32, LN)]
    scratch += [v(2, NR, LN), v(2, 32, LN), v(2, 32, LN)] * 2
    scratch += [v(2, 32, LN)] * 6
    scratch += [v(2, NR, LN), v(2, 32, LN), v(2, 32, LN), v(2, NR, LN), v(2, 32, LN)]
    scratch += [v(2, 2, NR, LN), v(2, 2, 32, LN), v(2, 2, 32, LN)]
    scratch += [v(2, 2, 8, 1, LN), v(2, 8, LN), v(2, 8, LN), v(8, LN)]
    scratch += [sem(6, 2), sem(2, 6), sem(2, 6), sem(2, 3), sem(2, 3), sem(2, 3), sem(2, 2, 3), sem(2, 2, 8), sem(2, 2, 8), sem(2)]
    xp, hist = pl.pallas_call(
        kernel,
        out_shape=(jax.ShapeDtypeStruct((2 * SYS, LN), F32), jax.ShapeDtypeStruct((8, LN), F32)),
        in_specs=[pl.BlockSpec(memory_space=pl.ANY)] * 6,
        out_specs=(pl.BlockSpec(memory_space=pl.ANY), pl.BlockSpec(memory_space=pltpu.VMEM)),
        scratch_shapes=scratch,
        compiler_params=pltpu.CompilerParams(collective_id=0, has_side_effects=True, vmem_limit_bytes=VMEM_MAIN),
        name='cg',
    )(s, b, x0, kx, ky, kz)
    return pl.pallas_call(
        unpack,
        out_shape=(jax.ShapeDtypeStruct((2, 64, 64, 64), F32), jax.ShapeDtypeStruct((2, ITERS + 1), F32)),
        in_specs=[pl.BlockSpec(memory_space=pl.ANY)] * 2,
        out_specs=[pl.BlockSpec(memory_space=pl.ANY)] * 2,
        scratch_shapes=[v(2 * SYS, LN), v(2, 64, 64, 64), v(8, LN), v(2, ITERS + 1), sem(2 * CHUNKS), sem(2 * CHUNKS, 2), sem(2)],
        compiler_params=pltpu.CompilerParams(vmem_limit_bytes=60 * 1024 * 1024),
        name='unpack',
    )(xp, hist)


def solution(mesh):
    field = P(None, 'px', 'py', 'pz')
    return jax.shard_map(run, mesh=mesh, in_specs=(field,) * 6, out_specs=(field, P(None, None)), check_vma=False)
```

```python
import jax
import jax.numpy as jnp
from jax import lax
from jax.experimental import pallas as pl
from jax.experimental.pallas import tpu as pltpu
from jax.sharding import PartitionSpec as P

ITERS = 20
F32 = jnp.float32
MESH = pl.DeviceIdType.MESH

NP = 32
NR = 64
LN = 128
PR = 80
KR = 72
SYS = NP * NR
PSYS = (NP + 1) * PR
KSYS = NP * KR
IN_FLIGHT = 3
AHEAD = 3


def roll(val, shift):
    if isinstance(shift, int):
        shift = shift % LN
    return pltpu.roll(val, shift, 1)


def kernel(s_hbm, b_hbm, x0_hbm, kx_hbm, ky_hbm, kz_hbm, x_out, hist_out,
           st_s, st_b, st_x, st_kx, st_ky, st_kz,
           X, R, Q, PB, PZ, RZ, KX, KXM, KY, KZ, KZF, D, KF,
           ix, iy, iz, jx, jy, jz, sxy, sxz, sky, skz, sy, sz, sry, srz,
           rhx, rhy, rhz, phx, phy, qhx, qhy, qhz,
           red, rho_s, alpha_s, hist_s,
           ld_sem, isend, irecv, rsend, rrecv, qsend, qrecv, dsend, drecv, out_sem):
    pz, py, px = lax.axis_index('pz'), lax.axis_index('py'), lax.axis_index('px')
    nbr = {'x': (pz, py, 1 - px), 'y': (pz, 1 - py, px), 'z': (1 - pz, py, px)}
    others = {}
    for m in range(1, 8):
        others[m] = (1 - pz if m & 4 else pz, 1 - py if m & 2 else py, 1 - px if m & 1 else px)

    lane = lax.broadcasted_iota(jnp.int32, (8, LN), 1)
    row8 = lax.broadcasted_iota(jnp.int32, (8, LN), 0)

    def lanes(n):
        return lax.broadcasted_iota(jnp.int32, (n, LN), 1)

    zf = 63 * (1 - pz)
    xf = 31 * (1 - px)
    yf = 63 * (1 - py)
    hrow = 72 - 65 * py
    to_z = 127 - 126 * pz
    fro_z = 1 + 126 * pz

    def face_mask(n):
        return (lanes(n) % 64) == zf

    def splits(n):
        return lanes(n) < 64

    order = [(num, c) for c in range(2) for num in range(6)]
    pairs = ((x0_hbm, st_x), (kz_hbm, st_kz), (ky_hbm, st_ky), (kx_hbm, st_kx), (s_hbm, st_s), (b_hbm, st_b))
    loads = [pltpu.make_async_copy(pairs[num][0].at[c], pairs[num][1].at[c], ld_sem.at[num, c]) for num, c in order]
    for cp in loads[:IN_FLIGHT]:
        cp.start()

    def loaded(num, c):
        n = c * 6 + num
        loads[n].wait()
        if n + IN_FLIGHT < len(loads):
            loads[n + IN_FLIGHT].start()

    barrier = pltpu.get_barrier_semaphore()
    for m in range(1, 8):
        pl.semaphore_signal(barrier, inc=1, device_id=others[m], device_id_type=MESH)

    def packed(st, c, x):
        return jnp.concatenate([st[c, x], st[c, x + NP]], axis=1)

    def pick(T, val, x, f):
        l64 = lanes(32) % 64
        T = jnp.where(l64 == x, roll(val[:32], lax.rem(x - f + LN, LN)), T)
        return jnp.where(l64 == x + 32, roll(val[32:], lax.rem(x + 32 - f + LN, LN)), T)

    def spread(G, x, f):
        return jnp.concatenate([roll(G, lax.rem(f - x + LN, LN)), roll(G, lax.rem(f - x - 32 + LN, LN))], axis=0)

    zero32 = jnp.zeros((32, LN), F32)

    def remote(src, dst, send_sem, recv_sem, dev):
        return pltpu.make_async_remote_copy(src_ref=src, dst_ref=dst, send_sem=send_sem, recv_sem=recv_sem, device_id=dev, device_id_type=MESH)

    def x_plane(ref, c):
        return ref.at[pl.ds(pl.multiple_of(c * SYS + xf * NR, 8), NR)]

    def rows(x, c):
        return pl.ds(pl.multiple_of(c * SYS + x * NR, 8), NR)

    first = []
    for c in range(2):
        first.append([
            remote(sxz.at[c], iz.at[c], isend.at[c, 0], irecv.at[c, 0], nbr['z']),
            remote(sxy.at[c], iy.at[c], isend.at[c, 1], irecv.at[c, 1], nbr['y']),
            remote(x_plane(X, c), ix.at[c], isend.at[c, 2], irecv.at[c, 2], nbr['x']),
            remote(skz.at[c], jz.at[c], isend.at[c, 3], irecv.at[c, 3], nbr['z']),
            remote(sky.at[c], jy.at[c], isend.at[c, 4], irecv.at[c, 4], nbr['y']),
            remote(KX.at[pl.ds(c * SYS + 31 * NR, NR)], jx.at[c], isend.at[c, 5], irecv.at[c, 5], nbr['x'])])

    def prepare_x0(c):
        loaded(0, c)

        def pack_x(x, T):
            u = packed(st_x, c, x)
            X[rows(x, c)] = u
            base = pl.multiple_of(c * PSYS + x * PR, 8)
            PB[pl.ds(base, 8)] = jnp.zeros((8, LN), F32)
            PB[pl.ds(base + 72, 8)] = jnp.zeros((8, LN), F32)
            PB[pl.ds(base + 8, NR)] = u
            return pick(T, u, x, zf)
        sxz[c] = lax.fori_loop(0, NP, pack_x, zero32, unroll=8)
        sxy[c] = X[pl.ds(c * SYS + yf, 32, stride=NR)]

    def prepare_kz(c):
        loaded(1, c)

        def pack_z(x, T):
            u = packed(st_kz, c, x)
            inner = jnp.where(lanes(NR) % 64 == 63, 0.0, u)
            moved = roll(inner, 1)
            KZ[rows(x, c)] = jnp.where(pz == 1, moved, inner)
            KZF[rows(x, c)] = jnp.where(pz == 1, inner, moved)
            return pick(T, u, x, 63)
        skz[c] = lax.fori_loop(0, NP, pack_z, zero32, unroll=8)

    def prepare_ky(c):
        loaded(2, c)

        def pack_ky(x, carry):
            u = packed(st_ky, c, x)
            row = lax.broadcasted_iota(jnp.int32, (NR, LN), 0)
            u = jnp.where(jnp.logical_and(row == NR - 1, py == 1), 0.0, u)
            KY[pl.ds(pl.multiple_of(c * KSYS + x * KR + 8, 8), NR)] = u
            return carry
        lax.fori_loop(0, NP, pack_ky, 0, unroll=8)
        sky[c] = KY[pl.ds(c * KSYS + 71, 32, stride=KR)]

    def prepare_kx(c):
        loaded(3, c)

        def pack_kx(x, carry):
            KX[rows(x, c)] = packed(st_kx, c, x)
            return carry
        lax.fori_loop(0, NP, pack_kx, 0, unroll=8)
        last = KX[pl.ds(c * SYS + 31 * NR, NR)]
        edge = jnp.logical_and(lanes(NR) >= 64, px == 1)
        KX[pl.ds(c * SYS + 31 * NR, NR)] = jnp.where(edge, 0.0, last)

    def prepare_sb(c):
        loaded(4, c)
        loaded(5, c)

        def pack_sb(x, carry):
            D[rows(x, c)] = packed(st_s, c, x)
            R[rows(x, c)] = packed(st_b, c, x)
            return carry
        lax.fori_loop(0, NP, pack_sb, 0, unroll=8)

    prepare_x0(0)
    pl.semaphore_wait(barrier, 7)
    for cp in first[0][:3]:
        cp.start()
    prepare_kz(0)
    first[0][3].start()
    prepare_ky(0)
    first[0][4].start()
    prepare_kx(0)
    first[0][5].start()
    prepare_sb(0)
    prepare_x0(1)
    for cp in first[1][:3]:
        cp.start()
    prepare_kz(1)
    first[1][3].start()
    prepare_ky(1)
    first[1][4].start()

    def reduce_copies(kind, c):
        return [remote(red.at[kind, c, 0], red.at[kind, c, m], dsend.at[kind, c, m], drecv.at[kind, c, m], others[m]) for m in (7, 6, 5, 4, 3, 2, 1)]

    def reduce_start(kind, c, part):
        red[kind, c, 0] = jnp.sum(part, axis=0, keepdims=True)
        for cp in reduce_copies(kind, c):
            cp.start()

    def reduce_end(kind, c):
        for cp in reduce_copies(kind, c):
            cp.wait_recv()
        v = [red[kind, c, m] for m in range(8)]
        total = ((v[0] + v[1]) + (v[2] + v[3])) + ((v[4] + v[5]) + (v[6] + v[7]))
        total = jnp.broadcast_to(total, (8, LN))
        return jnp.broadcast_to(jnp.sum(total, axis=1, keepdims=True), (8, LN))

    def reduce_sent(kind, c):
        for cp in reduce_copies(kind, c):
            cp.wait_send()

    def fold(val):
        return jnp.sum(val.reshape(-1, 8, LN), axis=0)

    def wide(vec, n):
        return jnp.broadcast_to(vec[None], (n // 8, 8, LN)).reshape(n, LN)

    def z_face(ref, c, to_sz, to_sy):
        def plane(x, T):
            return pick(T, ref[rows(x, c)], x, zf)
        to_sz[c] = lax.fori_loop(0, NP, plane, zero32, unroll=8)
        to_sy[c] = ref[pl.ds(c * SYS + yf, 32, stride=NR)]

    def turn_r(c):
        G = rhz[c]
        mask = face_mask(NR)

        def plane(x, carry):
            RZ[rows(x, c)] = jnp.where(mask, spread(G, x, zf), roll(R[rows(x, c)], to_z))
            return carry
        lax.fori_loop(0, NP, plane, 0, unroll=8)

    def r_copies(c):
        return [
            remote(srz.at[c], rhz.at[c], rsend.at[c, 0], rrecv.at[c, 0], nbr['z']),
            remote(sry.at[c], rhy.at[c], rsend.at[c, 1], rrecv.at[c, 1], nbr['y']),
            remote(x_plane(R, c), rhx.at[c], rsend.at[c, 2], rrecv.at[c, 2], nbr['x'])]

    def start(c):
        for cp in first[c]:
            cp.wait_recv()
        lo = splits(NR)
        kx_last = KX[pl.ds(c * SYS + 31 * NR, NR)]
        KXM[c] = roll(jnp.where(lo, kx_last, jnp.where(px == 1, jx[c], 0.0)), 64)
        KY[pl.ds(c * KSYS + 7, 32, stride=KR)] = jnp.where(py == 1, jy[c], 0.0)
        KF[c] = jnp.where(pz == 1, jz[c], skz[c])
        PB[pl.ds(c * PSYS + hrow, 32, stride=PR)] = iy[c]
        u_first = PB[pl.ds(c * PSYS + 8, NR)]
        u_last = PB[pl.ds(c * PSYS + 31 * PR + 8, NR)]
        PB[pl.ds(c * PSYS + 32 * PR + 8, NR)] = roll(jnp.where(lo, ix[c], u_first), 64)
        low = roll(jnp.where(lo, u_last, ix[c]), 64)
        kf, uf = KF[c], iz[c]
        mask = face_mask(NR)

        def start_plane(x, carry):
            acc, fx_prev, kx_prev, u = carry
            base = pl.multiple_of(c * PSYS + x * PR, 8)
            at = rows(x, c)
            kbase = pl.multiple_of(c * KSYS + x * KR, 8)
            nxt = PB[pl.ds(base + PR + 8, NR)]
            yu = PB[pl.ds(base + 9, NR)]
            yl = PB[pl.ds(base + 7, NR)]
            s = D[at]
            kxv = KX[at]
            kyv = KY[pl.ds(kbase + 8, NR)]
            kyl = KY[pl.ds(kbase + 7, NR)]
            kzf = jnp.where(mask, spread(kf, x, zf), KZ[at])
            uz = jnp.where(mask, spread(uf, x, zf), roll(u, to_z))
            fx = kxv * (u - nxt)
            fz = kzf * (u - uz)
            fz_away = roll(jnp.where(mask, 0.0, fz), fro_z)
            D[at] = s + (kxv + kx_prev) + (kyv + kyl) + (kzf + KZF[at])
            KZF[at] = kzf
            PZ[at] = uz
            r = R[at] - (s * u + (fx - fx_prev) + (kyv * (u - yu) - kyl * (yl - u)) + (fz - fz_away))
            R[at] = r
            return acc + fold(r * r), fx, kxv, nxt
        init = (jnp.zeros((8, LN), F32), KXM[c] * (low - u_first), KXM[c], u_first)
        acc = lax.fori_loop(0, NP, start_plane, init, unroll=4)[0]
        reduce_start(0, c, acc)
        z_face(R, c, srz, sry)
        for cp in r_copies(c):
            cp.start()

    start(0)
    prepare_kx(1)
    first[1][5].start()
    prepare_sb(1)
    start(1)
    hist_s[...] = jnp.zeros((8, LN), F32)
    for c in range(2):
        phx[c] = jnp.zeros((NR, LN), F32)
        phy[c] = zero32
        for cp in first[c]:
            cp.wait_send()
    for cp in r_copies(0):
        cp.wait_recv()
    turn_r(0)

    def q_copies(c, par):
        return [
            remote(sz.at[c], qhz.at[par, c], qsend.at[c, 0], qrecv.at[par, c, 0], nbr['z']),
            remote(sy.at[c], qhy.at[par, c], qsend.at[c, 1], qrecv.at[par, c, 1], nbr['y']),
            remote(x_plane(Q, c), qhx.at[par, c], qsend.at[c, 2], qrecv.at[par, c, 2], nbr['x'])]

    def note(c, k, rho):
        hist_s[...] = jnp.where(jnp.logical_and(lane == k, row8 == c), rho, hist_s[...])

    def product(c, beta):
        b64 = wide(beta, NR)
        hx = rhx[c] + b64 * phx[c]
        hy = rhy[c] + wide(beta, 32) * phy[c]
        phx[c] = hx
        phy[c] = hy
        PB[pl.ds(c * PSYS + hrow, 32, stride=PR)] = hy
        lo = splits(NR)

        def direction(x):
            at = pl.ds(c * PSYS + x * PR + 8, NR)
            val = R[pl.ds(c * SYS + x * NR, NR)] + b64 * PB[at]
            PB[at] = val
            return val

        def turn(x, p):
            return roll(KZ[pl.ds(c * SYS + x * NR, NR)] * p, fro_z)

        def load_p(x):
            return PB[pl.ds(c * PSYS + x * PR + 8, NR)]

        p_last = direction(NP - 1)
        p_first = direction(0)
        above = roll(jnp.where(lo, hx, p_first), 64)
        below = roll(jnp.where(lo, p_last, hx), 64)
        turned = {0: turn(0, p_first)}
        for x in range(1, AHEAD):
            turned[x] = turn(x, direction(x))
        cur, kxp_prev = p_first, KXM[c] * below
        acc = jnp.zeros((8, LN), F32)
        for x in range(NP):
            w = x + AHEAD
            if w < NP:
                turned[w] = turn(w, direction(w) if w < NP - 1 else load_p(w))
            nxt = load_p(x + 1) if x + 1 < NP else above
            base = c * PSYS + x * PR
            at = pl.ds(c * SYS + x * NR, NR)
            kbase = c * KSYS + x * KR
            kxv = KX[at]
            kxp = kxv * cur
            q = D[at] * cur - kxp_prev - kxv * nxt
            q = q - KY[pl.ds(kbase + 8, NR)] * PB[pl.ds(base + 9, NR)]
            q = q - KY[pl.ds(kbase + 7, NR)] * PB[pl.ds(base + 7, NR)]
            pz_new = RZ[at] + b64 * PZ[at]
            PZ[at] = pz_new
            q = q - KZF[at] * pz_new - turned.pop(x)
            Q[at] = q
            acc = acc + fold(cur * q)
            cur, kxp_prev = nxt, kxp
        return acc

    outs = [pltpu.make_async_copy(X.at[pl.ds(c * SYS, SYS)], x_out.at[pl.ds(c * SYS, SYS)], out_sem.at[c]) for c in range(2)]

    def halo_r(c, par):
        for cp in q_copies(c, par):
            cp.wait_recv()
        alpha = alpha_s[c]
        rhx[c] = rhx[c] - wide(alpha, NR) * qhx[par, c]
        rhy[c] = rhy[c] - wide(alpha, 32) * qhy[par, c]
        rhz[c] = rhz[c] - wide(alpha, 32) * qhz[par, c]

    def q_sent(c, par):
        for cp in q_copies(c, par):
            cp.wait_send()

    def first_half(c, k, par):
        rho = reduce_end(0, c)
        note(c, k, rho)
        beta = jnp.where(k == 0, 0.0, rho / rho_s[c])
        rho_s[c] = rho
        reduce_start(1, c, product(c, beta))
        reduce_sent(0, c)
        z_face(Q, c, sz, sy)
        for cp in q_copies(c, par):
            cp.start()

    def second_half(c, k):
        alpha = rho_s[c] / reduce_end(1, c)
        alpha_s[c] = alpha
        a_pl = wide(alpha, NR)
        acc = jnp.zeros((8, LN), F32)
        for x in range(NP):
            at = pl.ds(c * SYS + x * NR, NR)
            r = R[at] - a_pl * Q[at]
            R[at] = r
            acc = acc + fold(r * r)
        reduce_start(0, c, acc)

        def step_x(x, carry):
            X[rows(x, c)] = X[rows(x, c)] + a_pl * PB[pl.ds(pl.multiple_of(c * PSYS + x * PR + 8, 8), NR)]
            return carry
        lax.fori_loop(0, NP, step_x, 0, unroll=4)

        @pl.when(k == ITERS - 1)
        def _():
            outs[c].start()
        reduce_sent(1, c)

    def body(k, carry):
        par = k % 2
        first_half(0, k, par)

        @pl.when(k == 0)
        def _():
            for cp in r_copies(1):
                cp.wait_recv()

        @pl.when(k > 0)
        def _():
            halo_r(1, 1 - par)
            q_sent(1, 1 - par)
        turn_r(1)
        first_half(1, k, par)

        @pl.when(k == 0)
        def _():
            for c in range(2):
                for cp in r_copies(c):
                    cp.wait_send()
        second_half(0, k)
        halo_r(0, par)
        turn_r(0)
        second_half(1, k)
        q_sent(0, par)
        return carry

    lax.fori_loop(0, ITERS, body, 0)
    for c in range(2):
        note(c, ITERS, reduce_end(0, c))
        reduce_sent(0, c)
    for cp in q_copies(1, (ITERS - 1) % 2):
        cp.wait()
    hist_out[...] = jnp.sqrt(hist_s[...] * (1.0 / (128 * 128 * 128)))
    for cp in outs:
        cp.wait()


CHUNKS = 2
VMEM_MAIN = 60 * 1024 * 1024


def unpack(xp, hist, x_out, hist_out, buf, st, hs, ho, in_sem, out_sem, h_sem):
    planes = NP // CHUNKS
    hist_in = pltpu.make_async_copy(hist, hs, h_sem.at[0])
    hist_in.start()
    loads = []
    for n in range(2 * CHUNKS):
        at = pl.ds(n * planes * NR, planes * NR)
        loads.append(pltpu.make_async_copy(xp.at[at], buf.at[at], in_sem.at[n]))
        loads[n].start()
    stores = []
    for n in range(2 * CHUNKS):
        c, x0 = n // CHUNKS, n % CHUNKS * planes
        loads[n].wait()

        def plane(x, carry):
            val = buf[pl.ds(pl.multiple_of(n * planes * NR + x * NR, 8), NR)]
            st[c, x0 + x] = val[:, :64]
            st[c, x0 + x + NP] = roll(val, 64)[:, :64]
            return carry
        lax.fori_loop(0, planes, plane, 0, unroll=16)
        for h in range(2):
            at = pl.ds(x0 + NP * h, planes)
            stores.append(pltpu.make_async_copy(st.at[c, at], x_out.at[c, at], out_sem.at[n, h]))
            stores[-1].start()
    hist_in.wait()
    ho[...] = hs[:2, :ITERS + 1]
    stores.append(pltpu.make_async_copy(ho, hist_out, h_sem.at[1]))
    stores[-1].start()
    for cp in stores:
        cp.wait()


def run(s, b, x0, kx, ky, kz):
    v = lambda *shape: pltpu.VMEM(shape, F32)
    sem = lambda *shape: pltpu.SemaphoreType.DMA(shape)
    scratch = [v(2, 64, 64, 64)] * 6
    full = v(2 * SYS, LN)
    scratch += [full, full, full, v(2 * PSYS, LN), full, full, full, v(2, NR, LN), v(2 * KSYS, LN), full, full, full, v(2, 32, LN)]
    scratch += [v(2, NR, LN), v(2, 32, LN), v(2, 32, LN)] * 2
    scratch += [v(2, 32, LN)] * 8
    scratch += [v(2, NR, LN), v(2, 32, LN), v(2, 32, LN), v(2, NR, LN), v(2, 32, LN)]
    scratch += [v(2, 2, NR, LN), v(2, 2, 32, LN), v(2, 2, 32, LN)]
    scratch += [v(2, 2, 8, 1, LN), v(2, 8, LN), v(2, 8, LN), v(8, LN)]
    scratch += [sem(6, 2), sem(2, 6), sem(2, 6), sem(2, 3), sem(2, 3), sem(2, 3), sem(2, 2, 3), sem(2, 2, 8), sem(2, 2, 8), sem(2)]
    xp, hist = pl.pallas_call(
        kernel,
        out_shape=(jax.ShapeDtypeStruct((2 * SYS, LN), F32), jax.ShapeDtypeStruct((8, LN), F32)),
        in_specs=[pl.BlockSpec(memory_space=pl.ANY)] * 6,
        out_specs=(pl.BlockSpec(memory_space=pl.ANY), pl.BlockSpec(memory_space=pltpu.VMEM)),
        scratch_shapes=scratch,
        compiler_params=pltpu.CompilerParams(collective_id=0, has_side_effects=True, vmem_limit_bytes=VMEM_MAIN),
        name='cg',
    )(s, b, x0, kx, ky, kz)
    return pl.pallas_call(
        unpack,
        out_shape=(jax.ShapeDtypeStruct((2, 64, 64, 64), F32), jax.ShapeDtypeStruct((2, ITERS + 1), F32)),
        in_specs=[pl.BlockSpec(memory_space=pl.ANY)] * 2,
        out_specs=[pl.BlockSpec(memory_space=pl.ANY)] * 2,
        scratch_shapes=[v(2 * SYS, LN), v(2, 64, 64, 64), v(8, LN), v(2, ITERS + 1), sem(2 * CHUNKS), sem(2 * CHUNKS, 2), sem(2)],
        compiler_params=pltpu.CompilerParams(vmem_limit_bytes=60 * 1024 * 1024),
        name='unpack',
    )(xp, hist)


def solution(mesh):
    field = P(None, 'px', 'py', 'pz')
    return jax.shard_map(run, mesh=mesh, in_specs=(field,) * 6, out_specs=(field, P(None, None)), check_vma=False)
```

```python
import jax
import jax.numpy as jnp
from jax import lax
from jax.experimental import pallas as pl
from jax.experimental.pallas import tpu as pltpu
from jax.sharding import PartitionSpec as P

ITERS = 20
F32 = jnp.float32
MESH = pl.DeviceIdType.MESH

NP = 32
NR = 64
LN = 128
PR = 80
KR = 72
SYS = NP * NR
PSYS = (NP + 1) * PR
KSYS = NP * KR
IN_FLIGHT = 3
AHEAD = 3


def roll(val, shift):
    if isinstance(shift, int):
        shift = shift % LN
    return pltpu.roll(val, shift, 1)


def kernel(s_hbm, b_hbm, x0_hbm, kx_hbm, ky_hbm, kz_hbm, x_out, hist_out,
           st_s, st_b, st_x, st_kx, st_ky, st_kz,
           X, R, Q, PB, PZ, RZ, KX, KXM, KY, KZ, KZF, D, KF,
           ix, iy, iz, jx, jy, jz, sxy, sxz, sky, skz, sy, sz, sry, srz,
           rhx, rhy, rhz, phx, phy, qhx, qhy, qhz,
           red, rho_s, alpha_s, hist_s,
           ld_sem, isend, irecv, rsend, rrecv, qsend, qrecv, dsend, drecv, out_sem):
    pz, py, px = lax.axis_index('pz'), lax.axis_index('py'), lax.axis_index('px')
    nbr = {'x': (pz, py, 1 - px), 'y': (pz, 1 - py, px), 'z': (1 - pz, py, px)}
    others = {}
    for m in range(1, 8):
        others[m] = (1 - pz if m & 4 else pz, 1 - py if m & 2 else py, 1 - px if m & 1 else px)

    lane = lax.broadcasted_iota(jnp.int32, (8, LN), 1)
    row8 = lax.broadcasted_iota(jnp.int32, (8, LN), 0)

    def lanes(n):
        return lax.broadcasted_iota(jnp.int32, (n, LN), 1)

    zf = 63 * (1 - pz)
    xf = 31 * (1 - px)
    yf = 63 * (1 - py)
    hrow = 72 - 65 * py
    to_z = 127 - 126 * pz
    fro_z = 1 + 126 * pz

    def face_mask(n):
        return (lanes(n) % 64) == zf

    def splits(n):
        return lanes(n) < 64

    order = [(num, c) for c in range(2) for num in range(6)]
    pairs = ((x0_hbm, st_x), (kz_hbm, st_kz), (ky_hbm, st_ky), (kx_hbm, st_kx), (s_hbm, st_s), (b_hbm, st_b))
    loads = [pltpu.make_async_copy(pairs[num][0].at[c], pairs[num][1].at[c], ld_sem.at[num, c]) for num, c in order]
    for cp in loads[:IN_FLIGHT]:
        cp.start()

    def loaded(num, c):
        n = c * 6 + num
        loads[n].wait()
        if n + IN_FLIGHT < len(loads):
            loads[n + IN_FLIGHT].start()

    barrier = pltpu.get_barrier_semaphore()
    for m in range(1, 8):
        pl.semaphore_signal(barrier, inc=1, device_id=others[m], device_id_type=MESH)

    def packed(st, c, x):
        return jnp.concatenate([st[c, x], st[c, x + NP]], axis=1)

    def pick(T, val, x, f):
        l64 = lanes(32) % 64
        T = jnp.where(l64 == x, roll(val[:32], lax.rem(x - f + LN, LN)), T)
        return jnp.where(l64 == x + 32, roll(val[32:], lax.rem(x + 32 - f + LN, LN)), T)

    def spread(G, x, f):
        return jnp.concatenate([roll(G, lax.rem(f - x + LN, LN)), roll(G, lax.rem(f - x - 32 + LN, LN))], axis=0)

    zero32 = jnp.zeros((32, LN), F32)

    def remote(src, dst, send_sem, recv_sem, dev):
        return pltpu.make_async_remote_copy(src_ref=src, dst_ref=dst, send_sem=send_sem, recv_sem=recv_sem, device_id=dev, device_id_type=MESH)

    def x_plane(ref, c):
        return ref.at[pl.ds(pl.multiple_of(c * SYS + xf * NR, 8), NR)]

    def rows(x, c):
        return pl.ds(pl.multiple_of(c * SYS + x * NR, 8), NR)

    first = []
    for c in range(2):
        first.append([
            remote(sxz.at[c], iz.at[c], isend.at[c, 0], irecv.at[c, 0], nbr['z']),
            remote(sxy.at[c], iy.at[c], isend.at[c, 1], irecv.at[c, 1], nbr['y']),
            remote(x_plane(X, c), ix.at[c], isend.at[c, 2], irecv.at[c, 2], nbr['x']),
            remote(skz.at[c], jz.at[c], isend.at[c, 3], irecv.at[c, 3], nbr['z']),
            remote(sky.at[c], jy.at[c], isend.at[c, 4], irecv.at[c, 4], nbr['y']),
            remote(KX.at[pl.ds(c * SYS + 31 * NR, NR)], jx.at[c], isend.at[c, 5], irecv.at[c, 5], nbr['x'])])

    def prepare_x0(c):
        loaded(0, c)

        def pack_x(x, T):
            u = packed(st_x, c, x)
            X[rows(x, c)] = u
            base = pl.multiple_of(c * PSYS + x * PR, 8)
            PB[pl.ds(base, 8)] = jnp.zeros((8, LN), F32)
            PB[pl.ds(base + 72, 8)] = jnp.zeros((8, LN), F32)
            PB[pl.ds(base + 8, NR)] = u
            return pick(T, u, x, zf)
        sxz[c] = lax.fori_loop(0, NP, pack_x, zero32, unroll=8)
        sxy[c] = X[pl.ds(c * SYS + yf, 32, stride=NR)]

    def prepare_kz(c):
        loaded(1, c)

        def pack_z(x, T):
            u = packed(st_kz, c, x)
            inner = jnp.where(lanes(NR) % 64 == 63, 0.0, u)
            moved = roll(inner, 1)
            KZ[rows(x, c)] = jnp.where(pz == 1, moved, inner)
            KZF[rows(x, c)] = jnp.where(pz == 1, inner, moved)
            return pick(T, u, x, 63)
        skz[c] = lax.fori_loop(0, NP, pack_z, zero32, unroll=8)

    def prepare_ky(c):
        loaded(2, c)

        def pack_ky(x, carry):
            u = packed(st_ky, c, x)
            row = lax.broadcasted_iota(jnp.int32, (NR, LN), 0)
            u = jnp.where(jnp.logical_and(row == NR - 1, py == 1), 0.0, u)
            KY[pl.ds(pl.multiple_of(c * KSYS + x * KR + 8, 8), NR)] = u
            return carry
        lax.fori_loop(0, NP, pack_ky, 0, unroll=8)
        sky[c] = KY[pl.ds(c * KSYS + 71, 32, stride=KR)]

    def prepare_kx(c):
        loaded(3, c)

        def pack_kx(x, carry):
            KX[rows(x, c)] = packed(st_kx, c, x)
            return carry
        lax.fori_loop(0, NP, pack_kx, 0, unroll=8)
        last = KX[pl.ds(c * SYS + 31 * NR, NR)]
        edge = jnp.logical_and(lanes(NR) >= 64, px == 1)
        KX[pl.ds(c * SYS + 31 * NR, NR)] = jnp.where(edge, 0.0, last)

    def prepare_sb(c):
        loaded(4, c)
        loaded(5, c)

        def pack_sb(x, carry):
            D[rows(x, c)] = packed(st_s, c, x)
            R[rows(x, c)] = packed(st_b, c, x)
            return carry
        lax.fori_loop(0, NP, pack_sb, 0, unroll=8)

    prepare_x0(0)
    pl.semaphore_wait(barrier, 7)
    for cp in first[0][:3]:
        cp.start()
    prepare_kz(0)
    first[0][3].start()
    prepare_ky(0)
    first[0][4].start()
    prepare_kx(0)
    first[0][5].start()
    prepare_sb(0)
    prepare_x0(1)
    for cp in first[1][:3]:
        cp.start()
    prepare_kz(1)
    first[1][3].start()
    prepare_ky(1)
    first[1][4].start()

    def reduce_copies(kind, c):
        return [remote(red.at[kind, c, 0], red.at[kind, c, m], dsend.at[kind, c, m], drecv.at[kind, c, m], others[m]) for m in (7, 6, 5, 4, 3, 2, 1)]

    def reduce_start(kind, c, part):
        red[kind, c, 0] = jnp.sum(part, axis=0, keepdims=True)
        for cp in reduce_copies(kind, c):
            cp.start()

    def reduce_end(kind, c):
        for cp in reduce_copies(kind, c):
            cp.wait_recv()
        v = [red[kind, c, m] for m in range(8)]
        total = ((v[0] + v[1]) + (v[2] + v[3])) + ((v[4] + v[5]) + (v[6] + v[7]))
        total = jnp.broadcast_to(total, (8, LN))
        return jnp.broadcast_to(jnp.sum(total, axis=1, keepdims=True), (8, LN))

    def reduce_sent(kind, c):
        for cp in reduce_copies(kind, c):
            cp.wait_send()

    def fold(val):
        return jnp.sum(val.reshape(-1, 8, LN), axis=0)

    def wide(vec, n):
        return jnp.broadcast_to(vec[None], (n // 8, 8, LN)).reshape(n, LN)

    def z_face(ref, c, to_sz, to_sy):
        def plane(x, T):
            return pick(T, ref[rows(x, c)], x, zf)
        to_sz[c] = lax.fori_loop(0, NP, plane, zero32, unroll=8)
        to_sy[c] = ref[pl.ds(c * SYS + yf, 32, stride=NR)]

    def turn_r(c):
        G = rhz[c]
        mask = face_mask(NR)

        def plane(x, carry):
            RZ[rows(x, c)] = jnp.where(mask, spread(G, x, zf), roll(R[rows(x, c)], to_z))
            return carry
        lax.fori_loop(0, NP, plane, 0, unroll=8)

    def r_copies(c):
        return [
            remote(srz.at[c], rhz.at[c], rsend.at[c, 0], rrecv.at[c, 0], nbr['z']),
            remote(sry.at[c], rhy.at[c], rsend.at[c, 1], rrecv.at[c, 1], nbr['y']),
            remote(x_plane(R, c), rhx.at[c], rsend.at[c, 2], rrecv.at[c, 2], nbr['x'])]

    def start(c):
        for cp in first[c]:
            cp.wait_recv()
        lo = splits(NR)
        kx_last = KX[pl.ds(c * SYS + 31 * NR, NR)]
        KXM[c] = roll(jnp.where(lo, kx_last, jnp.where(px == 1, jx[c], 0.0)), 64)
        KY[pl.ds(c * KSYS + 7, 32, stride=KR)] = jnp.where(py == 1, jy[c], 0.0)
        KF[c] = jnp.where(pz == 1, jz[c], skz[c])
        PB[pl.ds(c * PSYS + hrow, 32, stride=PR)] = iy[c]
        u_first = PB[pl.ds(c * PSYS + 8, NR)]
        u_last = PB[pl.ds(c * PSYS + 31 * PR + 8, NR)]
        PB[pl.ds(c * PSYS + 32 * PR + 8, NR)] = roll(jnp.where(lo, ix[c], u_first), 64)
        low = roll(jnp.where(lo, u_last, ix[c]), 64)
        kf, uf = KF[c], iz[c]
        mask = face_mask(NR)

        def start_plane(x, carry):
            acc, fx_prev, kx_prev, u = carry
            base = pl.multiple_of(c * PSYS + x * PR, 8)
            at = rows(x, c)
            kbase = pl.multiple_of(c * KSYS + x * KR, 8)
            nxt = PB[pl.ds(base + PR + 8, NR)]
            yu = PB[pl.ds(base + 9, NR)]
            yl = PB[pl.ds(base + 7, NR)]
            s = D[at]
            kxv = KX[at]
            kyv = KY[pl.ds(kbase + 8, NR)]
            kyl = KY[pl.ds(kbase + 7, NR)]
            kzf = jnp.where(mask, spread(kf, x, zf), KZ[at])
            uz = jnp.where(mask, spread(uf, x, zf), roll(u, to_z))
            fx = kxv * (u - nxt)
            fz = kzf * (u - uz)
            fz_away = roll(jnp.where(mask, 0.0, fz), fro_z)
            D[at] = s + (kxv + kx_prev) + (kyv + kyl) + (kzf + KZF[at])
            KZF[at] = kzf
            PZ[at] = uz
            r = R[at] - (s * u + (fx - fx_prev) + (kyv * (u - yu) - kyl * (yl - u)) + (fz - fz_away))
            R[at] = r
            return acc + fold(r * r), fx, kxv, nxt
        init = (jnp.zeros((8, LN), F32), KXM[c] * (low - u_first), KXM[c], u_first)
        acc = lax.fori_loop(0, NP, start_plane, init, unroll=4)[0]
        reduce_start(0, c, acc)
        z_face(R, c, srz, sry)
        for cp in r_copies(c):
            cp.start()

    start(0)
    prepare_kx(1)
    first[1][5].start()
    prepare_sb(1)
    start(1)
    hist_s[...] = jnp.zeros((8, LN), F32)
    for c in range(2):
        phx[c] = jnp.zeros((NR, LN), F32)
        phy[c] = zero32
        for cp in first[c]:
            cp.wait_send()
    for cp in r_copies(0):
        cp.wait_recv()
    turn_r(0)

    def q_copies(c, par):
        return [
            remote(sz.at[c], qhz.at[par, c], qsend.at[c, 0], qrecv.at[par, c, 0], nbr['z']),
            remote(sy.at[c], qhy.at[par, c], qsend.at[c, 1], qrecv.at[par, c, 1], nbr['y']),
            remote(x_plane(Q, c), qhx.at[par, c], qsend.at[c, 2], qrecv.at[par, c, 2], nbr['x'])]

    def note(c, k, rho):
        hist_s[...] = jnp.where(jnp.logical_and(lane == k, row8 == c), rho, hist_s[...])

    def product(c, beta):
        b64 = wide(beta, NR)
        hx = rhx[c] + b64 * phx[c]
        hy = rhy[c] + wide(beta, 32) * phy[c]
        phx[c] = hx
        phy[c] = hy
        PB[pl.ds(c * PSYS + hrow, 32, stride=PR)] = hy
        lo = splits(NR)

        def direction(x):
            at = pl.ds(c * PSYS + x * PR + 8, NR)
            val = R[pl.ds(c * SYS + x * NR, NR)] + b64 * PB[at]
            PB[at] = val
            return val

        def turn(x, p):
            return roll(KZ[pl.ds(c * SYS + x * NR, NR)] * p, fro_z)

        def load_p(x):
            return PB[pl.ds(c * PSYS + x * PR + 8, NR)]

        p_last = direction(NP - 1)
        p_first = direction(0)
        above = roll(jnp.where(lo, hx, p_first), 64)
        below = roll(jnp.where(lo, p_last, hx), 64)
        turned = {0: turn(0, p_first)}
        for x in range(1, AHEAD):
            turned[x] = turn(x, direction(x))
        cur, kxp_prev = p_first, KXM[c] * below
        acc = jnp.zeros((8, LN), F32)
        for x in range(NP):
            w = x + AHEAD
            if w < NP:
                turned[w] = turn(w, direction(w) if w < NP - 1 else load_p(w))
            nxt = load_p(x + 1) if x + 1 < NP else above
            base = c * PSYS + x * PR
            at = pl.ds(c * SYS + x * NR, NR)
            kbase = c * KSYS + x * KR
            kxv = KX[at]
            kxp = kxv * cur
            q = D[at] * cur - kxp_prev - kxv * nxt
            q = q - KY[pl.ds(kbase + 8, NR)] * PB[pl.ds(base + 9, NR)]
            q = q - KY[pl.ds(kbase + 7, NR)] * PB[pl.ds(base + 7, NR)]
            pz_new = RZ[at] + b64 * PZ[at]
            PZ[at] = pz_new
            q = q - KZF[at] * pz_new - turned.pop(x)
            Q[at] = q
            acc = acc + fold(cur * q)
            cur, kxp_prev = nxt, kxp
        return acc

    outs = [pltpu.make_async_copy(X.at[pl.ds(c * SYS, SYS)], x_out.at[pl.ds(c * SYS, SYS)], out_sem.at[c]) for c in range(2)]

    def halo_r(c, par):
        for cp in q_copies(c, par):
            cp.wait_recv()
        alpha = alpha_s[c]
        rhx[c] = rhx[c] - wide(alpha, NR) * qhx[par, c]
        rhy[c] = rhy[c] - wide(alpha, 32) * qhy[par, c]
        rhz[c] = rhz[c] - wide(alpha, 32) * qhz[par, c]

    def q_sent(c, par):
        for cp in q_copies(c, par):
            cp.wait_send()

    def first_half(c, k, par):
        rho = reduce_end(0, c)
        note(c, k, rho)
        beta = jnp.where(k == 0, 0.0, rho / rho_s[c])
        rho_s[c] = rho
        reduce_start(1, c, product(c, beta))
        reduce_sent(0, c)
        z_face(Q, c, sz, sy)
        for cp in q_copies(c, par):
            cp.start()

    def second_half(c, k):
        alpha = rho_s[c] / reduce_end(1, c)
        alpha_s[c] = alpha
        a_pl = wide(alpha, NR)
        acc = jnp.zeros((8, LN), F32)
        for x in range(NP):
            at = pl.ds(c * SYS + x * NR, NR)
            r = R[at] - a_pl * Q[at]
            R[at] = r
            acc = acc + fold(r * r)
        reduce_start(0, c, acc)

        def step_x(x, carry):
            X[rows(x, c)] = X[rows(x, c)] + a_pl * PB[pl.ds(pl.multiple_of(c * PSYS + x * PR + 8, 8), NR)]
            return carry
        lax.fori_loop(0, NP, step_x, 0, unroll=4)

        @pl.when(k == ITERS - 1)
        def _():
            outs[c].start()
        reduce_sent(1, c)

    def body(k, carry):
        par = k % 2
        first_half(0, k, par)

        @pl.when(k == 0)
        def _():
            for cp in r_copies(1):
                cp.wait_recv()

        @pl.when(k > 0)
        def _():
            halo_r(1, 1 - par)
            q_sent(1, 1 - par)
        turn_r(1)
        first_half(1, k, par)

        @pl.when(k == 0)
        def _():
            for c in range(2):
                for cp in r_copies(c):
                    cp.wait_send()
        second_half(0, k)
        second_half(1, k)
        halo_r(0, par)
        turn_r(0)
        q_sent(0, par)
        return carry

    lax.fori_loop(0, ITERS, body, 0)
    for c in range(2):
        note(c, ITERS, reduce_end(0, c))
        reduce_sent(0, c)
    for cp in q_copies(1, (ITERS - 1) % 2):
        cp.wait()
    hist_out[...] = jnp.sqrt(hist_s[...] * (1.0 / (128 * 128 * 128)))
    for cp in outs:
        cp.wait()


CHUNKS = 2
VMEM_MAIN = 60 * 1024 * 1024


def unpack(xp, hist, x_out, hist_out, buf, st, hs, ho, in_sem, out_sem, h_sem):
    planes = NP // CHUNKS
    hist_in = pltpu.make_async_copy(hist, hs, h_sem.at[0])
    hist_in.start()
    loads = []
    for n in range(2 * CHUNKS):
        at = pl.ds(n * planes * NR, planes * NR)
        loads.append(pltpu.make_async_copy(xp.at[at], buf.at[at], in_sem.at[n]))
        loads[n].start()
    stores = []
    for n in range(2 * CHUNKS):
        c, x0 = n // CHUNKS, n % CHUNKS * planes
        loads[n].wait()

        def plane(x, carry):
            val = buf[pl.ds(pl.multiple_of(n * planes * NR + x * NR, 8), NR)]
            st[c, x0 + x] = val[:, :64]
            st[c, x0 + x + NP] = roll(val, 64)[:, :64]
            return carry
        lax.fori_loop(0, planes, plane, 0, unroll=16)
        for h in range(2):
            at = pl.ds(x0 + NP * h, planes)
            stores.append(pltpu.make_async_copy(st.at[c, at], x_out.at[c, at], out_sem.at[n, h]))
            stores[-1].start()
    hist_in.wait()
    ho[...] = hs[:2, :ITERS + 1]
    stores.append(pltpu.make_async_copy(ho, hist_out, h_sem.at[1]))
    stores[-1].start()
    for cp in stores:
        cp.wait()


def run(s, b, x0, kx, ky, kz):
    v = lambda *shape: pltpu.VMEM(shape, F32)
    sem = lambda *shape: pltpu.SemaphoreType.DMA(shape)
    scratch = [v(2, 64, 64, 64)] * 6
    full = v(2 * SYS, LN)
    scratch += [full, full, full, v(2 * PSYS, LN), full, full, full, v(2, NR, LN), v(2 * KSYS, LN), full, full, full, v(2, 32, LN)]
    scratch += [v(2, NR, LN), v(2, 32, LN), v(2, 32, LN)] * 2
    scratch += [v(2, 32, LN)] * 8
    scratch += [v(2, NR, LN), v(2, 32, LN), v(2, 32, LN), v(2, NR, LN), v(2, 32, LN)]
    scratch += [v(2, 2, NR, LN), v(2, 2, 32, LN), v(2, 2, 32, LN)]
    scratch += [v(2, 2, 8, 1, LN), v(2, 8, LN), v(2, 8, LN), v(8, LN)]
    scratch += [sem(6, 2), sem(2, 6), sem(2, 6), sem(2, 3), sem(2, 3), sem(2, 3), sem(2, 2, 3), sem(2, 2, 8), sem(2, 2, 8), sem(2)]
    xp, hist = pl.pallas_call(
        kernel,
        out_shape=(jax.ShapeDtypeStruct((2 * SYS, LN), F32), jax.ShapeDtypeStruct((8, LN), F32)),
        in_specs=[pl.BlockSpec(memory_space=pl.ANY)] * 6,
        out_specs=(pl.BlockSpec(memory_space=pl.ANY), pl.BlockSpec(memory_space=pltpu.VMEM)),
        scratch_shapes=scratch,
        compiler_params=pltpu.CompilerParams(collective_id=0, has_side_effects=True, vmem_limit_bytes=VMEM_MAIN),
        name='cg',
    )(s, b, x0, kx, ky, kz)
    return pl.pallas_call(
        unpack,
        out_shape=(jax.ShapeDtypeStruct((2, 64, 64, 64), F32), jax.ShapeDtypeStruct((2, ITERS + 1), F32)),
        in_specs=[pl.BlockSpec(memory_space=pl.ANY)] * 2,
        out_specs=[pl.BlockSpec(memory_space=pl.ANY)] * 2,
        scratch_shapes=[v(2 * SYS, LN), v(2, 64, 64, 64), v(8, LN), v(2, ITERS + 1), sem(2 * CHUNKS), sem(2 * CHUNKS, 2), sem(2)],
        compiler_params=pltpu.CompilerParams(vmem_limit_bytes=60 * 1024 * 1024),
        name='unpack',
    )(xp, hist)


def solution(mesh):
    field = P(None, 'px', 'py', 'pz')
    return jax.shard_map(run, mesh=mesh, in_specs=(field,) * 6, out_specs=(field, P(None, None)), check_vma=False)
```

```python
import jax
import jax.numpy as jnp
from jax import lax
from jax.experimental import pallas as pl
from jax.experimental.pallas import tpu as pltpu
from jax.sharding import PartitionSpec as P

ITERS = 20
F32 = jnp.float32
MESH = pl.DeviceIdType.MESH

NP = 32
NR = 64
LN = 128
PR = 80
KR = 72
SYS = NP * NR
PSYS = (NP + 1) * PR
KSYS = NP * KR
IN_FLIGHT = 3
AHEAD = 3


def roll(val, shift):
    if isinstance(shift, int):
        shift = shift % LN
    return pltpu.roll(val, shift, 1)


def kernel(s_hbm, b_hbm, x0_hbm, kx_hbm, ky_hbm, kz_hbm, x_out, hist_out,
           st_s, st_b, st_x, st_kx, st_ky, st_kz,
           X, R, Q, PB, PZ, RZ, KX, KXM, KY, KZ, KZF, D, KF,
           ix, iy, iz, jx, jy, jz, sxy, sxz, sky, skz, sy, sz, sry, srz,
           rhx, rhy, rhz, phx, phy, qhx, qhy, qhz,
           red, rho_s, alpha_s, hist_s,
           ld_sem, isend, irecv, rsend, rrecv, qsend, qrecv, dsend, drecv, out_sem):
    pz, py, px = lax.axis_index('pz'), lax.axis_index('py'), lax.axis_index('px')
    nbr = {'x': (pz, py, 1 - px), 'y': (pz, 1 - py, px), 'z': (1 - pz, py, px)}
    others = {}
    for m in range(1, 8):
        others[m] = (1 - pz if m & 4 else pz, 1 - py if m & 2 else py, 1 - px if m & 1 else px)

    lane = lax.broadcasted_iota(jnp.int32, (8, LN), 1)
    row8 = lax.broadcasted_iota(jnp.int32, (8, LN), 0)

    def lanes(n):
        return lax.broadcasted_iota(jnp.int32, (n, LN), 1)

    zf = 63 * (1 - pz)
    xf = 31 * (1 - px)
    yf = 63 * (1 - py)
    hrow = 72 - 65 * py
    to_z = 127 - 126 * pz
    fro_z = 1 + 126 * pz

    def face_mask(n):
        return (lanes(n) % 64) == zf

    def splits(n):
        return lanes(n) < 64

    order = [(num, c) for c in range(2) for num in range(6)]
    pairs = ((x0_hbm, st_x), (kz_hbm, st_kz), (ky_hbm, st_ky), (kx_hbm, st_kx), (s_hbm, st_s), (b_hbm, st_b))
    loads = [pltpu.make_async_copy(pairs[num][0].at[c], pairs[num][1].at[c], ld_sem.at[num, c]) for num, c in order]
    for cp in loads[:IN_FLIGHT]:
        cp.start()

    def loaded(num, c):
        n = c * 6 + num
        loads[n].wait()
        if n + IN_FLIGHT < len(loads):
            loads[n + IN_FLIGHT].start()

    barrier = pltpu.get_barrier_semaphore()
    for m in range(1, 8):
        pl.semaphore_signal(barrier, inc=1, device_id=others[m], device_id_type=MESH)

    def packed(st, c, x):
        return jnp.concatenate([st[c, x], st[c, x + NP]], axis=1)

    def pick(T, val, x, f):
        l64 = lanes(32) % 64
        T = jnp.where(l64 == x, roll(val[:32], lax.rem(x - f + LN, LN)), T)
        return jnp.where(l64 == x + 32, roll(val[32:], lax.rem(x + 32 - f + LN, LN)), T)

    def spread(G, x, f):
        return jnp.concatenate([roll(G, lax.rem(f - x + LN, LN)), roll(G, lax.rem(f - x - 32 + LN, LN))], axis=0)

    zero32 = jnp.zeros((32, LN), F32)

    def remote(src, dst, send_sem, recv_sem, dev):
        return pltpu.make_async_remote_copy(src_ref=src, dst_ref=dst, send_sem=send_sem, recv_sem=recv_sem, device_id=dev, device_id_type=MESH)

    def x_plane(ref, c):
        return ref.at[pl.ds(pl.multiple_of(c * SYS + xf * NR, 8), NR)]

    def rows(x, c):
        return pl.ds(pl.multiple_of(c * SYS + x * NR, 8), NR)

    first = []
    for c in range(2):
        first.append([
            remote(sxz.at[c], iz.at[c], isend.at[c, 0], irecv.at[c, 0], nbr['z']),
            remote(sxy.at[c], iy.at[c], isend.at[c, 1], irecv.at[c, 1], nbr['y']),
            remote(x_plane(X, c), ix.at[c], isend.at[c, 2], irecv.at[c, 2], nbr['x']),
            remote(skz.at[c], jz.at[c], isend.at[c, 3], irecv.at[c, 3], nbr['z']),
            remote(sky.at[c], jy.at[c], isend.at[c, 4], irecv.at[c, 4], nbr['y']),
            remote(KX.at[pl.ds(c * SYS + 31 * NR, NR)], jx.at[c], isend.at[c, 5], irecv.at[c, 5], nbr['x'])])

    def prepare_x0(c):
        loaded(0, c)

        def pack_x(x, T):
            u = packed(st_x, c, x)
            X[rows(x, c)] = u
            base = pl.multiple_of(c * PSYS + x * PR, 8)
            PB[pl.ds(base, 8)] = jnp.zeros((8, LN), F32)
            PB[pl.ds(base + 72, 8)] = jnp.zeros((8, LN), F32)
            PB[pl.ds(base + 8, NR)] = u
            return pick(T, u, x, zf)
        sxz[c] = lax.fori_loop(0, NP, pack_x, zero32, unroll=8)
        sxy[c] = X[pl.ds(c * SYS + yf, 32, stride=NR)]

    def prepare_kz(c):
        loaded(1, c)

        def pack_z(x, T):
            u = packed(st_kz, c, x)
            inner = jnp.where(lanes(NR) % 64 == 63, 0.0, u)
            moved = roll(inner, 1)
            KZ[rows(x, c)] = jnp.where(pz == 1, moved, inner)
            KZF[rows(x, c)] = jnp.where(pz == 1, inner, moved)
            return pick(T, u, x, 63)
        skz[c] = lax.fori_loop(0, NP, pack_z, zero32, unroll=8)

    def prepare_ky(c):
        loaded(2, c)

        def pack_ky(x, carry):
            u = packed(st_ky, c, x)
            row = lax.broadcasted_iota(jnp.int32, (NR, LN), 0)
            u = jnp.where(jnp.logical_and(row == NR - 1, py == 1), 0.0, u)
            KY[pl.ds(pl.multiple_of(c * KSYS + x * KR + 8, 8), NR)] = u
            return carry
        lax.fori_loop(0, NP, pack_ky, 0, unroll=8)
        sky[c] = KY[pl.ds(c * KSYS + 71, 32, stride=KR)]

    def prepare_kx(c):
        loaded(3, c)

        def pack_kx(x, carry):
            KX[rows(x, c)] = packed(st_kx, c, x)
            return carry
        lax.fori_loop(0, NP, pack_kx, 0, unroll=8)
        last = KX[pl.ds(c * SYS + 31 * NR, NR)]
        edge = jnp.logical_and(lanes(NR) >= 64, px == 1)
        KX[pl.ds(c * SYS + 31 * NR, NR)] = jnp.where(edge, 0.0, last)

    def prepare_sb(c):
        loaded(4, c)
        loaded(5, c)

        def pack_sb(x, carry):
            D[rows(x, c)] = packed(st_s, c, x)
            R[rows(x, c)] = packed(st_b, c, x)
            return carry
        lax.fori_loop(0, NP, pack_sb, 0, unroll=8)

    prepare_x0(0)
    pl.semaphore_wait(barrier, 7)
    for cp in first[0][:3]:
        cp.start()
    prepare_kz(0)
    first[0][3].start()
    prepare_ky(0)
    first[0][4].start()
    prepare_kx(0)
    first[0][5].start()
    prepare_sb(0)
    prepare_x0(1)
    for cp in first[1][:3]:
        cp.start()
    prepare_kz(1)
    first[1][3].start()
    prepare_ky(1)
    first[1][4].start()

    def reduce_copies(kind, c):
        return [remote(red.at[kind, c, 0], red.at[kind, c, m], dsend.at[kind, c, m], drecv.at[kind, c, m], others[m]) for m in (7, 6, 5, 4, 3, 2, 1)]

    def reduce_start(kind, c, part):
        red[kind, c, 0] = jnp.sum(part, axis=0, keepdims=True)
        for cp in reduce_copies(kind, c):
            cp.start()

    def reduce_arrived(kind, c):
        for cp in reduce_copies(kind, c):
            cp.wait_recv()

    def reduce_end(kind, c):
        v = [red[kind, c, m] for m in range(8)]
        total = ((v[0] + v[1]) + (v[2] + v[3])) + ((v[4] + v[5]) + (v[6] + v[7]))
        total = jnp.broadcast_to(total, (8, LN))
        return jnp.broadcast_to(jnp.sum(total, axis=1, keepdims=True), (8, LN))

    def reduce_sent(kind, c):
        for cp in reduce_copies(kind, c):
            cp.wait_send()

    def fold(val):
        return jnp.sum(val.reshape(-1, 8, LN), axis=0)

    def wide(vec, n):
        return jnp.broadcast_to(vec[None], (n // 8, 8, LN)).reshape(n, LN)

    def z_face(ref, c, to_sz, to_sy):
        def plane(x, T):
            return pick(T, ref[rows(x, c)], x, zf)
        to_sz[c] = lax.fori_loop(0, NP, plane, zero32, unroll=8)
        to_sy[c] = ref[pl.ds(c * SYS + yf, 32, stride=NR)]

    def turn_r(c):
        G = rhz[c]
        mask = face_mask(NR)

        def plane(x, carry):
            RZ[rows(x, c)] = jnp.where(mask, spread(G, x, zf), roll(R[rows(x, c)], to_z))
            return carry
        lax.fori_loop(0, NP, plane, 0, unroll=8)

    def r_copies(c):
        return [
            remote(srz.at[c], rhz.at[c], rsend.at[c, 0], rrecv.at[c, 0], nbr['z']),
            remote(sry.at[c], rhy.at[c], rsend.at[c, 1], rrecv.at[c, 1], nbr['y']),
            remote(x_plane(R, c), rhx.at[c], rsend.at[c, 2], rrecv.at[c, 2], nbr['x'])]

    def start(c):
        for cp in first[c]:
            cp.wait_recv()
        lo = splits(NR)
        kx_last = KX[pl.ds(c * SYS + 31 * NR, NR)]
        KXM[c] = roll(jnp.where(lo, kx_last, jnp.where(px == 1, jx[c], 0.0)), 64)
        KY[pl.ds(c * KSYS + 7, 32, stride=KR)] = jnp.where(py == 1, jy[c], 0.0)
        KF[c] = jnp.where(pz == 1, jz[c], skz[c])
        PB[pl.ds(c * PSYS + hrow, 32, stride=PR)] = iy[c]
        u_first = PB[pl.ds(c * PSYS + 8, NR)]
        u_last = PB[pl.ds(c * PSYS + 31 * PR + 8, NR)]
        PB[pl.ds(c * PSYS + 32 * PR + 8, NR)] = roll(jnp.where(lo, ix[c], u_first), 64)
        low = roll(jnp.where(lo, u_last, ix[c]), 64)
        kf, uf = KF[c], iz[c]
        mask = face_mask(NR)

        def start_plane(x, carry):
            acc, fx_prev, kx_prev, u = carry
            base = pl.multiple_of(c * PSYS + x * PR, 8)
            at = rows(x, c)
            kbase = pl.multiple_of(c * KSYS + x * KR, 8)
            nxt = PB[pl.ds(base + PR + 8, NR)]
            yu = PB[pl.ds(base + 9, NR)]
            yl = PB[pl.ds(base + 7, NR)]
            s = D[at]
            kxv = KX[at]
            kyv = KY[pl.ds(kbase + 8, NR)]
            kyl = KY[pl.ds(kbase + 7, NR)]
            kzf = jnp.where(mask, spread(kf, x, zf), KZ[at])
            uz = jnp.where(mask, spread(uf, x, zf), roll(u, to_z))
            fx = kxv * (u - nxt)
            fz = kzf * (u - uz)
            fz_away = roll(jnp.where(mask, 0.0, fz), fro_z)
            D[at] = s + (kxv + kx_prev) + (kyv + kyl) + (kzf + KZF[at])
            KZF[at] = kzf
            PZ[at] = uz
            r = R[at] - (s * u + (fx - fx_prev) + (kyv * (u - yu) - kyl * (yl - u)) + (fz - fz_away))
            R[at] = r
            return acc + fold(r * r), fx, kxv, nxt
        init = (jnp.zeros((8, LN), F32), KXM[c] * (low - u_first), KXM[c], u_first)
        acc = lax.fori_loop(0, NP, start_plane, init, unroll=4)[0]
        reduce_start(0, c, acc)
        z_face(R, c, srz, sry)
        for cp in r_copies(c):
            cp.start()

    start(0)
    prepare_kx(1)
    first[1][5].start()
    prepare_sb(1)
    start(1)
    hist_s[...] = jnp.zeros((8, LN), F32)
    for c in range(2):
        phx[c] = jnp.zeros((NR, LN), F32)
        phy[c] = zero32
        for cp in first[c]:
            cp.wait_send()
    for cp in r_copies(0):
        cp.wait_recv()
    turn_r(0)
    reduce_arrived(0, 1)

    def q_copies(c, par):
        return [
            remote(sz.at[c], qhz.at[par, c], qsend.at[c, 0], qrecv.at[par, c, 0], nbr['z']),
            remote(sy.at[c], qhy.at[par, c], qsend.at[c, 1], qrecv.at[par, c, 1], nbr['y']),
            remote(x_plane(Q, c), qhx.at[par, c], qsend.at[c, 2], qrecv.at[par, c, 2], nbr['x'])]

    def note(c, k, rho):
        hist_s[...] = jnp.where(jnp.logical_and(lane == k, row8 == c), rho, hist_s[...])

    def product(c, beta):
        b64 = wide(beta, NR)
        hx = rhx[c] + b64 * phx[c]
        hy = rhy[c] + wide(beta, 32) * phy[c]
        phx[c] = hx
        phy[c] = hy
        PB[pl.ds(c * PSYS + hrow, 32, stride=PR)] = hy
        lo = splits(NR)

        def direction(x):
            at = pl.ds(c * PSYS + x * PR + 8, NR)
            val = R[pl.ds(c * SYS + x * NR, NR)] + b64 * PB[at]
            PB[at] = val
            return val

        def turn(x, p):
            return roll(KZ[pl.ds(c * SYS + x * NR, NR)] * p, fro_z)

        def load_p(x):
            return PB[pl.ds(c * PSYS + x * PR + 8, NR)]

        p_last = direction(NP - 1)
        p_first = direction(0)
        above = roll(jnp.where(lo, hx, p_first), 64)
        below = roll(jnp.where(lo, p_last, hx), 64)
        turned = {0: turn(0, p_first)}
        for x in range(1, AHEAD):
            turned[x] = turn(x, direction(x))
        cur, kxp_prev = p_first, KXM[c] * below
        acc = jnp.zeros((8, LN), F32)
        for x in range(NP):
            w = x + AHEAD
            if w < NP:
                turned[w] = turn(w, direction(w) if w < NP - 1 else load_p(w))
            nxt = load_p(x + 1) if x + 1 < NP else above
            base = c * PSYS + x * PR
            at = pl.ds(c * SYS + x * NR, NR)
            kbase = c * KSYS + x * KR
            kxv = KX[at]
            kxp = kxv * cur
            q = D[at] * cur - kxp_prev - kxv * nxt
            q = q - KY[pl.ds(kbase + 8, NR)] * PB[pl.ds(base + 9, NR)]
            q = q - KY[pl.ds(kbase + 7, NR)] * PB[pl.ds(base + 7, NR)]
            pz_new = RZ[at] + b64 * PZ[at]
            PZ[at] = pz_new
            q = q - KZF[at] * pz_new - turned.pop(x)
            Q[at] = q
            acc = acc + fold(cur * q)
            cur, kxp_prev = nxt, kxp
        return acc

    outs = [pltpu.make_async_copy(X.at[pl.ds(c * SYS, SYS)], x_out.at[pl.ds(c * SYS, SYS)], out_sem.at[c]) for c in range(2)]

    def halo_r(c, par):
        for cp in q_copies(c, par):
            cp.wait_recv()
        alpha = alpha_s[c]
        rhx[c] = rhx[c] - wide(alpha, NR) * qhx[par, c]
        rhy[c] = rhy[c] - wide(alpha, 32) * qhy[par, c]
        rhz[c] = rhz[c] - wide(alpha, 32) * qhz[par, c]

    def q_sent(c, par):
        for cp in q_copies(c, par):
            cp.wait_send()

    def first_half(c, k, par):
        if c == 0:
            reduce_arrived(0, c)
        else:
            pl.when(k > 0)(lambda: reduce_arrived(0, c))
        rho = reduce_end(0, c)
        note(c, k, rho)
        beta = jnp.where(k == 0, 0.0, rho / rho_s[c])
        rho_s[c] = rho
        reduce_start(1, c, product(c, beta))
        reduce_sent(0, c)
        z_face(Q, c, sz, sy)
        for cp in q_copies(c, par):
            cp.start()

    def second_half(c, k):
        reduce_arrived(1, c)
        alpha = rho_s[c] / reduce_end(1, c)
        alpha_s[c] = alpha
        a_pl = wide(alpha, NR)
        acc = jnp.zeros((8, LN), F32)
        for x in range(NP):
            at = pl.ds(c * SYS + x * NR, NR)
            r = R[at] - a_pl * Q[at]
            R[at] = r
            acc = acc + fold(r * r)
        reduce_start(0, c, acc)

        def step_x(x, carry):
            X[rows(x, c)] = X[rows(x, c)] + a_pl * PB[pl.ds(pl.multiple_of(c * PSYS + x * PR + 8, 8), NR)]
            return carry
        lax.fori_loop(0, NP, step_x, 0, unroll=4)

        @pl.when(k == ITERS - 1)
        def _():
            outs[c].start()
        reduce_sent(1, c)

    def body(k, carry):
        par = k % 2
        first_half(0, k, par)

        @pl.when(k == 0)
        def _():
            for cp in r_copies(1):
                cp.wait_recv()

        @pl.when(k > 0)
        def _():
            halo_r(1, 1 - par)
            q_sent(1, 1 - par)
        turn_r(1)
        first_half(1, k, par)

        @pl.when(k == 0)
        def _():
            for c in range(2):
                for cp in r_copies(c):
                    cp.wait_send()
        second_half(0, k)
        halo_r(0, par)
        turn_r(0)
        second_half(1, k)
        q_sent(0, par)
        return carry

    lax.fori_loop(0, ITERS, body, 0)
    for c in range(2):
        reduce_arrived(0, c)
        note(c, ITERS, reduce_end(0, c))
        reduce_sent(0, c)
    for cp in q_copies(1, (ITERS - 1) % 2):
        cp.wait()
    hist_out[...] = jnp.sqrt(hist_s[...] * (1.0 / (128 * 128 * 128)))
    for cp in outs:
        cp.wait()


CHUNKS = 2
VMEM_MAIN = 60 * 1024 * 1024


def unpack(xp, hist, x_out, hist_out, buf, st, hs, ho, in_sem, out_sem, h_sem):
    planes = NP // CHUNKS
    hist_in = pltpu.make_async_copy(hist, hs, h_sem.at[0])
    hist_in.start()
    loads = []
    for n in range(2 * CHUNKS):
        at = pl.ds(n * planes * NR, planes * NR)
        loads.append(pltpu.make_async_copy(xp.at[at], buf.at[at], in_sem.at[n]))
        loads[n].start()
    stores = []
    for n in range(2 * CHUNKS):
        c, x0 = n // CHUNKS, n % CHUNKS * planes
        loads[n].wait()

        def plane(x, carry):
            val = buf[pl.ds(pl.multiple_of(n * planes * NR + x * NR, 8), NR)]
            st[c, x0 + x] = val[:, :64]
            st[c, x0 + x + NP] = roll(val, 64)[:, :64]
            return carry
        lax.fori_loop(0, planes, plane, 0, unroll=16)
        for h in range(2):
            at = pl.ds(x0 + NP * h, planes)
            stores.append(pltpu.make_async_copy(st.at[c, at], x_out.at[c, at], out_sem.at[n, h]))
            stores[-1].start()
    hist_in.wait()
    ho[...] = hs[:2, :ITERS + 1]
    stores.append(pltpu.make_async_copy(ho, hist_out, h_sem.at[1]))
    stores[-1].start()
    for cp in stores:
        cp.wait()


def run(s, b, x0, kx, ky, kz):
    v = lambda *shape: pltpu.VMEM(shape, F32)
    sem = lambda *shape: pltpu.SemaphoreType.DMA(shape)
    scratch = [v(2, 64, 64, 64)] * 6
    full = v(2 * SYS, LN)
    scratch += [full, full, full, v(2 * PSYS, LN), full, full, full, v(2, NR, LN), v(2 * KSYS, LN), full, full, full, v(2, 32, LN)]
    scratch += [v(2, NR, LN), v(2, 32, LN), v(2, 32, LN)] * 2
    scratch += [v(2, 32, LN)] * 8
    scratch += [v(2, NR, LN), v(2, 32, LN), v(2, 32, LN), v(2, NR, LN), v(2, 32, LN)]
    scratch += [v(2, 2, NR, LN), v(2, 2, 32, LN), v(2, 2, 32, LN)]
    scratch += [v(2, 2, 8, 1, LN), v(2, 8, LN), v(2, 8, LN), v(8, LN)]
    scratch += [sem(6, 2), sem(2, 6), sem(2, 6), sem(2, 3), sem(2, 3), sem(2, 3), sem(2, 2, 3), sem(2, 2, 8), sem(2, 2, 8), sem(2)]
    xp, hist = pl.pallas_call(
        kernel,
        out_shape=(jax.ShapeDtypeStruct((2 * SYS, LN), F32), jax.ShapeDtypeStruct((8, LN), F32)),
        in_specs=[pl.BlockSpec(memory_space=pl.ANY)] * 6,
        out_specs=(pl.BlockSpec(memory_space=pl.ANY), pl.BlockSpec(memory_space=pltpu.VMEM)),
        scratch_shapes=scratch,
        compiler_params=pltpu.CompilerParams(collective_id=0, has_side_effects=True, vmem_limit_bytes=VMEM_MAIN),
        name='cg',
    )(s, b, x0, kx, ky, kz)
    return pl.pallas_call(
        unpack,
        out_shape=(jax.ShapeDtypeStruct((2, 64, 64, 64), F32), jax.ShapeDtypeStruct((2, ITERS + 1), F32)),
        in_specs=[pl.BlockSpec(memory_space=pl.ANY)] * 2,
        out_specs=[pl.BlockSpec(memory_space=pl.ANY)] * 2,
        scratch_shapes=[v(2 * SYS, LN), v(2, 64, 64, 64), v(8, LN), v(2, ITERS + 1), sem(2 * CHUNKS), sem(2 * CHUNKS, 2), sem(2)],
        compiler_params=pltpu.CompilerParams(vmem_limit_bytes=60 * 1024 * 1024),
        name='unpack',
    )(xp, hist)


def solution(mesh):
    field = P(None, 'px', 'py', 'pz')
    return jax.shard_map(run, mesh=mesh, in_specs=(field,) * 6, out_specs=(field, P(None, None)), check_vma=False)
```

```python
import jax
import jax.numpy as jnp
from jax import lax
from jax.experimental import pallas as pl
from jax.experimental.pallas import tpu as pltpu
from jax.sharding import PartitionSpec as P

ITERS = 20
F32 = jnp.float32
MESH = pl.DeviceIdType.MESH

NP = 32
NR = 64
LN = 128
PR = 80
KR = 72
SYS = NP * NR
PSYS = (NP + 1) * PR
KSYS = NP * KR
IN_FLIGHT = 3
AHEAD = 3


def roll(val, shift):
    if isinstance(shift, int):
        shift = shift % LN
    return pltpu.roll(val, shift, 1)


def kernel(s_hbm, b_hbm, x0_hbm, kx_hbm, ky_hbm, kz_hbm, x_out, hist_out,
           st_s, st_b, st_x, st_kx, st_ky, st_kz,
           X, R, Q, PB, PZ, RZ, KX, KXM, KY, KYL, KZ, KZF, D, KF,
           ix, iy, iz, jx, jy, jz, sxy, sxz, sky, skz, sy, sz, sry, srz,
           rhx, rhy, rhz, phx, phy, qhx, qhy, qhz,
           red, rho_s, alpha_s, hist_s,
           ld_sem, isend, irecv, rsend, rrecv, qsend, qrecv, dsend, drecv, out_sem):
    pz, py, px = lax.axis_index('pz'), lax.axis_index('py'), lax.axis_index('px')
    nbr = {'x': (pz, py, 1 - px), 'y': (pz, 1 - py, px), 'z': (1 - pz, py, px)}
    others = {}
    for m in range(1, 8):
        others[m] = (1 - pz if m & 4 else pz, 1 - py if m & 2 else py, 1 - px if m & 1 else px)

    lane = lax.broadcasted_iota(jnp.int32, (8, LN), 1)
    row8 = lax.broadcasted_iota(jnp.int32, (8, LN), 0)

    def lanes(n):
        return lax.broadcasted_iota(jnp.int32, (n, LN), 1)

    zf = 63 * (1 - pz)
    xf = 31 * (1 - px)
    yf = 63 * (1 - py)
    hrow = 72 - 65 * py
    to_z = 127 - 126 * pz
    fro_z = 1 + 126 * pz

    def face_mask(n):
        return (lanes(n) % 64) == zf

    def splits(n):
        return lanes(n) < 64

    order = [(num, c) for c in range(2) for num in range(6)]
    pairs = ((x0_hbm, st_x), (kz_hbm, st_kz), (ky_hbm, st_ky), (kx_hbm, st_kx), (s_hbm, st_s), (b_hbm, st_b))
    loads = [pltpu.make_async_copy(pairs[num][0].at[c], pairs[num][1].at[c], ld_sem.at[num, c]) for num, c in order]
    for cp in loads[:IN_FLIGHT]:
        cp.start()

    def loaded(num, c):
        n = c * 6 + num
        loads[n].wait()
        if n + IN_FLIGHT < len(loads):
            loads[n + IN_FLIGHT].start()

    barrier = pltpu.get_barrier_semaphore()
    for m in range(1, 8):
        pl.semaphore_signal(barrier, inc=1, device_id=others[m], device_id_type=MESH)

    def packed(st, c, x):
        return jnp.concatenate([st[c, x], st[c, x + NP]], axis=1)

    def pick(T, val, x, f):
        l64 = lanes(32) % 64
        T = jnp.where(l64 == x, roll(val[:32], lax.rem(x - f + LN, LN)), T)
        return jnp.where(l64 == x + 32, roll(val[32:], lax.rem(x + 32 - f + LN, LN)), T)

    def spread(G, x, f):
        return jnp.concatenate([roll(G, lax.rem(f - x + LN, LN)), roll(G, lax.rem(f - x - 32 + LN, LN))], axis=0)

    zero32 = jnp.zeros((32, LN), F32)

    def remote(src, dst, send_sem, recv_sem, dev):
        return pltpu.make_async_remote_copy(src_ref=src, dst_ref=dst, send_sem=send_sem, recv_sem=recv_sem, device_id=dev, device_id_type=MESH)

    def x_plane(ref, c):
        return ref.at[pl.ds(pl.multiple_of(c * SYS + xf * NR, 8), NR)]

    def rows(x, c):
        return pl.ds(pl.multiple_of(c * SYS + x * NR, 8), NR)

    first = []
    for c in range(2):
        first.append([
            remote(sxz.at[c], iz.at[c], isend.at[c, 0], irecv.at[c, 0], nbr['z']),
            remote(sxy.at[c], iy.at[c], isend.at[c, 1], irecv.at[c, 1], nbr['y']),
            remote(x_plane(X, c), ix.at[c], isend.at[c, 2], irecv.at[c, 2], nbr['x']),
            remote(skz.at[c], jz.at[c], isend.at[c, 3], irecv.at[c, 3], nbr['z']),
            remote(sky.at[c], jy.at[c], isend.at[c, 4], irecv.at[c, 4], nbr['y']),
            remote(KX.at[pl.ds(c * SYS + 31 * NR, NR)], jx.at[c], isend.at[c, 5], irecv.at[c, 5], nbr['x'])])

    def prepare_x0(c):
        loaded(0, c)

        def pack_x(x, T):
            u = packed(st_x, c, x)
            X[rows(x, c)] = u
            base = pl.multiple_of(c * PSYS + x * PR, 8)
            PB[pl.ds(base, 8)] = jnp.zeros((8, LN), F32)
            PB[pl.ds(base + 72, 8)] = jnp.zeros((8, LN), F32)
            PB[pl.ds(base + 8, NR)] = u
            return pick(T, u, x, zf)
        sxz[c] = lax.fori_loop(0, NP, pack_x, zero32, unroll=8)
        sxy[c] = X[pl.ds(c * SYS + yf, 32, stride=NR)]

    def prepare_kz(c):
        loaded(1, c)

        def pack_z(x, T):
            u = packed(st_kz, c, x)
            inner = jnp.where(lanes(NR) % 64 == 63, 0.0, u)
            moved = roll(inner, 1)
            KZ[rows(x, c)] = jnp.where(pz == 1, moved, inner)
            KZF[rows(x, c)] = jnp.where(pz == 1, inner, moved)
            return pick(T, u, x, 63)
        skz[c] = lax.fori_loop(0, NP, pack_z, zero32, unroll=8)

    def prepare_ky(c):
        loaded(2, c)

        def pack_ky(x, carry):
            u = packed(st_ky, c, x)
            row = lax.broadcasted_iota(jnp.int32, (NR, LN), 0)
            u = jnp.where(jnp.logical_and(row == NR - 1, py == 1), 0.0, u)
            KY[pl.ds(pl.multiple_of(c * KSYS + x * KR + 8, 8), NR)] = u
            return carry
        lax.fori_loop(0, NP, pack_ky, 0, unroll=8)
        sky[c] = KY[pl.ds(c * KSYS + 71, 32, stride=KR)]

    def prepare_kx(c):
        loaded(3, c)

        def pack_kx(x, carry):
            KX[rows(x, c)] = packed(st_kx, c, x)
            return carry
        lax.fori_loop(0, NP, pack_kx, 0, unroll=8)
        last = KX[pl.ds(c * SYS + 31 * NR, NR)]
        edge = jnp.logical_and(lanes(NR) >= 64, px == 1)
        KX[pl.ds(c * SYS + 31 * NR, NR)] = jnp.where(edge, 0.0, last)

    def prepare_sb(c):
        loaded(4, c)
        loaded(5, c)

        def pack_sb(x, carry):
            D[rows(x, c)] = packed(st_s, c, x)
            R[rows(x, c)] = packed(st_b, c, x)
            return carry
        lax.fori_loop(0, NP, pack_sb, 0, unroll=8)

    prepare_x0(0)
    pl.semaphore_wait(barrier, 7)
    for cp in first[0][:3]:
        cp.start()
    prepare_kz(0)
    first[0][3].start()
    prepare_ky(0)
    first[0][4].start()
    prepare_kx(0)
    first[0][5].start()
    prepare_sb(0)
    prepare_x0(1)
    for cp in first[1][:3]:
        cp.start()
    prepare_kz(1)
    first[1][3].start()
    prepare_ky(1)
    first[1][4].start()

    def reduce_copies(kind, c):
        return [remote(red.at[kind, c, 0], red.at[kind, c, m], dsend.at[kind, c, m], drecv.at[kind, c, m], others[m]) for m in (7, 6, 5, 4, 3, 2, 1)]

    def reduce_start(kind, c, part):
        red[kind, c, 0] = jnp.sum(part, axis=0, keepdims=True)
        for cp in reduce_copies(kind, c):
            cp.start()

    def reduce_end(kind, c):
        for cp in reduce_copies(kind, c):
            cp.wait_recv()
        v = [red[kind, c, m] for m in range(8)]
        total = ((v[0] + v[1]) + (v[2] + v[3])) + ((v[4] + v[5]) + (v[6] + v[7]))
        total = jnp.broadcast_to(total, (8, LN))
        return jnp.broadcast_to(jnp.sum(total, axis=1, keepdims=True), (8, LN))

    def reduce_sent(kind, c):
        for cp in reduce_copies(kind, c):
            cp.wait_send()

    def fold(val):
        return jnp.sum(val.reshape(-1, 8, LN), axis=0)

    def wide(vec, n):
        return jnp.broadcast_to(vec[None], (n // 8, 8, LN)).reshape(n, LN)

    def z_face(ref, c, to_sz, to_sy):
        def plane(x, T):
            return pick(T, ref[rows(x, c)], x, zf)
        to_sz[c] = lax.fori_loop(0, NP, plane, zero32, unroll=8)
        to_sy[c] = ref[pl.ds(c * SYS + yf, 32, stride=NR)]

    def turn_r(c):
        G = rhz[c]
        mask = face_mask(NR)

        def plane(x, carry):
            RZ[rows(x, c)] = jnp.where(mask, spread(G, x, zf), roll(R[rows(x, c)], to_z))
            return carry
        lax.fori_loop(0, NP, plane, 0, unroll=8)

    def r_copies(c):
        return [
            remote(srz.at[c], rhz.at[c], rsend.at[c, 0], rrecv.at[c, 0], nbr['z']),
            remote(sry.at[c], rhy.at[c], rsend.at[c, 1], rrecv.at[c, 1], nbr['y']),
            remote(x_plane(R, c), rhx.at[c], rsend.at[c, 2], rrecv.at[c, 2], nbr['x'])]

    def start(c):
        for cp in first[c]:
            cp.wait_recv()
        lo = splits(NR)
        kx_last = KX[pl.ds(c * SYS + 31 * NR, NR)]
        KXM[c] = roll(jnp.where(lo, kx_last, jnp.where(px == 1, jx[c], 0.0)), 64)
        KY[pl.ds(c * KSYS + 7, 32, stride=KR)] = jnp.where(py == 1, jy[c], 0.0)
        KF[c] = jnp.where(pz == 1, jz[c], skz[c])
        PB[pl.ds(c * PSYS + hrow, 32, stride=PR)] = iy[c]
        u_first = PB[pl.ds(c * PSYS + 8, NR)]
        u_last = PB[pl.ds(c * PSYS + 31 * PR + 8, NR)]
        PB[pl.ds(c * PSYS + 32 * PR + 8, NR)] = roll(jnp.where(lo, ix[c], u_first), 64)
        low = roll(jnp.where(lo, u_last, ix[c]), 64)
        kf, uf = KF[c], iz[c]
        mask = face_mask(NR)

        def start_plane(x, carry):
            acc, fx_prev, kx_prev, u = carry
            base = pl.multiple_of(c * PSYS + x * PR, 8)
            at = rows(x, c)
            kbase = pl.multiple_of(c * KSYS + x * KR, 8)
            nxt = PB[pl.ds(base + PR + 8, NR)]
            yu = PB[pl.ds(base + 9, NR)]
            yl = PB[pl.ds(base + 7, NR)]
            s = D[at]
            kxv = KX[at]
            kyv = KY[pl.ds(kbase + 8, NR)]
            kyl = KY[pl.ds(kbase + 7, NR)]
            kzf = jnp.where(mask, spread(kf, x, zf), KZ[at])
            uz = jnp.where(mask, spread(uf, x, zf), roll(u, to_z))
            fx = kxv * (u - nxt)
            fz = kzf * (u - uz)
            fz_away = roll(jnp.where(mask, 0.0, fz), fro_z)
            D[at] = s + (kxv + kx_prev) + (kyv + kyl) + (kzf + KZF[at])
            KZF[at] = kzf
            KYL[at] = kyl
            PZ[at] = uz
            r = R[at] - (s * u + (fx - fx_prev) + (kyv * (u - yu) - kyl * (yl - u)) + (fz - fz_away))
            R[at] = r
            return acc + fold(r * r), fx, kxv, nxt
        init = (jnp.zeros((8, LN), F32), KXM[c] * (low - u_first), KXM[c], u_first)
        acc = lax.fori_loop(0, NP, start_plane, init, unroll=4)[0]
        reduce_start(0, c, acc)
        z_face(R, c, srz, sry)
        for cp in r_copies(c):
            cp.start()

    start(0)
    prepare_kx(1)
    first[1][5].start()
    prepare_sb(1)
    start(1)
    hist_s[...] = jnp.zeros((8, LN), F32)
    for c in range(2):
        phx[c] = jnp.zeros((NR, LN), F32)
        phy[c] = zero32
        for cp in first[c]:
            cp.wait_send()
    for cp in r_copies(0):
        cp.wait_recv()
    turn_r(0)

    def q_copies(c, par):
        return [
            remote(sz.at[c], qhz.at[par, c], qsend.at[c, 0], qrecv.at[par, c, 0], nbr['z']),
            remote(sy.at[c], qhy.at[par, c], qsend.at[c, 1], qrecv.at[par, c, 1], nbr['y']),
            remote(x_plane(Q, c), qhx.at[par, c], qsend.at[c, 2], qrecv.at[par, c, 2], nbr['x'])]

    def note(c, k, rho):
        hist_s[...] = jnp.where(jnp.logical_and(lane == k, row8 == c), rho, hist_s[...])

    def product(c, beta):
        b64 = wide(beta, NR)
        hx = rhx[c] + b64 * phx[c]
        hy = rhy[c] + wide(beta, 32) * phy[c]
        phx[c] = hx
        phy[c] = hy
        PB[pl.ds(c * PSYS + hrow, 32, stride=PR)] = hy
        lo = splits(NR)

        def direction(x):
            at = pl.ds(c * PSYS + x * PR + 8, NR)
            val = R[pl.ds(c * SYS + x * NR, NR)] + b64 * PB[at]
            PB[at] = val
            return val

        def turn(x, p):
            return roll(KZ[pl.ds(c * SYS + x * NR, NR)] * p, fro_z)

        def load_p(x):
            return PB[pl.ds(c * PSYS + x * PR + 8, NR)]

        p_last = direction(NP - 1)
        p_first = direction(0)
        above = roll(jnp.where(lo, hx, p_first), 64)
        below = roll(jnp.where(lo, p_last, hx), 64)
        turned = {0: turn(0, p_first)}
        for x in range(1, AHEAD):
            turned[x] = turn(x, direction(x))
        cur, kxp_prev = p_first, KXM[c] * below
        acc = jnp.zeros((8, LN), F32)
        for x in range(NP):
            w = x + AHEAD
            if w < NP:
                turned[w] = turn(w, direction(w) if w < NP - 1 else load_p(w))
            nxt = load_p(x + 1) if x + 1 < NP else above
            base = c * PSYS + x * PR
            at = pl.ds(c * SYS + x * NR, NR)
            kbase = c * KSYS + x * KR
            kxv = KX[at]
            kxp = kxv * cur
            q = D[at] * cur - kxp_prev - kxv * nxt
            q = q - KY[pl.ds(kbase + 8, NR)] * PB[pl.ds(base + 9, NR)]
            q = q - KYL[at] * PB[pl.ds(base + 7, NR)]
            pz_new = RZ[at] + b64 * PZ[at]
            PZ[at] = pz_new
            q = q - KZF[at] * pz_new - turned.pop(x)
            Q[at] = q
            acc = acc + fold(cur * q)
            cur, kxp_prev = nxt, kxp
        return acc

    outs = [pltpu.make_async_copy(X.at[pl.ds(c * SYS, SYS)], x_out.at[pl.ds(c * SYS, SYS)], out_sem.at[c]) for c in range(2)]

    def halo_r(c, par):
        for cp in q_copies(c, par):
            cp.wait_recv()
        alpha = alpha_s[c]
        rhx[c] = rhx[c] - wide(alpha, NR) * qhx[par, c]
        rhy[c] = rhy[c] - wide(alpha, 32) * qhy[par, c]
        rhz[c] = rhz[c] - wide(alpha, 32) * qhz[par, c]

    def q_sent(c, par):
        for cp in q_copies(c, par):
            cp.wait_send()

    def first_half(c, k, par):
        rho = reduce_end(0, c)
        note(c, k, rho)
        beta = jnp.where(k == 0, 0.0, rho / rho_s[c])
        rho_s[c] = rho
        reduce_start(1, c, product(c, beta))
        reduce_sent(0, c)
        z_face(Q, c, sz, sy)
        for cp in q_copies(c, par):
            cp.start()

    def second_half(c, k):
        alpha = rho_s[c] / reduce_end(1, c)
        alpha_s[c] = alpha
        a_pl = wide(alpha, NR)
        acc = jnp.zeros((8, LN), F32)
        for x in range(NP):
            at = pl.ds(c * SYS + x * NR, NR)
            r = R[at] - a_pl * Q[at]
            R[at] = r
            acc = acc + fold(r * r)
        reduce_start(0, c, acc)

        def step_x(x, carry):
            X[rows(x, c)] = X[rows(x, c)] + a_pl * PB[pl.ds(pl.multiple_of(c * PSYS + x * PR + 8, 8), NR)]
            return carry
        lax.fori_loop(0, NP, step_x, 0, unroll=4)

        @pl.when(k == ITERS - 1)
        def _():
            outs[c].start()
        reduce_sent(1, c)

    def body(k, carry):
        par = k % 2
        first_half(0, k, par)

        @pl.when(k == 0)
        def _():
            for cp in r_copies(1):
                cp.wait_recv()

        @pl.when(k > 0)
        def _():
            halo_r(1, 1 - par)
            q_sent(1, 1 - par)
        turn_r(1)
        first_half(1, k, par)

        @pl.when(k == 0)
        def _():
            for c in range(2):
                for cp in r_copies(c):
                    cp.wait_send()
        second_half(0, k)
        halo_r(0, par)
        turn_r(0)
        second_half(1, k)
        q_sent(0, par)
        return carry

    lax.fori_loop(0, ITERS, body, 0)
    for c in range(2):
        note(c, ITERS, reduce_end(0, c))
        reduce_sent(0, c)
    for cp in q_copies(1, (ITERS - 1) % 2):
        cp.wait()
    hist_out[...] = jnp.sqrt(hist_s[...] * (1.0 / (128 * 128 * 128)))
    for cp in outs:
        cp.wait()


CHUNKS = 2
VMEM_MAIN = 60 * 1024 * 1024


def unpack(xp, hist, x_out, hist_out, buf, st, hs, ho, in_sem, out_sem, h_sem):
    planes = NP // CHUNKS
    hist_in = pltpu.make_async_copy(hist, hs, h_sem.at[0])
    hist_in.start()
    loads = []
    for n in range(2 * CHUNKS):
        at = pl.ds(n * planes * NR, planes * NR)
        loads.append(pltpu.make_async_copy(xp.at[at], buf.at[at], in_sem.at[n]))
        loads[n].start()
    stores = []
    for n in range(2 * CHUNKS):
        c, x0 = n // CHUNKS, n % CHUNKS * planes
        loads[n].wait()

        def plane(x, carry):
            val = buf[pl.ds(pl.multiple_of(n * planes * NR + x * NR, 8), NR)]
            st[c, x0 + x] = val[:, :64]
            st[c, x0 + x + NP] = roll(val, 64)[:, :64]
            return carry
        lax.fori_loop(0, planes, plane, 0, unroll=16)
        for h in range(2):
            at = pl.ds(x0 + NP * h, planes)
            stores.append(pltpu.make_async_copy(st.at[c, at], x_out.at[c, at], out_sem.at[n, h]))
            stores[-1].start()
    hist_in.wait()
    ho[...] = hs[:2, :ITERS + 1]
    stores.append(pltpu.make_async_copy(ho, hist_out, h_sem.at[1]))
    stores[-1].start()
    for cp in stores:
        cp.wait()


def run(s, b, x0, kx, ky, kz):
    v = lambda *shape: pltpu.VMEM(shape, F32)
    sem = lambda *shape: pltpu.SemaphoreType.DMA(shape)
    scratch = [v(2, 64, 64, 64)] * 6
    full = v(2 * SYS, LN)
    scratch += [full, full, full, v(2 * PSYS, LN), full, full, full, v(2, NR, LN), v(2 * KSYS, LN), full, full, full, full, v(2, 32, LN)]
    scratch += [v(2, NR, LN), v(2, 32, LN), v(2, 32, LN)] * 2
    scratch += [v(2, 32, LN)] * 8
    scratch += [v(2, NR, LN), v(2, 32, LN), v(2, 32, LN), v(2, NR, LN), v(2, 32, LN)]
    scratch += [v(2, 2, NR, LN), v(2, 2, 32, LN), v(2, 2, 32, LN)]
    scratch += [v(2, 2, 8, 1, LN), v(2, 8, LN), v(2, 8, LN), v(8, LN)]
    scratch += [sem(6, 2), sem(2, 6), sem(2, 6), sem(2, 3), sem(2, 3), sem(2, 3), sem(2, 2, 3), sem(2, 2, 8), sem(2, 2, 8), sem(2)]
    xp, hist = pl.pallas_call(
        kernel,
        out_shape=(jax.ShapeDtypeStruct((2 * SYS, LN), F32), jax.ShapeDtypeStruct((8, LN), F32)),
        in_specs=[pl.BlockSpec(memory_space=pl.ANY)] * 6,
        out_specs=(pl.BlockSpec(memory_space=pl.ANY), pl.BlockSpec(memory_space=pltpu.VMEM)),
        scratch_shapes=scratch,
        compiler_params=pltpu.CompilerParams(collective_id=0, has_side_effects=True, vmem_limit_bytes=VMEM_MAIN),
        name='cg',
    )(s, b, x0, kx, ky, kz)
    return pl.pallas_call(
        unpack,
        out_shape=(jax.ShapeDtypeStruct((2, 64, 64, 64), F32), jax.ShapeDtypeStruct((2, ITERS + 1), F32)),
        in_specs=[pl.BlockSpec(memory_space=pl.ANY)] * 2,
        out_specs=[pl.BlockSpec(memory_space=pl.ANY)] * 2,
        scratch_shapes=[v(2 * SYS, LN), v(2, 64, 64, 64), v(8, LN), v(2, ITERS + 1), sem(2 * CHUNKS), sem(2 * CHUNKS, 2), sem(2)],
        compiler_params=pltpu.CompilerParams(vmem_limit_bytes=60 * 1024 * 1024),
        name='unpack',
    )(xp, hist)


def solution(mesh):
    field = P(None, 'px', 'py', 'pz')
    return jax.shard_map(run, mesh=mesh, in_specs=(field,) * 6, out_specs=(field, P(None, None)), check_vma=False)
```

```python
import jax
import jax.numpy as jnp
from jax import lax
from jax.experimental import pallas as pl
from jax.experimental.pallas import tpu as pltpu
from jax.sharding import PartitionSpec as P

ITERS = 20
F32 = jnp.float32
MESH = pl.DeviceIdType.MESH

NP = 32
NR = 64
LN = 128
PR = 80
KR = 72
SYS = NP * NR
PSYS = (NP + 1) * PR
KSYS = NP * KR
IN_FLIGHT = 3
AHEAD = 3


def roll(val, shift):
    if isinstance(shift, int):
        shift = shift % LN
    return pltpu.roll(val, shift, 1)


def kernel(s_hbm, b_hbm, x0_hbm, kx_hbm, ky_hbm, kz_hbm, X, hist_out,
           st_s, st_b, st_x, st_kx, st_ky, st_kz,
           R, Q, PB, PZ, RZ, KX, KXM, KY, KZ, KZF, D, KF,
           ix, iy, iz, jx, jy, jz, sxy, sxz, sky, skz, sy, sz, sry, srz,
           rhx, rhy, rhz, phx, phy, qhx, qhy, qhz,
           red, rho_s, alpha_s, hist_s,
           ld_sem, isend, irecv, rsend, rrecv, qsend, qrecv, dsend, drecv):
    pz, py, px = lax.axis_index('pz'), lax.axis_index('py'), lax.axis_index('px')
    nbr = {'x': (pz, py, 1 - px), 'y': (pz, 1 - py, px), 'z': (1 - pz, py, px)}
    others = {}
    for m in range(1, 8):
        others[m] = (1 - pz if m & 4 else pz, 1 - py if m & 2 else py, 1 - px if m & 1 else px)

    lane = lax.broadcasted_iota(jnp.int32, (8, LN), 1)
    row8 = lax.broadcasted_iota(jnp.int32, (8, LN), 0)

    def lanes(n):
        return lax.broadcasted_iota(jnp.int32, (n, LN), 1)

    zf = 63 * (1 - pz)
    xf = 31 * (1 - px)
    yf = 63 * (1 - py)
    hrow = 72 - 65 * py
    to_z = 127 - 126 * pz
    fro_z = 1 + 126 * pz

    def face_mask(n):
        return (lanes(n) % 64) == zf

    def splits(n):
        return lanes(n) < 64

    order = [(num, c) for c in range(2) for num in range(6)]
    pairs = ((x0_hbm, st_x), (kz_hbm, st_kz), (ky_hbm, st_ky), (kx_hbm, st_kx), (s_hbm, st_s), (b_hbm, st_b))
    loads = [pltpu.make_async_copy(pairs[num][0].at[c], pairs[num][1].at[c], ld_sem.at[num, c]) for num, c in order]
    for cp in loads[:IN_FLIGHT]:
        cp.start()

    def loaded(num, c):
        n = c * 6 + num
        loads[n].wait()
        if n + IN_FLIGHT < len(loads):
            loads[n + IN_FLIGHT].start()

    barrier = pltpu.get_barrier_semaphore()
    for m in range(1, 8):
        pl.semaphore_signal(barrier, inc=1, device_id=others[m], device_id_type=MESH)

    def packed(st, c, x):
        return jnp.concatenate([st[c, x], st[c, x + NP]], axis=1)

    def pick(T, val, x, f):
        l64 = lanes(32) % 64
        T = jnp.where(l64 == x, roll(val[:32], lax.rem(x - f + LN, LN)), T)
        return jnp.where(l64 == x + 32, roll(val[32:], lax.rem(x + 32 - f + LN, LN)), T)

    def spread(G, x, f):
        return jnp.concatenate([roll(G, lax.rem(f - x + LN, LN)), roll(G, lax.rem(f - x - 32 + LN, LN))], axis=0)

    zero32 = jnp.zeros((32, LN), F32)

    def remote(src, dst, send_sem, recv_sem, dev):
        return pltpu.make_async_remote_copy(src_ref=src, dst_ref=dst, send_sem=send_sem, recv_sem=recv_sem, device_id=dev, device_id_type=MESH)

    def x_plane(ref, c):
        return ref.at[pl.ds(pl.multiple_of(c * SYS + xf * NR, 8), NR)]

    def rows(x, c):
        return pl.ds(pl.multiple_of(c * SYS + x * NR, 8), NR)

    first = []
    for c in range(2):
        first.append([
            remote(sxz.at[c], iz.at[c], isend.at[c, 0], irecv.at[c, 0], nbr['z']),
            remote(sxy.at[c], iy.at[c], isend.at[c, 1], irecv.at[c, 1], nbr['y']),
            remote(x_plane(X, c), ix.at[c], isend.at[c, 2], irecv.at[c, 2], nbr['x']),
            remote(skz.at[c], jz.at[c], isend.at[c, 3], irecv.at[c, 3], nbr['z']),
            remote(sky.at[c], jy.at[c], isend.at[c, 4], irecv.at[c, 4], nbr['y']),
            remote(KX.at[pl.ds(c * SYS + 31 * NR, NR)], jx.at[c], isend.at[c, 5], irecv.at[c, 5], nbr['x'])])

    def prepare_x0(c):
        loaded(0, c)

        def pack_x(x, T):
            u = packed(st_x, c, x)
            X[rows(x, c)] = u
            base = pl.multiple_of(c * PSYS + x * PR, 8)
            PB[pl.ds(base, 8)] = jnp.zeros((8, LN), F32)
            PB[pl.ds(base + 72, 8)] = jnp.zeros((8, LN), F32)
            PB[pl.ds(base + 8, NR)] = u
            return pick(T, u, x, zf)
        sxz[c] = lax.fori_loop(0, NP, pack_x, zero32, unroll=8)
        sxy[c] = X[pl.ds(c * SYS + yf, 32, stride=NR)]

    def prepare_kz(c):
        loaded(1, c)

        def pack_z(x, T):
            u = packed(st_kz, c, x)
            inner = jnp.where(lanes(NR) % 64 == 63, 0.0, u)
            moved = roll(inner, 1)
            KZ[rows(x, c)] = jnp.where(pz == 1, moved, inner)
            KZF[rows(x, c)] = jnp.where(pz == 1, inner, moved)
            return pick(T, u, x, 63)
        skz[c] = lax.fori_loop(0, NP, pack_z, zero32, unroll=8)

    def prepare_ky(c):
        loaded(2, c)

        def pack_ky(x, carry):
            u = packed(st_ky, c, x)
            row = lax.broadcasted_iota(jnp.int32, (NR, LN), 0)
            u = jnp.where(jnp.logical_and(row == NR - 1, py == 1), 0.0, u)
            KY[pl.ds(pl.multiple_of(c * KSYS + x * KR + 8, 8), NR)] = u
            return carry
        lax.fori_loop(0, NP, pack_ky, 0, unroll=8)
        sky[c] = KY[pl.ds(c * KSYS + 71, 32, stride=KR)]

    def prepare_kx(c):
        loaded(3, c)

        def pack_kx(x, carry):
            KX[rows(x, c)] = packed(st_kx, c, x)
            return carry
        lax.fori_loop(0, NP, pack_kx, 0, unroll=8)
        last = KX[pl.ds(c * SYS + 31 * NR, NR)]
        edge = jnp.logical_and(lanes(NR) >= 64, px == 1)
        KX[pl.ds(c * SYS + 31 * NR, NR)] = jnp.where(edge, 0.0, last)

    def prepare_sb(c):
        loaded(4, c)
        loaded(5, c)

        def pack_sb(x, carry):
            D[rows(x, c)] = packed(st_s, c, x)
            R[rows(x, c)] = packed(st_b, c, x)
            return carry
        lax.fori_loop(0, NP, pack_sb, 0, unroll=8)

    prepare_x0(0)
    pl.semaphore_wait(barrier, 7)
    for cp in first[0][:3]:
        cp.start()
    prepare_kz(0)
    first[0][3].start()
    prepare_ky(0)
    first[0][4].start()
    prepare_kx(0)
    first[0][5].start()
    prepare_sb(0)
    prepare_x0(1)
    for cp in first[1][:3]:
        cp.start()
    prepare_kz(1)
    first[1][3].start()
    prepare_ky(1)
    first[1][4].start()

    def reduce_copies(kind, c):
        return [remote(red.at[kind, c, 0], red.at[kind, c, m], dsend.at[kind, c, m], drecv.at[kind, c, m], others[m]) for m in (7, 6, 5, 4, 3, 2, 1)]

    def reduce_start(kind, c, part):
        red[kind, c, 0] = jnp.sum(part, axis=0, keepdims=True)
        for cp in reduce_copies(kind, c):
            cp.start()

    def reduce_end(kind, c):
        for cp in reduce_copies(kind, c):
            cp.wait_recv()
        v = [red[kind, c, m] for m in range(8)]
        total = ((v[0] + v[1]) + (v[2] + v[3])) + ((v[4] + v[5]) + (v[6] + v[7]))
        total = jnp.broadcast_to(total, (8, LN))
        return jnp.broadcast_to(jnp.sum(total, axis=1, keepdims=True), (8, LN))

    def reduce_sent(kind, c):
        for cp in reduce_copies(kind, c):
            cp.wait_send()

    def fold(val):
        return jnp.sum(val.reshape(-1, 8, LN), axis=0)

    def wide(vec, n):
        return jnp.broadcast_to(vec[None], (n // 8, 8, LN)).reshape(n, LN)

    def z_face(ref, c, to_sz, to_sy):
        def plane(x, T):
            return pick(T, ref[rows(x, c)], x, zf)
        to_sz[c] = lax.fori_loop(0, NP, plane, zero32, unroll=8)
        to_sy[c] = ref[pl.ds(c * SYS + yf, 32, stride=NR)]

    def turn_r(c):
        G = rhz[c]
        mask = face_mask(NR)

        def plane(x, carry):
            RZ[rows(x, c)] = jnp.where(mask, spread(G, x, zf), roll(R[rows(x, c)], to_z))
            return carry
        lax.fori_loop(0, NP, plane, 0, unroll=8)

    def r_copies(c):
        return [
            remote(srz.at[c], rhz.at[c], rsend.at[c, 0], rrecv.at[c, 0], nbr['z']),
            remote(sry.at[c], rhy.at[c], rsend.at[c, 1], rrecv.at[c, 1], nbr['y']),
            remote(x_plane(R, c), rhx.at[c], rsend.at[c, 2], rrecv.at[c, 2], nbr['x'])]

    def start(c):
        for cp in first[c]:
            cp.wait_recv()
        lo = splits(NR)
        kx_last = KX[pl.ds(c * SYS + 31 * NR, NR)]
        KXM[c] = roll(jnp.where(lo, kx_last, jnp.where(px == 1, jx[c], 0.0)), 64)
        KY[pl.ds(c * KSYS + 7, 32, stride=KR)] = jnp.where(py == 1, jy[c], 0.0)
        KF[c] = jnp.where(pz == 1, jz[c], skz[c])
        PB[pl.ds(c * PSYS + hrow, 32, stride=PR)] = iy[c]
        u_first = PB[pl.ds(c * PSYS + 8, NR)]
        u_last = PB[pl.ds(c * PSYS + 31 * PR + 8, NR)]
        PB[pl.ds(c * PSYS + 32 * PR + 8, NR)] = roll(jnp.where(lo, ix[c], u_first), 64)
        low = roll(jnp.where(lo, u_last, ix[c]), 64)
        kf, uf = KF[c], iz[c]
        mask = face_mask(NR)

        def start_plane(x, carry):
            acc, fx_prev, kx_prev, u = carry
            base = pl.multiple_of(c * PSYS + x * PR, 8)
            at = rows(x, c)
            kbase = pl.multiple_of(c * KSYS + x * KR, 8)
            nxt = PB[pl.ds(base + PR + 8, NR)]
            yu = PB[pl.ds(base + 9, NR)]
            yl = PB[pl.ds(base + 7, NR)]
            s = D[at]
            kxv = KX[at]
            kyv = KY[pl.ds(kbase + 8, NR)]
            kyl = KY[pl.ds(kbase + 7, NR)]
            kzf = jnp.where(mask, spread(kf, x, zf), KZ[at])
            uz = jnp.where(mask, spread(uf, x, zf), roll(u, to_z))
            fx = kxv * (u - nxt)
            fz = kzf * (u - uz)
            fz_away = roll(jnp.where(mask, 0.0, fz), fro_z)
            D[at] = s + (kxv + kx_prev) + (kyv + kyl) + (kzf + KZF[at])
            KZF[at] = kzf
            PZ[at] = uz
            r = R[at] - (s * u + (fx - fx_prev) + (kyv * (u - yu) - kyl * (yl - u)) + (fz - fz_away))
            R[at] = r
            return acc + fold(r * r), fx, kxv, nxt
        init = (jnp.zeros((8, LN), F32), KXM[c] * (low - u_first), KXM[c], u_first)
        acc = lax.fori_loop(0, NP, start_plane, init, unroll=4)[0]
        reduce_start(0, c, acc)
        z_face(R, c, srz, sry)
        for cp in r_copies(c):
            cp.start()

    start(0)
    prepare_kx(1)
    first[1][5].start()
    prepare_sb(1)
    start(1)
    hist_s[...] = jnp.zeros((8, LN), F32)
    for c in range(2):
        phx[c] = jnp.zeros((NR, LN), F32)
        phy[c] = zero32
        for cp in first[c]:
            cp.wait_send()
    for cp in r_copies(0):
        cp.wait_recv()
    turn_r(0)

    def q_copies(c, par):
        return [
            remote(sz.at[c], qhz.at[par, c], qsend.at[c, 0], qrecv.at[par, c, 0], nbr['z']),
            remote(sy.at[c], qhy.at[par, c], qsend.at[c, 1], qrecv.at[par, c, 1], nbr['y']),
            remote(x_plane(Q, c), qhx.at[par, c], qsend.at[c, 2], qrecv.at[par, c, 2], nbr['x'])]

    def note(c, k, rho):
        hist_s[...] = jnp.where(jnp.logical_and(lane == k, row8 == c), rho, hist_s[...])

    def product(c, beta):
        b64 = wide(beta, NR)
        hx = rhx[c] + b64 * phx[c]
        hy = rhy[c] + wide(beta, 32) * phy[c]
        phx[c] = hx
        phy[c] = hy
        PB[pl.ds(c * PSYS + hrow, 32, stride=PR)] = hy
        lo = splits(NR)

        def direction(x):
            at = pl.ds(c * PSYS + x * PR + 8, NR)
            val = R[pl.ds(c * SYS + x * NR, NR)] + b64 * PB[at]
            PB[at] = val
            return val

        def turn(x, p):
            return roll(KZ[pl.ds(c * SYS + x * NR, NR)] * p, fro_z)

        def load_p(x):
            return PB[pl.ds(c * PSYS + x * PR + 8, NR)]

        p_last = direction(NP - 1)
        p_first = direction(0)
        above = roll(jnp.where(lo, hx, p_first), 64)
        below = roll(jnp.where(lo, p_last, hx), 64)
        turned = {0: turn(0, p_first)}
        for x in range(1, AHEAD):
            turned[x] = turn(x, direction(x))
        cur, kxp_prev = p_first, KXM[c] * below
        acc = jnp.zeros((8, LN), F32)
        for x in range(NP):
            w = x + AHEAD
            if w < NP:
                turned[w] = turn(w, direction(w) if w < NP - 1 else load_p(w))
            nxt = load_p(x + 1) if x + 1 < NP else above
            base = c * PSYS + x * PR
            at = pl.ds(c * SYS + x * NR, NR)
            kbase = c * KSYS + x * KR
            kxv = KX[at]
            kxp = kxv * cur
            q = D[at] * cur - kxp_prev - kxv * nxt
            q = q - KY[pl.ds(kbase + 8, NR)] * PB[pl.ds(base + 9, NR)]
            q = q - KY[pl.ds(kbase + 7, NR)] * PB[pl.ds(base + 7, NR)]
            pz_new = RZ[at] + b64 * PZ[at]
            PZ[at] = pz_new
            q = q - KZF[at] * pz_new - turned.pop(x)
            Q[at] = q
            acc = acc + fold(cur * q)
            cur, kxp_prev = nxt, kxp
        return acc

    def halo_r(c, par):
        for cp in q_copies(c, par):
            cp.wait_recv()
        alpha = alpha_s[c]
        rhx[c] = rhx[c] - wide(alpha, NR) * qhx[par, c]
        rhy[c] = rhy[c] - wide(alpha, 32) * qhy[par, c]
        rhz[c] = rhz[c] - wide(alpha, 32) * qhz[par, c]

    def q_sent(c, par):
        for cp in q_copies(c, par):
            cp.wait_send()

    def first_half(c, k, par):
        rho = reduce_end(0, c)
        note(c, k, rho)
        beta = jnp.where(k == 0, 0.0, rho / rho_s[c])
        rho_s[c] = rho
        reduce_start(1, c, product(c, beta))
        reduce_sent(0, c)
        z_face(Q, c, sz, sy)
        for cp in q_copies(c, par):
            cp.start()

    def second_half(c, k):
        alpha = rho_s[c] / reduce_end(1, c)
        alpha_s[c] = alpha
        a_pl = wide(alpha, NR)
        acc = jnp.zeros((8, LN), F32)
        for x in range(NP):
            at = pl.ds(c * SYS + x * NR, NR)
            r = R[at] - a_pl * Q[at]
            R[at] = r
            acc = acc + fold(r * r)
        reduce_start(0, c, acc)

        def step_x(x, carry):
            X[rows(x, c)] = X[rows(x, c)] + a_pl * PB[pl.ds(pl.multiple_of(c * PSYS + x * PR + 8, 8), NR)]
            return carry
        lax.fori_loop(0, NP, step_x, 0, unroll=4)
        reduce_sent(1, c)

    def body(k, carry):
        par = k % 2
        first_half(0, k, par)

        @pl.when(k == 0)
        def _():
            for cp in r_copies(1):
                cp.wait_recv()

        @pl.when(k > 0)
        def _():
            halo_r(1, 1 - par)
            q_sent(1, 1 - par)
        turn_r(1)
        first_half(1, k, par)

        @pl.when(k == 0)
        def _():
            for c in range(2):
                for cp in r_copies(c):
                    cp.wait_send()
        second_half(0, k)
        halo_r(0, par)
        turn_r(0)
        second_half(1, k)
        q_sent(0, par)
        return carry

    lax.fori_loop(0, ITERS, body, 0)
    for c in range(2):
        note(c, ITERS, reduce_end(0, c))
        reduce_sent(0, c)
    for cp in q_copies(1, (ITERS - 1) % 2):
        cp.wait()
    hist_out[...] = jnp.sqrt(hist_s[...] * (1.0 / (128 * 128 * 128)))


CHUNKS = 4
VMEM_MAIN = 54 * 1024 * 1024


def unpack(buf, hist, x_out, hist_out, st, ho, out_sem, h_sem):
    planes = NP // CHUNKS
    ho[...] = hist[:2, :ITERS + 1]
    stores = [pltpu.make_async_copy(ho, hist_out, h_sem)]
    stores[0].start()
    for n in range(2 * CHUNKS):
        c, x0 = n // CHUNKS, n % CHUNKS * planes

        def plane(x, carry):
            val = buf[pl.ds(pl.multiple_of(n * planes * NR + x * NR, 8), NR)]
            st[c, x0 + x] = val[:, :64]
            st[c, x0 + x + NP] = roll(val, 64)[:, :64]
            return carry
        lax.fori_loop(0, planes, plane, 0, unroll=8)
        for h in range(2):
            at = pl.ds(x0 + NP * h, planes)
            stores.append(pltpu.make_async_copy(st.at[c, at], x_out.at[c, at], out_sem.at[n, h]))
            stores[-1].start()
    for cp in stores:
        cp.wait()


def run(s, b, x0, kx, ky, kz):
    v = lambda *shape: pltpu.VMEM(shape, F32)
    sem = lambda *shape: pltpu.SemaphoreType.DMA(shape)
    scratch = [v(2, 64, 64, 64)] * 6
    full = v(2 * SYS, LN)
    scratch += [full, full, v(2 * PSYS, LN), full, full, full, v(2, NR, LN), v(2 * KSYS, LN), full, full, full, v(2, 32, LN)]
    scratch += [v(2, NR, LN), v(2, 32, LN), v(2, 32, LN)] * 2
    scratch += [v(2, 32, LN)] * 8
    scratch += [v(2, NR, LN), v(2, 32, LN), v(2, 32, LN), v(2, NR, LN), v(2, 32, LN)]
    scratch += [v(2, 2, NR, LN), v(2, 2, 32, LN), v(2, 2, 32, LN)]
    scratch += [v(2, 2, 8, 1, LN), v(2, 8, LN), v(2, 8, LN), v(8, LN)]
    scratch += [sem(6, 2), sem(2, 6), sem(2, 6), sem(2, 3), sem(2, 3), sem(2, 3), sem(2, 2, 3), sem(2, 2, 8), sem(2, 2, 8)]
    xp, hist = pl.pallas_call(
        kernel,
        out_shape=(pltpu.VMEM((2 * SYS, LN), F32), pltpu.VMEM((8, LN), F32)),
        in_specs=[pl.BlockSpec(memory_space=pl.ANY)] * 6,
        out_specs=(pl.BlockSpec(memory_space=pltpu.VMEM), pl.BlockSpec(memory_space=pltpu.VMEM)),
        scratch_shapes=scratch,
        compiler_params=pltpu.CompilerParams(collective_id=0, has_side_effects=True, vmem_limit_bytes=VMEM_MAIN),
        name='cg',
    )(s, b, x0, kx, ky, kz)
    return pl.pallas_call(
        unpack,
        out_shape=(jax.ShapeDtypeStruct((2, 64, 64, 64), F32), jax.ShapeDtypeStruct((2, ITERS + 1), F32)),
        in_specs=[pl.BlockSpec(memory_space=pltpu.VMEM)] * 2,
        out_specs=[pl.BlockSpec(memory_space=pl.ANY)] * 2,
        scratch_shapes=[v(2, 64, 64, 64), v(2, ITERS + 1), sem(2 * CHUNKS, 2), pltpu.SemaphoreType.DMA],
        compiler_params=pltpu.CompilerParams(vmem_limit_bytes=12 * 1024 * 1024),
        name='unpack',
    )(xp, hist)


def solution(mesh):
    field = P(None, 'px', 'py', 'pz')
    return jax.shard_map(run, mesh=mesh, in_specs=(field,) * 6, out_specs=(field, P(None, None)), check_vma=False)
```

```python
import jax
import jax.numpy as jnp
from jax import lax
from jax.experimental import pallas as pl
from jax.experimental.pallas import tpu as pltpu
from jax.sharding import PartitionSpec as P

ITERS = 20
F32 = jnp.float32
MESH = pl.DeviceIdType.MESH

NP = 32
NR = 64
LN = 128
PR = 80
KR = 72
SYS = NP * NR
PSYS = (NP + 1) * PR
KSYS = NP * KR
IN_FLIGHT = 3
AHEAD = 3


def roll(val, shift):
    if isinstance(shift, int):
        shift = shift % LN
    return pltpu.roll(val, shift, 1)


def kernel(s_hbm, b_hbm, x0_hbm, kx_hbm, ky_hbm, kz_hbm, X, hist_out,
           st_s, st_b, st_x, st_kx, st_ky, st_kz,
           R, Q, PB, PZ, RZ, KX, KXM, KY, KZ, KZF, D, KF,
           ix, iy, iz, jx, jy, jz, sxy, sxz, sky, skz, sy, sz, sry, srz,
           rhx, rhy, rhz, phx, phy, qhx, qhy, qhz,
           red, rho_s, alpha_s, hist_s,
           ld_sem, isend, irecv, rsend, rrecv, qsend, qrecv, dsend, drecv):
    pz, py, px = lax.axis_index('pz'), lax.axis_index('py'), lax.axis_index('px')
    nbr = {'x': (pz, py, 1 - px), 'y': (pz, 1 - py, px), 'z': (1 - pz, py, px)}
    others = {}
    for m in range(1, 8):
        others[m] = (1 - pz if m & 4 else pz, 1 - py if m & 2 else py, 1 - px if m & 1 else px)

    lane = lax.broadcasted_iota(jnp.int32, (8, LN), 1)
    row8 = lax.broadcasted_iota(jnp.int32, (8, LN), 0)

    def lanes(n):
        return lax.broadcasted_iota(jnp.int32, (n, LN), 1)

    zf = 63 * (1 - pz)
    xf = 31 * (1 - px)
    yf = 63 * (1 - py)
    hrow = 72 - 65 * py
    to_z = 127 - 126 * pz
    fro_z = 1 + 126 * pz

    def face_mask(n):
        return (lanes(n) % 64) == zf

    def splits(n):
        return lanes(n) < 64

    order = [(num, c) for c in range(2) for num in range(6)]
    pairs = ((x0_hbm, st_x), (kz_hbm, st_kz), (ky_hbm, st_ky), (kx_hbm, st_kx), (s_hbm, st_s), (b_hbm, st_b))
    loads = [pltpu.make_async_copy(pairs[num][0].at[c], pairs[num][1].at[c], ld_sem.at[num, c]) for num, c in order]
    for cp in loads[:IN_FLIGHT]:
        cp.start()

    def loaded(num, c):
        n = c * 6 + num
        loads[n].wait()
        if n + IN_FLIGHT < len(loads):
            loads[n + IN_FLIGHT].start()

    barrier = pltpu.get_barrier_semaphore()
    for m in range(1, 8):
        pl.semaphore_signal(barrier, inc=1, device_id=others[m], device_id_type=MESH)

    def packed(st, c, x):
        return jnp.concatenate([st[c, x], st[c, x + NP]], axis=1)

    def pick(T, val, x, f):
        l64 = lanes(32) % 64
        T = jnp.where(l64 == x, roll(val[:32], lax.rem(x - f + LN, LN)), T)
        return jnp.where(l64 == x + 32, roll(val[32:], lax.rem(x + 32 - f + LN, LN)), T)

    def spread(G, x, f):
        return jnp.concatenate([roll(G, lax.rem(f - x + LN, LN)), roll(G, lax.rem(f - x - 32 + LN, LN))], axis=0)

    zero32 = jnp.zeros((32, LN), F32)

    def remote(src, dst, send_sem, recv_sem, dev):
        return pltpu.make_async_remote_copy(src_ref=src, dst_ref=dst, send_sem=send_sem, recv_sem=recv_sem, device_id=dev, device_id_type=MESH)

    def x_plane(ref, c):
        return ref.at[pl.ds(pl.multiple_of(c * SYS + xf * NR, 8), NR)]

    def rows(x, c):
        return pl.ds(pl.multiple_of(c * SYS + x * NR, 8), NR)

    first = []
    for c in range(2):
        first.append([
            remote(sxz.at[c], iz.at[c], isend.at[c, 0], irecv.at[c, 0], nbr['z']),
            remote(sxy.at[c], iy.at[c], isend.at[c, 1], irecv.at[c, 1], nbr['y']),
            remote(x_plane(X, c), ix.at[c], isend.at[c, 2], irecv.at[c, 2], nbr['x']),
            remote(skz.at[c], jz.at[c], isend.at[c, 3], irecv.at[c, 3], nbr['z']),
            remote(sky.at[c], jy.at[c], isend.at[c, 4], irecv.at[c, 4], nbr['y']),
            remote(KX.at[pl.ds(c * SYS + 31 * NR, NR)], jx.at[c], isend.at[c, 5], irecv.at[c, 5], nbr['x'])])

    def prepare_x0(c):
        loaded(0, c)

        def pack_x(x, T):
            u = packed(st_x, c, x)
            X[rows(x, c)] = u
            base = pl.multiple_of(c * PSYS + x * PR, 8)
            PB[pl.ds(base, 8)] = jnp.zeros((8, LN), F32)
            PB[pl.ds(base + 72, 8)] = jnp.zeros((8, LN), F32)
            PB[pl.ds(base + 8, NR)] = u
            return pick(T, u, x, zf)
        sxz[c] = lax.fori_loop(0, NP, pack_x, zero32, unroll=8)
        sxy[c] = X[pl.ds(c * SYS + yf, 32, stride=NR)]

    def prepare_kz(c):
        loaded(1, c)

        def pack_z(x, T):
            u = packed(st_kz, c, x)
            inner = jnp.where(lanes(NR) % 64 == 63, 0.0, u)
            moved = roll(inner, 1)
            KZ[rows(x, c)] = jnp.where(pz == 1, moved, inner)
            KZF[rows(x, c)] = jnp.where(pz == 1, inner, moved)
            return pick(T, u, x, 63)
        skz[c] = lax.fori_loop(0, NP, pack_z, zero32, unroll=8)

    def prepare_ky(c):
        loaded(2, c)

        def pack_ky(x, carry):
            u = packed(st_ky, c, x)
            row = lax.broadcasted_iota(jnp.int32, (NR, LN), 0)
            u = jnp.where(jnp.logical_and(row == NR - 1, py == 1), 0.0, u)
            KY[pl.ds(pl.multiple_of(c * KSYS + x * KR + 8, 8), NR)] = u
            return carry
        lax.fori_loop(0, NP, pack_ky, 0, unroll=8)
        sky[c] = KY[pl.ds(c * KSYS + 71, 32, stride=KR)]

    def prepare_kx(c):
        loaded(3, c)

        def pack_kx(x, carry):
            KX[rows(x, c)] = packed(st_kx, c, x)
            return carry
        lax.fori_loop(0, NP, pack_kx, 0, unroll=8)
        last = KX[pl.ds(c * SYS + 31 * NR, NR)]
        edge = jnp.logical_and(lanes(NR) >= 64, px == 1)
        KX[pl.ds(c * SYS + 31 * NR, NR)] = jnp.where(edge, 0.0, last)

    def prepare_sb(c):
        loaded(4, c)
        loaded(5, c)

        def pack_sb(x, carry):
            D[rows(x, c)] = packed(st_s, c, x)
            R[rows(x, c)] = packed(st_b, c, x)
            return carry
        lax.fori_loop(0, NP, pack_sb, 0, unroll=8)

    prepare_x0(0)
    pl.semaphore_wait(barrier, 7)
    for cp in first[0][:3]:
        cp.start()
    prepare_kz(0)
    first[0][3].start()
    prepare_ky(0)
    first[0][4].start()
    prepare_kx(0)
    first[0][5].start()
    prepare_sb(0)
    prepare_x0(1)
    for cp in first[1][:3]:
        cp.start()
    prepare_kz(1)
    first[1][3].start()
    prepare_ky(1)
    first[1][4].start()

    def reduce_copies(kind, c):
        return [remote(red.at[kind, c, 0], red.at[kind, c, m], dsend.at[kind, c, m], drecv.at[kind, c, m], others[m]) for m in (7, 6, 5, 4, 3, 2, 1)]

    def reduce_start(kind, c, part):
        red[kind, c, 0] = jnp.sum(part, axis=0, keepdims=True)
        for cp in reduce_copies(kind, c):
            cp.start()

    def reduce_end(kind, c):
        for cp in reduce_copies(kind, c):
            cp.wait_recv()
        v = [red[kind, c, m] for m in range(8)]
        total = ((v[0] + v[1]) + (v[2] + v[3])) + ((v[4] + v[5]) + (v[6] + v[7]))
        total = jnp.broadcast_to(total, (8, LN))
        return jnp.broadcast_to(jnp.sum(total, axis=1, keepdims=True), (8, LN))

    def reduce_sent(kind, c):
        for cp in reduce_copies(kind, c):
            cp.wait_send()

    def fold(val):
        return jnp.sum(val.reshape(-1, 8, LN), axis=0)

    def wide(vec, n):
        return jnp.broadcast_to(vec[None], (n // 8, 8, LN)).reshape(n, LN)

    def z_face(ref, c, to_sz, to_sy):
        def plane(x, T):
            return pick(T, ref[rows(x, c)], x, zf)
        to_sz[c] = lax.fori_loop(0, NP, plane, zero32, unroll=16)
        to_sy[c] = ref[pl.ds(c * SYS + yf, 32, stride=NR)]

    def turn_r(c):
        G = rhz[c]
        mask = face_mask(NR)

        def plane(x, carry):
            RZ[rows(x, c)] = jnp.where(mask, spread(G, x, zf), roll(R[rows(x, c)], to_z))
            return carry
        lax.fori_loop(0, NP, plane, 0, unroll=16)

    def r_copies(c):
        return [
            remote(srz.at[c], rhz.at[c], rsend.at[c, 0], rrecv.at[c, 0], nbr['z']),
            remote(sry.at[c], rhy.at[c], rsend.at[c, 1], rrecv.at[c, 1], nbr['y']),
            remote(x_plane(R, c), rhx.at[c], rsend.at[c, 2], rrecv.at[c, 2], nbr['x'])]

    def start(c):
        for cp in first[c]:
            cp.wait_recv()
        lo = splits(NR)
        kx_last = KX[pl.ds(c * SYS + 31 * NR, NR)]
        KXM[c] = roll(jnp.where(lo, kx_last, jnp.where(px == 1, jx[c], 0.0)), 64)
        KY[pl.ds(c * KSYS + 7, 32, stride=KR)] = jnp.where(py == 1, jy[c], 0.0)
        KF[c] = jnp.where(pz == 1, jz[c], skz[c])
        PB[pl.ds(c * PSYS + hrow, 32, stride=PR)] = iy[c]
        u_first = PB[pl.ds(c * PSYS + 8, NR)]
        u_last = PB[pl.ds(c * PSYS + 31 * PR + 8, NR)]
        PB[pl.ds(c * PSYS + 32 * PR + 8, NR)] = roll(jnp.where(lo, ix[c], u_first), 64)
        low = roll(jnp.where(lo, u_last, ix[c]), 64)
        kf, uf = KF[c], iz[c]
        mask = face_mask(NR)

        def start_plane(x, carry):
            acc, fx_prev, kx_prev, u = carry
            base = pl.multiple_of(c * PSYS + x * PR, 8)
            at = rows(x, c)
            kbase = pl.multiple_of(c * KSYS + x * KR, 8)
            nxt = PB[pl.ds(base + PR + 8, NR)]
            yu = PB[pl.ds(base + 9, NR)]
            yl = PB[pl.ds(base + 7, NR)]
            s = D[at]
            kxv = KX[at]
            kyv = KY[pl.ds(kbase + 8, NR)]
            kyl = KY[pl.ds(kbase + 7, NR)]
            kzf = jnp.where(mask, spread(kf, x, zf), KZ[at])
            uz = jnp.where(mask, spread(uf, x, zf), roll(u, to_z))
            fx = kxv * (u - nxt)
            fz = kzf * (u - uz)
            fz_away = roll(jnp.where(mask, 0.0, fz), fro_z)
            D[at] = s + (kxv + kx_prev) + (kyv + kyl) + (kzf + KZF[at])
            KZF[at] = kzf
            PZ[at] = uz
            r = R[at] - (s * u + (fx - fx_prev) + (kyv * (u - yu) - kyl * (yl - u)) + (fz - fz_away))
            R[at] = r
            return acc + fold(r * r), fx, kxv, nxt
        init = (jnp.zeros((8, LN), F32), KXM[c] * (low - u_first), KXM[c], u_first)
        acc = lax.fori_loop(0, NP, start_plane, init, unroll=4)[0]
        reduce_start(0, c, acc)
        z_face(R, c, srz, sry)
        for cp in r_copies(c):
            cp.start()

    prepare_kx(1)
    first[1][5].start()
    start(0)
    prepare_sb(1)
    start(1)
    hist_s[...] = jnp.zeros((8, LN), F32)
    for c in range(2):
        phx[c] = jnp.zeros((NR, LN), F32)
        phy[c] = zero32
        for cp in first[c]:
            cp.wait_send()
    for cp in r_copies(0):
        cp.wait_recv()
    turn_r(0)

    def q_copies(c, par):
        return [
            remote(sz.at[c], qhz.at[par, c], qsend.at[c, 0], qrecv.at[par, c, 0], nbr['z']),
            remote(sy.at[c], qhy.at[par, c], qsend.at[c, 1], qrecv.at[par, c, 1], nbr['y']),
            remote(x_plane(Q, c), qhx.at[par, c], qsend.at[c, 2], qrecv.at[par, c, 2], nbr['x'])]

    def note(c, k, rho):
        hist_s[...] = jnp.where(jnp.logical_and(lane == k, row8 == c), rho, hist_s[...])

    def product(c, beta):
        b64 = wide(beta, NR)
        hx = rhx[c] + b64 * phx[c]
        hy = rhy[c] + wide(beta, 32) * phy[c]
        phx[c] = hx
        phy[c] = hy
        PB[pl.ds(c * PSYS + hrow, 32, stride=PR)] = hy
        lo = splits(NR)

        def direction(x):
            at = pl.ds(c * PSYS + x * PR + 8, NR)
            val = R[pl.ds(c * SYS + x * NR, NR)] + b64 * PB[at]
            PB[at] = val
            return val

        def turn(x, p):
            return roll(KZ[pl.ds(c * SYS + x * NR, NR)] * p, fro_z)

        def load_p(x):
            return PB[pl.ds(c * PSYS + x * PR + 8, NR)]

        p_last = direction(NP - 1)
        p_first = direction(0)
        above = roll(jnp.where(lo, hx, p_first), 64)
        below = roll(jnp.where(lo, p_last, hx), 64)
        turned = {0: turn(0, p_first)}
        for x in range(1, AHEAD):
            turned[x] = turn(x, direction(x))
        cur, kxp_prev = p_first, KXM[c] * below
        acc = jnp.zeros((8, LN), F32)
        for x in range(NP):
            w = x + AHEAD
            if w < NP:
                turned[w] = turn(w, direction(w) if w < NP - 1 else load_p(w))
            nxt = load_p(x + 1) if x + 1 < NP else above
            base = c * PSYS + x * PR
            at = pl.ds(c * SYS + x * NR, NR)
            kbase = c * KSYS + x * KR
            kxv = KX[at]
            kxp = kxv * cur
            q = D[at] * cur - kxp_prev - kxv * nxt
            q = q - KY[pl.ds(kbase + 8, NR)] * PB[pl.ds(base + 9, NR)]
            q = q - KY[pl.ds(kbase + 7, NR)] * PB[pl.ds(base + 7, NR)]
            pz_new = RZ[at] + b64 * PZ[at]
            PZ[at] = pz_new
            q = q - KZF[at] * pz_new - turned.pop(x)
            Q[at] = q
            acc = acc + fold(cur * q)
            cur, kxp_prev = nxt, kxp
        return acc

    def halo_r(c, par):
        for cp in q_copies(c, par):
            cp.wait_recv()
        alpha = alpha_s[c]
        rhx[c] = rhx[c] - wide(alpha, NR) * qhx[par, c]
        rhy[c] = rhy[c] - wide(alpha, 32) * qhy[par, c]
        rhz[c] = rhz[c] - wide(alpha, 32) * qhz[par, c]

    def q_sent(c, par):
        for cp in q_copies(c, par):
            cp.wait_send()

    def first_half(c, k, par):
        rho = reduce_end(0, c)
        note(c, k, rho)
        beta = jnp.where(k == 0, 0.0, rho / rho_s[c])
        rho_s[c] = rho
        reduce_start(1, c, product(c, beta))
        reduce_sent(0, c)
        z_face(Q, c, sz, sy)
        for cp in q_copies(c, par):
            cp.start()

    def second_half(c, k):
        alpha = rho_s[c] / reduce_end(1, c)
        alpha_s[c] = alpha
        a_pl = wide(alpha, NR)
        acc = jnp.zeros((8, LN), F32)
        for x in range(NP):
            at = pl.ds(c * SYS + x * NR, NR)
            r = R[at] - a_pl * Q[at]
            R[at] = r
            acc = acc + fold(r * r)
        reduce_start(0, c, acc)

        def step_x(x, carry):
            X[rows(x, c)] = X[rows(x, c)] + a_pl * PB[pl.ds(pl.multiple_of(c * PSYS + x * PR + 8, 8), NR)]
            return carry
        lax.fori_loop(0, NP, step_x, 0, unroll=4)
        reduce_sent(1, c)

    def body(k, carry):
        par = k % 2
        first_half(0, k, par)

        @pl.when(k == 0)
        def _():
            for cp in r_copies(1):
                cp.wait_recv()

        @pl.when(k > 0)
        def _():
            halo_r(1, 1 - par)
            q_sent(1, 1 - par)
        turn_r(1)
        first_half(1, k, par)

        @pl.when(k == 0)
        def _():
            for c in range(2):
                for cp in r_copies(c):
                    cp.wait_send()
        second_half(0, k)
        halo_r(0, par)
        turn_r(0)
        second_half(1, k)
        q_sent(0, par)
        return carry

    lax.fori_loop(0, ITERS, body, 0)
    for c in range(2):
        note(c, ITERS, reduce_end(0, c))
        reduce_sent(0, c)
    for cp in q_copies(1, (ITERS - 1) % 2):
        cp.wait()
    hist_out[...] = jnp.sqrt(hist_s[...] * (1.0 / (128 * 128 * 128)))


CHUNKS = 4
VMEM_MAIN = 54 * 1024 * 1024


def unpack(buf, hist, x_out, hist_out, st, ho, out_sem, h_sem):
    planes = NP // CHUNKS
    ho[...] = hist[:2, :ITERS + 1]
    stores = [pltpu.make_async_copy(ho, hist_out, h_sem)]
    stores[0].start()
    for n in range(2 * CHUNKS):
        c, x0 = n // CHUNKS, n % CHUNKS * planes

        def plane(x, carry):
            val = buf[pl.ds(pl.multiple_of(n * planes * NR + x * NR, 8), NR)]
            st[c, x0 + x] = val[:, :64]
            st[c, x0 + x + NP] = roll(val, 64)[:, :64]
            return carry
        lax.fori_loop(0, planes, plane, 0, unroll=8)
        for h in range(2):
            at = pl.ds(x0 + NP * h, planes)
            stores.append(pltpu.make_async_copy(st.at[c, at], x_out.at[c, at], out_sem.at[n, h]))
            stores[-1].start()
    for cp in stores:
        cp.wait()


def run(s, b, x0, kx, ky, kz):
    v = lambda *shape: pltpu.VMEM(shape, F32)
    sem = lambda *shape: pltpu.SemaphoreType.DMA(shape)
    scratch = [v(2, 64, 64, 64)] * 6
    full = v(2 * SYS, LN)
    scratch += [full, full, v(2 * PSYS, LN), full, full, full, v(2, NR, LN), v(2 * KSYS, LN), full, full, full, v(2, 32, LN)]
    scratch += [v(2, NR, LN), v(2, 32, LN), v(2, 32, LN)] * 2
    scratch += [v(2, 32, LN)] * 8
    scratch += [v(2, NR, LN), v(2, 32, LN), v(2, 32, LN), v(2, NR, LN), v(2, 32, LN)]
    scratch += [v(2, 2, NR, LN), v(2, 2, 32, LN), v(2, 2, 32, LN)]
    scratch += [v(2, 2, 8, 1, LN), v(2, 8, LN), v(2, 8, LN), v(8, LN)]
    scratch += [sem(6, 2), sem(2, 6), sem(2, 6), sem(2, 3), sem(2, 3), sem(2, 3), sem(2, 2, 3), sem(2, 2, 8), sem(2, 2, 8)]
    xp, hist = pl.pallas_call(
        kernel,
        out_shape=(pltpu.VMEM((2 * SYS, LN), F32), pltpu.VMEM((8, LN), F32)),
        in_specs=[pl.BlockSpec(memory_space=pl.ANY)] * 6,
        out_specs=(pl.BlockSpec(memory_space=pltpu.VMEM), pl.BlockSpec(memory_space=pltpu.VMEM)),
        scratch_shapes=scratch,
        compiler_params=pltpu.CompilerParams(collective_id=0, has_side_effects=True, vmem_limit_bytes=VMEM_MAIN),
        name='cg',
    )(s, b, x0, kx, ky, kz)
    return pl.pallas_call(
        unpack,
        out_shape=(jax.ShapeDtypeStruct((2, 64, 64, 64), F32), jax.ShapeDtypeStruct((2, ITERS + 1), F32)),
        in_specs=[pl.BlockSpec(memory_space=pltpu.VMEM)] * 2,
        out_specs=[pl.BlockSpec(memory_space=pl.ANY)] * 2,
        scratch_shapes=[v(2, 64, 64, 64), v(2, ITERS + 1), sem(2 * CHUNKS, 2), pltpu.SemaphoreType.DMA],
        compiler_params=pltpu.CompilerParams(vmem_limit_bytes=12 * 1024 * 1024),
        name='unpack',
    )(xp, hist)


def solution(mesh):
    field = P(None, 'px', 'py', 'pz')
    return jax.shard_map(run, mesh=mesh, in_specs=(field,) * 6, out_specs=(field, P(None, None)), check_vma=False)
```

```python
import jax
import jax.numpy as jnp
from jax import lax
from jax.experimental import pallas as pl
from jax.experimental.pallas import tpu as pltpu
from jax.sharding import PartitionSpec as P

ITERS = 20
F32 = jnp.float32
MESH = pl.DeviceIdType.MESH

NP = 32
NR = 64
LN = 128
PR = 80
KR = 72
SYS = NP * NR
PSYS = (NP + 1) * PR
KSYS = NP * KR
IN_FLIGHT = 5
AHEAD = 3


def roll(val, shift):
    if isinstance(shift, int):
        shift = shift % LN
    return pltpu.roll(val, shift, 1)


def kernel(s_hbm, b_hbm, x0_hbm, kx_hbm, ky_hbm, kz_hbm, X, hist_out,
           st_s, st_b, st_x, st_kx, st_ky, st_kz,
           R, Q, PB, PZ, RZ, KX, KXM, KY, KZ, KZF, D, KF,
           ix, iy, iz, jx, jy, jz, sxy, sxz, sky, skz, sy, sz, sry, srz,
           rhx, rhy, rhz, phx, phy, qhx, qhy, qhz,
           red, rho_s, alpha_s, hist_s,
           ld_sem, isend, irecv, rsend, rrecv, qsend, qrecv, dsend, drecv):
    pz, py, px = lax.axis_index('pz'), lax.axis_index('py'), lax.axis_index('px')
    nbr = {'x': (pz, py, 1 - px), 'y': (pz, 1 - py, px), 'z': (1 - pz, py, px)}
    others = {}
    for m in range(1, 8):
        others[m] = (1 - pz if m & 4 else pz, 1 - py if m & 2 else py, 1 - px if m & 1 else px)

    lane = lax.broadcasted_iota(jnp.int32, (8, LN), 1)
    row8 = lax.broadcasted_iota(jnp.int32, (8, LN), 0)

    def lanes(n):
        return lax.broadcasted_iota(jnp.int32, (n, LN), 1)

    zf = 63 * (1 - pz)
    xf = 31 * (1 - px)
    yf = 63 * (1 - py)
    hrow = 72 - 65 * py
    to_z = 127 - 126 * pz
    fro_z = 1 + 126 * pz

    def face_mask(n):
        return (lanes(n) % 64) == zf

    def splits(n):
        return lanes(n) < 64

    order = [(num, c) for c in range(2) for num in range(6)]
    pairs = ((x0_hbm, st_x), (kz_hbm, st_kz), (ky_hbm, st_ky), (kx_hbm, st_kx), (s_hbm, st_s), (b_hbm, st_b))
    loads = [pltpu.make_async_copy(pairs[num][0].at[c], pairs[num][1].at[c], ld_sem.at[num, c]) for num, c in order]
    for cp in loads[:IN_FLIGHT]:
        cp.start()

    def loaded(num, c):
        n = c * 6 + num
        loads[n].wait()
        if n + IN_FLIGHT < len(loads):
            loads[n + IN_FLIGHT].start()

    barrier = pltpu.get_barrier_semaphore()
    for m in range(1, 8):
        pl.semaphore_signal(barrier, inc=1, device_id=others[m], device_id_type=MESH)

    def packed(st, c, x):
        return jnp.concatenate([st[c, x], st[c, x + NP]], axis=1)

    def pick(T, val, x, f):
        l64 = lanes(32) % 64
        T = jnp.where(l64 == x, roll(val[:32], lax.rem(x - f + LN, LN)), T)
        return jnp.where(l64 == x + 32, roll(val[32:], lax.rem(x + 32 - f + LN, LN)), T)

    def spread(G, x, f):
        return jnp.concatenate([roll(G, lax.rem(f - x + LN, LN)), roll(G, lax.rem(f - x - 32 + LN, LN))], axis=0)

    zero32 = jnp.zeros((32, LN), F32)

    def remote(src, dst, send_sem, recv_sem, dev):
        return pltpu.make_async_remote_copy(src_ref=src, dst_ref=dst, send_sem=send_sem, recv_sem=recv_sem, device_id=dev, device_id_type=MESH)

    def x_plane(ref, c):
        return ref.at[pl.ds(pl.multiple_of(c * SYS + xf * NR, 8), NR)]

    def rows(x, c):
        return pl.ds(pl.multiple_of(c * SYS + x * NR, 8), NR)

    first = []
    for c in range(2):
        first.append([
            remote(sxz.at[c], iz.at[c], isend.at[c, 0], irecv.at[c, 0], nbr['z']),
            remote(sxy.at[c], iy.at[c], isend.at[c, 1], irecv.at[c, 1], nbr['y']),
            remote(x_plane(X, c), ix.at[c], isend.at[c, 2], irecv.at[c, 2], nbr['x']),
            remote(skz.at[c], jz.at[c], isend.at[c, 3], irecv.at[c, 3], nbr['z']),
            remote(sky.at[c], jy.at[c], isend.at[c, 4], irecv.at[c, 4], nbr['y']),
            remote(KX.at[pl.ds(c * SYS + 31 * NR, NR)], jx.at[c], isend.at[c, 5], irecv.at[c, 5], nbr['x'])])

    def prepare_x0(c):
        loaded(0, c)

        def pack_x(x, T):
            u = packed(st_x, c, x)
            X[rows(x, c)] = u
            base = pl.multiple_of(c * PSYS + x * PR, 8)
            PB[pl.ds(base, 8)] = jnp.zeros((8, LN), F32)
            PB[pl.ds(base + 72, 8)] = jnp.zeros((8, LN), F32)
            PB[pl.ds(base + 8, NR)] = u
            return pick(T, u, x, zf)
        sxz[c] = lax.fori_loop(0, NP, pack_x, zero32, unroll=8)
        sxy[c] = X[pl.ds(c * SYS + yf, 32, stride=NR)]

    def prepare_kz(c):
        loaded(1, c)

        def pack_z(x, T):
            u = packed(st_kz, c, x)
            inner = jnp.where(lanes(NR) % 64 == 63, 0.0, u)
            moved = roll(inner, 1)
            KZ[rows(x, c)] = jnp.where(pz == 1, moved, inner)
            KZF[rows(x, c)] = jnp.where(pz == 1, inner, moved)
            return pick(T, u, x, 63)
        skz[c] = lax.fori_loop(0, NP, pack_z, zero32, unroll=8)

    def prepare_ky(c):
        loaded(2, c)

        def pack_ky(x, carry):
            u = packed(st_ky, c, x)
            row = lax.broadcasted_iota(jnp.int32, (NR, LN), 0)
            u = jnp.where(jnp.logical_and(row == NR - 1, py == 1), 0.0, u)
            KY[pl.ds(pl.multiple_of(c * KSYS + x * KR + 8, 8), NR)] = u
            return carry
        lax.fori_loop(0, NP, pack_ky, 0, unroll=8)
        sky[c] = KY[pl.ds(c * KSYS + 71, 32, stride=KR)]

    def prepare_kx(c):
        loaded(3, c)

        def pack_kx(x, carry):
            KX[rows(x, c)] = packed(st_kx, c, x)
            return carry
        lax.fori_loop(0, NP, pack_kx, 0, unroll=8)
        last = KX[pl.ds(c * SYS + 31 * NR, NR)]
        edge = jnp.logical_and(lanes(NR) >= 64, px == 1)
        KX[pl.ds(c * SYS + 31 * NR, NR)] = jnp.where(edge, 0.0, last)

    def prepare_sb(c):
        loaded(4, c)
        loaded(5, c)

        def pack_sb(x, carry):
            D[rows(x, c)] = packed(st_s, c, x)
            R[rows(x, c)] = packed(st_b, c, x)
            return carry
        lax.fori_loop(0, NP, pack_sb, 0, unroll=8)

    prepare_x0(0)
    pl.semaphore_wait(barrier, 7)
    for cp in first[0][:3]:
        cp.start()
    prepare_kz(0)
    first[0][3].start()
    prepare_ky(0)
    first[0][4].start()
    prepare_kx(0)
    first[0][5].start()
    prepare_sb(0)
    prepare_x0(1)
    for cp in first[1][:3]:
        cp.start()
    prepare_kz(1)
    first[1][3].start()
    prepare_ky(1)
    first[1][4].start()

    def reduce_copies(kind, c):
        return [remote(red.at[kind, c, 0], red.at[kind, c, m], dsend.at[kind, c, m], drecv.at[kind, c, m], others[m]) for m in (7, 6, 5, 4, 3, 2, 1)]

    def reduce_start(kind, c, part):
        red[kind, c, 0] = jnp.sum(part, axis=0, keepdims=True)
        for cp in reduce_copies(kind, c):
            cp.start()

    def reduce_end(kind, c):
        for cp in reduce_copies(kind, c):
            cp.wait_recv()
        v = [red[kind, c, m] for m in range(8)]
        total = ((v[0] + v[1]) + (v[2] + v[3])) + ((v[4] + v[5]) + (v[6] + v[7]))
        total = jnp.broadcast_to(total, (8, LN))
        return jnp.broadcast_to(jnp.sum(total, axis=1, keepdims=True), (8, LN))

    def reduce_sent(kind, c):
        for cp in reduce_copies(kind, c):
            cp.wait_send()

    def fold(val):
        return jnp.sum(val.reshape(-1, 8, LN), axis=0)

    def wide(vec, n):
        return jnp.broadcast_to(vec[None], (n // 8, 8, LN)).reshape(n, LN)

    def z_face(ref, c, to_sz, to_sy):
        def plane(x, T):
            return pick(T, ref[rows(x, c)], x, zf)
        to_sz[c] = lax.fori_loop(0, NP, plane, zero32, unroll=32)
        to_sy[c] = ref[pl.ds(c * SYS + yf, 32, stride=NR)]

    def turn_r(c):
        G = rhz[c]
        mask = face_mask(NR)

        def plane(x, carry):
            RZ[rows(x, c)] = jnp.where(mask, spread(G, x, zf), roll(R[rows(x, c)], to_z))
            return carry
        lax.fori_loop(0, NP, plane, 0, unroll=32)

    def r_copies(c):
        return [
            remote(srz.at[c], rhz.at[c], rsend.at[c, 0], rrecv.at[c, 0], nbr['z']),
            remote(sry.at[c], rhy.at[c], rsend.at[c, 1], rrecv.at[c, 1], nbr['y']),
            remote(x_plane(R, c), rhx.at[c], rsend.at[c, 2], rrecv.at[c, 2], nbr['x'])]

    def start(c):
        for cp in first[c]:
            cp.wait_recv()
        lo = splits(NR)
        kx_last = KX[pl.ds(c * SYS + 31 * NR, NR)]
        KXM[c] = roll(jnp.where(lo, kx_last, jnp.where(px == 1, jx[c], 0.0)), 64)
        KY[pl.ds(c * KSYS + 7, 32, stride=KR)] = jnp.where(py == 1, jy[c], 0.0)
        KF[c] = jnp.where(pz == 1, jz[c], skz[c])
        PB[pl.ds(c * PSYS + hrow, 32, stride=PR)] = iy[c]
        u_first = PB[pl.ds(c * PSYS + 8, NR)]
        u_last = PB[pl.ds(c * PSYS + 31 * PR + 8, NR)]
        PB[pl.ds(c * PSYS + 32 * PR + 8, NR)] = roll(jnp.where(lo, ix[c], u_first), 64)
        low = roll(jnp.where(lo, u_last, ix[c]), 64)
        kf, uf = KF[c], iz[c]
        mask = face_mask(NR)

        def start_plane(x, carry):
            acc, fx_prev, kx_prev, u = carry
            base = pl.multiple_of(c * PSYS + x * PR, 8)
            at = rows(x, c)
            kbase = pl.multiple_of(c * KSYS + x * KR, 8)
            nxt = PB[pl.ds(base + PR + 8, NR)]
            yu = PB[pl.ds(base + 9, NR)]
            yl = PB[pl.ds(base + 7, NR)]
            s = D[at]
            kxv = KX[at]
            kyv = KY[pl.ds(kbase + 8, NR)]
            kyl = KY[pl.ds(kbase + 7, NR)]
            kzf = jnp.where(mask, spread(kf, x, zf), KZ[at])
            uz = jnp.where(mask, spread(uf, x, zf), roll(u, to_z))
            fx = kxv * (u - nxt)
            fz = kzf * (u - uz)
            fz_away = roll(jnp.where(mask, 0.0, fz), fro_z)
            D[at] = s + (kxv + kx_prev) + (kyv + kyl) + (kzf + KZF[at])
            KZF[at] = kzf
            PZ[at] = uz
            r = R[at] - (s * u + (fx - fx_prev) + (kyv * (u - yu) - kyl * (yl - u)) + (fz - fz_away))
            R[at] = r
            return acc + fold(r * r), fx, kxv, nxt
        init = (jnp.zeros((8, LN), F32), KXM[c] * (low - u_first), KXM[c], u_first)
        acc = lax.fori_loop(0, NP, start_plane, init, unroll=4)[0]
        reduce_start(0, c, acc)
        z_face(R, c, srz, sry)
        for cp in r_copies(c):
            cp.start()

    prepare_kx(1)
    first[1][5].start()
    start(0)
    prepare_sb(1)
    start(1)
    hist_s[...] = jnp.zeros((8, LN), F32)
    for c in range(2):
        phx[c] = jnp.zeros((NR, LN), F32)
        phy[c] = zero32
        for cp in first[c]:
            cp.wait_send()
    for cp in r_copies(0):
        cp.wait_recv()
    turn_r(0)

    def q_copies(c, par):
        return [
            remote(sz.at[c], qhz.at[par, c], qsend.at[c, 0], qrecv.at[par, c, 0], nbr['z']),
            remote(sy.at[c], qhy.at[par, c], qsend.at[c, 1], qrecv.at[par, c, 1], nbr['y']),
            remote(x_plane(Q, c), qhx.at[par, c], qsend.at[c, 2], qrecv.at[par, c, 2], nbr['x'])]

    def note(c, k, rho):
        hist_s[...] = jnp.where(jnp.logical_and(lane == k, row8 == c), rho, hist_s[...])

    def product(c, beta):
        b64 = wide(beta, NR)
        hx = rhx[c] + b64 * phx[c]
        hy = rhy[c] + wide(beta, 32) * phy[c]
        phx[c] = hx
        phy[c] = hy
        PB[pl.ds(c * PSYS + hrow, 32, stride=PR)] = hy
        lo = splits(NR)

        def direction(x):
            at = pl.ds(c * PSYS + x * PR + 8, NR)
            val = R[pl.ds(c * SYS + x * NR, NR)] + b64 * PB[at]
            PB[at] = val
            return val

        def turn(x, p):
            return roll(KZ[pl.ds(c * SYS + x * NR, NR)] * p, fro_z)

        def load_p(x):
            return PB[pl.ds(c * PSYS + x * PR + 8, NR)]

        p_last = direction(NP - 1)
        p_first = direction(0)
        above = roll(jnp.where(lo, hx, p_first), 64)
        below = roll(jnp.where(lo, p_last, hx), 64)
        turned = {0: turn(0, p_first)}
        for x in range(1, AHEAD):
            turned[x] = turn(x, direction(x))
        cur, kxp_prev = p_first, KXM[c] * below
        acc = jnp.zeros((8, LN), F32)
        for x in range(NP):
            w = x + AHEAD
            if w < NP:
                turned[w] = turn(w, direction(w) if w < NP - 1 else load_p(w))
            nxt = load_p(x + 1) if x + 1 < NP else above
            base = c * PSYS + x * PR
            at = pl.ds(c * SYS + x * NR, NR)
            kbase = c * KSYS + x * KR
            kxv = KX[at]
            kxp = kxv * cur
            q = D[at] * cur - kxp_prev - kxv * nxt
            q = q - KY[pl.ds(kbase + 8, NR)] * PB[pl.ds(base + 9, NR)]
            q = q - KY[pl.ds(kbase + 7, NR)] * PB[pl.ds(base + 7, NR)]
            pz_new = RZ[at] + b64 * PZ[at]
            PZ[at] = pz_new
            q = q - KZF[at] * pz_new - turned.pop(x)
            Q[at] = q
            acc = acc + fold(cur * q)
            cur, kxp_prev = nxt, kxp
        return acc

    def halo_r(c, par):
        for cp in q_copies(c, par):
            cp.wait_recv()
        alpha = alpha_s[c]
        rhx[c] = rhx[c] - wide(alpha, NR) * qhx[par, c]
        rhy[c] = rhy[c] - wide(alpha, 32) * qhy[par, c]
        rhz[c] = rhz[c] - wide(alpha, 32) * qhz[par, c]

    def q_sent(c, par):
        for cp in q_copies(c, par):
            cp.wait_send()

    def first_half(c, k, par):
        rho = reduce_end(0, c)
        note(c, k, rho)
        beta = jnp.where(k == 0, 0.0, rho / rho_s[c])
        rho_s[c] = rho
        reduce_start(1, c, product(c, beta))
        reduce_sent(0, c)
        z_face(Q, c, sz, sy)
        for cp in q_copies(c, par):
            cp.start()

    def second_half(c, k):
        alpha = rho_s[c] / reduce_end(1, c)
        alpha_s[c] = alpha
        a_pl = wide(alpha, NR)
        acc = jnp.zeros((8, LN), F32)
        for x in range(NP):
            at = pl.ds(c * SYS + x * NR, NR)
            r = R[at] - a_pl * Q[at]
            R[at] = r
            acc = acc + fold(r * r)
        reduce_start(0, c, acc)

        def step_x(x, carry):
            X[rows(x, c)] = X[rows(x, c)] + a_pl * PB[pl.ds(pl.multiple_of(c * PSYS + x * PR + 8, 8), NR)]
            return carry
        lax.fori_loop(0, NP, step_x, 0, unroll=4)
        reduce_sent(1, c)

    def body(k, carry):
        par = k % 2
        first_half(0, k, par)

        @pl.when(k == 0)
        def _():
            for cp in r_copies(1):
                cp.wait_recv()

        @pl.when(k > 0)
        def _():
            halo_r(1, 1 - par)
            q_sent(1, 1 - par)
        turn_r(1)
        first_half(1, k, par)

        @pl.when(k == 0)
        def _():
            for c in range(2):
                for cp in r_copies(c):
                    cp.wait_send()
        second_half(0, k)
        halo_r(0, par)
        turn_r(0)
        second_half(1, k)
        q_sent(0, par)
        return carry

    lax.fori_loop(0, ITERS, body, 0)
    for c in range(2):
        note(c, ITERS, reduce_end(0, c))
        reduce_sent(0, c)
    for cp in q_copies(1, (ITERS - 1) % 2):
        cp.wait()
    hist_out[...] = jnp.sqrt(hist_s[...] * (1.0 / (128 * 128 * 128)))


CHUNKS = 4
VMEM_MAIN = 54 * 1024 * 1024


def unpack(buf, hist, x_out, hist_out, st, ho, out_sem, h_sem):
    planes = NP // CHUNKS
    ho[...] = hist[:2, :ITERS + 1]
    stores = [pltpu.make_async_copy(ho, hist_out, h_sem)]
    stores[0].start()
    for n in range(2 * CHUNKS):
        c, x0 = n // CHUNKS, n % CHUNKS * planes

        def plane(x, carry):
            val = buf[pl.ds(pl.multiple_of(n * planes * NR + x * NR, 8), NR)]
            st[c, x0 + x] = val[:, :64]
            st[c, x0 + x + NP] = roll(val, 64)[:, :64]
            return carry
        lax.fori_loop(0, planes, plane, 0, unroll=8)
        for h in range(2):
            at = pl.ds(x0 + NP * h, planes)
            stores.append(pltpu.make_async_copy(st.at[c, at], x_out.at[c, at], out_sem.at[n, h]))
            stores[-1].start()
    for cp in stores:
        cp.wait()


def run(s, b, x0, kx, ky, kz):
    v = lambda *shape: pltpu.VMEM(shape, F32)
    sem = lambda *shape: pltpu.SemaphoreType.DMA(shape)
    scratch = [v(2, 64, 64, 64)] * 6
    full = v(2 * SYS, LN)
    scratch += [full, full, v(2 * PSYS, LN), full, full, full, v(2, NR, LN), v(2 * KSYS, LN), full, full, full, v(2, 32, LN)]
    scratch += [v(2, NR, LN), v(2, 32, LN), v(2, 32, LN)] * 2
    scratch += [v(2, 32, LN)] * 8
    scratch += [v(2, NR, LN), v(2, 32, LN), v(2, 32, LN), v(2, NR, LN), v(2, 32, LN)]
    scratch += [v(2, 2, NR, LN), v(2, 2, 32, LN), v(2, 2, 32, LN)]
    scratch += [v(2, 2, 8, 1, LN), v(2, 8, LN), v(2, 8, LN), v(8, LN)]
    scratch += [sem(6, 2), sem(2, 6), sem(2, 6), sem(2, 3), sem(2, 3), sem(2, 3), sem(2, 2, 3), sem(2, 2, 8), sem(2, 2, 8)]
    xp, hist = pl.pallas_call(
        kernel,
        out_shape=(pltpu.VMEM((2 * SYS, LN), F32), pltpu.VMEM((8, LN), F32)),
        in_specs=[pl.BlockSpec(memory_space=pl.ANY)] * 6,
        out_specs=(pl.BlockSpec(memory_space=pltpu.VMEM), pl.BlockSpec(memory_space=pltpu.VMEM)),
        scratch_shapes=scratch,
        compiler_params=pltpu.CompilerParams(collective_id=0, has_side_effects=True, vmem_limit_bytes=VMEM_MAIN),
        name='cg',
    )(s, b, x0, kx, ky, kz)
    return pl.pallas_call(
        unpack,
        out_shape=(jax.ShapeDtypeStruct((2, 64, 64, 64), F32), jax.ShapeDtypeStruct((2, ITERS + 1), F32)),
        in_specs=[pl.BlockSpec(memory_space=pltpu.VMEM)] * 2,
        out_specs=[pl.BlockSpec(memory_space=pl.ANY)] * 2,
        scratch_shapes=[v(2, 64, 64, 64), v(2, ITERS + 1), sem(2 * CHUNKS, 2), pltpu.SemaphoreType.DMA],
        compiler_params=pltpu.CompilerParams(vmem_limit_bytes=12 * 1024 * 1024),
        name='unpack',
    )(xp, hist)


def solution(mesh):
    field = P(None, 'px', 'py', 'pz')
    return jax.shard_map(run, mesh=mesh, in_specs=(field,) * 6, out_specs=(field, P(None, None)), check_vma=False)
```

```python
import jax
import jax.numpy as jnp
from jax import lax
from jax.experimental import pallas as pl
from jax.experimental.pallas import tpu as pltpu
from jax.sharding import PartitionSpec as P

ITERS = 20
F32 = jnp.float32
MESH = pl.DeviceIdType.MESH

NP = 32
NR = 64
LN = 128
PR = 80
KR = 72
SYS = NP * NR
PSYS = (NP + 1) * PR
KSYS = NP * KR
IN_FLIGHT = 5
AHEAD = 3


def roll(val, shift):
    if isinstance(shift, int):
        shift = shift % LN
    return pltpu.roll(val, shift, 1)


def kernel(s_hbm, b_hbm, x0_hbm, kx_hbm, ky_hbm, kz_hbm, X, hist_out,
           st_s, st_b, st_x, st_kx, st_ky, st_kz,
           R, Q, PB, PZ, RZ, KX, KXM, KY, KZ, KZF, D, KF,
           ix, iy, iz, jx, jy, jz, sxy, sxz, sky, skz, sy, sz, sry, srz,
           rhx, rhy, rhz, phx, phy, qhx, qhy, qhz,
           red, rho_s, alpha_s, hist_s,
           ld_sem, isend, irecv, rsend, rrecv, qsend, qrecv, dsend, drecv):
    pz, py, px = lax.axis_index('pz'), lax.axis_index('py'), lax.axis_index('px')
    nbr = {'x': (pz, py, 1 - px), 'y': (pz, 1 - py, px), 'z': (1 - pz, py, px)}
    others = {}
    for m in range(1, 8):
        others[m] = (1 - pz if m & 4 else pz, 1 - py if m & 2 else py, 1 - px if m & 1 else px)

    lane = lax.broadcasted_iota(jnp.int32, (8, LN), 1)
    row8 = lax.broadcasted_iota(jnp.int32, (8, LN), 0)

    def lanes(n):
        return lax.broadcasted_iota(jnp.int32, (n, LN), 1)

    zf = 63 * (1 - pz)
    xf = 31 * (1 - px)
    yf = 63 * (1 - py)
    hrow = 72 - 65 * py
    to_z = 127 - 126 * pz
    fro_z = 1 + 126 * pz

    def face_mask(n):
        return (lanes(n) % 64) == zf

    def splits(n):
        return lanes(n) < 64

    order = [(num, c) for c in range(2) for num in range(6)]
    pairs = ((x0_hbm, st_x), (kz_hbm, st_kz), (ky_hbm, st_ky), (kx_hbm, st_kx), (s_hbm, st_s), (b_hbm, st_b))
    loads = [pltpu.make_async_copy(pairs[num][0].at[c], pairs[num][1].at[c], ld_sem.at[num, c]) for num, c in order]
    for cp in loads[:IN_FLIGHT]:
        cp.start()

    def loaded(num, c):
        n = c * 6 + num
        loads[n].wait()
        if n + IN_FLIGHT < len(loads):
            loads[n + IN_FLIGHT].start()

    barrier = pltpu.get_barrier_semaphore()
    for m in range(1, 8):
        pl.semaphore_signal(barrier, inc=1, device_id=others[m], device_id_type=MESH)

    def packed(st, c, x):
        return jnp.concatenate([st[c, x], st[c, x + NP]], axis=1)

    def pick(T, val, x, f):
        l64 = lanes(32) % 64
        T = jnp.where(l64 == x, roll(val[:32], lax.rem(x - f + LN, LN)), T)
        return jnp.where(l64 == x + 32, roll(val[32:], lax.rem(x + 32 - f + LN, LN)), T)

    def spread(G, x, f):
        return jnp.concatenate([roll(G, lax.rem(f - x + LN, LN)), roll(G, lax.rem(f - x - 32 + LN, LN))], axis=0)

    zero32 = jnp.zeros((32, LN), F32)

    def remote(src, dst, send_sem, recv_sem, dev):
        return pltpu.make_async_remote_copy(src_ref=src, dst_ref=dst, send_sem=send_sem, recv_sem=recv_sem, device_id=dev, device_id_type=MESH)

    def x_plane(ref, c):
        return ref.at[pl.ds(pl.multiple_of(c * SYS + xf * NR, 8), NR)]

    def rows(x, c):
        return pl.ds(pl.multiple_of(c * SYS + x * NR, 8), NR)

    first = []
    for c in range(2):
        first.append([
            remote(sxz.at[c], iz.at[c], isend.at[c, 0], irecv.at[c, 0], nbr['z']),
            remote(sxy.at[c], iy.at[c], isend.at[c, 1], irecv.at[c, 1], nbr['y']),
            remote(x_plane(X, c), ix.at[c], isend.at[c, 2], irecv.at[c, 2], nbr['x']),
            remote(skz.at[c], jz.at[c], isend.at[c, 3], irecv.at[c, 3], nbr['z']),
            remote(sky.at[c], jy.at[c], isend.at[c, 4], irecv.at[c, 4], nbr['y']),
            remote(KX.at[pl.ds(c * SYS + 31 * NR, NR)], jx.at[c], isend.at[c, 5], irecv.at[c, 5], nbr['x'])])

    def prepare_x0(c):
        loaded(0, c)

        def pack_x(x, T):
            u = packed(st_x, c, x)
            X[rows(x, c)] = u
            base = pl.multiple_of(c * PSYS + x * PR, 8)
            PB[pl.ds(base, 8)] = jnp.zeros((8, LN), F32)
            PB[pl.ds(base + 72, 8)] = jnp.zeros((8, LN), F32)
            PB[pl.ds(base + 8, NR)] = u
            return pick(T, u, x, zf)
        sxz[c] = lax.fori_loop(0, NP, pack_x, zero32, unroll=16)
        sxy[c] = X[pl.ds(c * SYS + yf, 32, stride=NR)]

    def prepare_kz(c):
        loaded(1, c)

        def pack_z(x, T):
            u = packed(st_kz, c, x)
            inner = jnp.where(lanes(NR) % 64 == 63, 0.0, u)
            moved = roll(inner, 1)
            KZ[rows(x, c)] = jnp.where(pz == 1, moved, inner)
            KZF[rows(x, c)] = jnp.where(pz == 1, inner, moved)
            return pick(T, u, x, 63)
        skz[c] = lax.fori_loop(0, NP, pack_z, zero32, unroll=16)

    def prepare_ky(c):
        loaded(2, c)

        def pack_ky(x, carry):
            u = packed(st_ky, c, x)
            row = lax.broadcasted_iota(jnp.int32, (NR, LN), 0)
            u = jnp.where(jnp.logical_and(row == NR - 1, py == 1), 0.0, u)
            KY[pl.ds(pl.multiple_of(c * KSYS + x * KR + 8, 8), NR)] = u
            return carry
        lax.fori_loop(0, NP, pack_ky, 0, unroll=16)
        sky[c] = KY[pl.ds(c * KSYS + 71, 32, stride=KR)]

    def prepare_kx(c):
        loaded(3, c)

        def pack_kx(x, carry):
            KX[rows(x, c)] = packed(st_kx, c, x)
            return carry
        lax.fori_loop(0, NP, pack_kx, 0, unroll=16)
        last = KX[pl.ds(c * SYS + 31 * NR, NR)]
        edge = jnp.logical_and(lanes(NR) >= 64, px == 1)
        KX[pl.ds(c * SYS + 31 * NR, NR)] = jnp.where(edge, 0.0, last)

    def prepare_sb(c):
        loaded(4, c)
        loaded(5, c)

        def pack_sb(x, carry):
            D[rows(x, c)] = packed(st_s, c, x)
            R[rows(x, c)] = packed(st_b, c, x)
            return carry
        lax.fori_loop(0, NP, pack_sb, 0, unroll=16)

    prepare_x0(0)
    pl.semaphore_wait(barrier, 7)
    for cp in first[0][:3]:
        cp.start()
    prepare_kz(0)
    first[0][3].start()
    prepare_ky(0)
    first[0][4].start()
    prepare_kx(0)
    first[0][5].start()
    prepare_sb(0)
    prepare_x0(1)
    for cp in first[1][:3]:
        cp.start()
    prepare_kz(1)
    first[1][3].start()
    prepare_ky(1)
    first[1][4].start()

    def reduce_copies(kind, c):
        return [remote(red.at[kind, c, 0], red.at[kind, c, m], dsend.at[kind, c, m], drecv.at[kind, c, m], others[m]) for m in (7, 6, 5, 4, 3, 2, 1)]

    def reduce_start(kind, c, part):
        red[kind, c, 0] = jnp.sum(part, axis=0, keepdims=True)
        for cp in reduce_copies(kind, c):
            cp.start()

    def reduce_end(kind, c):
        for cp in reduce_copies(kind, c):
            cp.wait_recv()
        v = [red[kind, c, m] for m in range(8)]
        total = ((v[0] + v[1]) + (v[2] + v[3])) + ((v[4] + v[5]) + (v[6] + v[7]))
        total = jnp.broadcast_to(total, (8, LN))
        return jnp.broadcast_to(jnp.sum(total, axis=1, keepdims=True), (8, LN))

    def reduce_sent(kind, c):
        for cp in reduce_copies(kind, c):
            cp.wait_send()

    def fold(val):
        return jnp.sum(val.reshape(-1, 8, LN), axis=0)

    def wide(vec, n):
        return jnp.broadcast_to(vec[None], (n // 8, 8, LN)).reshape(n, LN)

    def z_face(ref, c, to_sz, to_sy):
        def plane(x, T):
            return pick(T, ref[rows(x, c)], x, zf)
        to_sz[c] = lax.fori_loop(0, NP, plane, zero32, unroll=32)
        to_sy[c] = ref[pl.ds(c * SYS + yf, 32, stride=NR)]

    def turn_r(c):
        G = rhz[c]
        mask = face_mask(NR)

        def plane(x, carry):
            RZ[rows(x, c)] = jnp.where(mask, spread(G, x, zf), roll(R[rows(x, c)], to_z))
            return carry
        lax.fori_loop(0, NP, plane, 0, unroll=32)

    def r_copies(c):
        return [
            remote(srz.at[c], rhz.at[c], rsend.at[c, 0], rrecv.at[c, 0], nbr['z']),
            remote(sry.at[c], rhy.at[c], rsend.at[c, 1], rrecv.at[c, 1], nbr['y']),
            remote(x_plane(R, c), rhx.at[c], rsend.at[c, 2], rrecv.at[c, 2], nbr['x'])]

    def start(c):
        for cp in first[c]:
            cp.wait_recv()
        lo = splits(NR)
        kx_last = KX[pl.ds(c * SYS + 31 * NR, NR)]
        KXM[c] = roll(jnp.where(lo, kx_last, jnp.where(px == 1, jx[c], 0.0)), 64)
        KY[pl.ds(c * KSYS + 7, 32, stride=KR)] = jnp.where(py == 1, jy[c], 0.0)
        KF[c] = jnp.where(pz == 1, jz[c], skz[c])
        PB[pl.ds(c * PSYS + hrow, 32, stride=PR)] = iy[c]
        u_first = PB[pl.ds(c * PSYS + 8, NR)]
        u_last = PB[pl.ds(c * PSYS + 31 * PR + 8, NR)]
        PB[pl.ds(c * PSYS + 32 * PR + 8, NR)] = roll(jnp.where(lo, ix[c], u_first), 64)
        low = roll(jnp.where(lo, u_last, ix[c]), 64)
        kf, uf = KF[c], iz[c]
        mask = face_mask(NR)

        def start_plane(x, carry):
            acc, fx_prev, kx_prev, u = carry
            base = pl.multiple_of(c * PSYS + x * PR, 8)
            at = rows(x, c)
            kbase = pl.multiple_of(c * KSYS + x * KR, 8)
            nxt = PB[pl.ds(base + PR + 8, NR)]
            yu = PB[pl.ds(base + 9, NR)]
            yl = PB[pl.ds(base + 7, NR)]
            s = D[at]
            kxv = KX[at]
            kyv = KY[pl.ds(kbase + 8, NR)]
            kyl = KY[pl.ds(kbase + 7, NR)]
            kzf = jnp.where(mask, spread(kf, x, zf), KZ[at])
            uz = jnp.where(mask, spread(uf, x, zf), roll(u, to_z))
            fx = kxv * (u - nxt)
            fz = kzf * (u - uz)
            fz_away = roll(jnp.where(mask, 0.0, fz), fro_z)
            D[at] = s + (kxv + kx_prev) + (kyv + kyl) + (kzf + KZF[at])
            KZF[at] = kzf
            PZ[at] = uz
            r = R[at] - (s * u + (fx - fx_prev) + (kyv * (u - yu) - kyl * (yl - u)) + (fz - fz_away))
            R[at] = r
            return acc + fold(r * r), fx, kxv, nxt
        init = (jnp.zeros((8, LN), F32), KXM[c] * (low - u_first), KXM[c], u_first)
        acc = lax.fori_loop(0, NP, start_plane, init, unroll=4)[0]
        reduce_start(0, c, acc)
        z_face(R, c, srz, sry)
        for cp in r_copies(c):
            cp.start()

    prepare_kx(1)
    first[1][5].start()
    start(0)
    prepare_sb(1)
    start(1)
    hist_s[...] = jnp.zeros((8, LN), F32)
    for c in range(2):
        phx[c] = jnp.zeros((NR, LN), F32)
        phy[c] = zero32
        for cp in first[c]:
            cp.wait_send()
    for cp in r_copies(0):
        cp.wait_recv()
    turn_r(0)

    def q_copies(c, par):
        return [
            remote(sz.at[c], qhz.at[par, c], qsend.at[c, 0], qrecv.at[par, c, 0], nbr['z']),
            remote(sy.at[c], qhy.at[par, c], qsend.at[c, 1], qrecv.at[par, c, 1], nbr['y']),
            remote(x_plane(Q, c), qhx.at[par, c], qsend.at[c, 2], qrecv.at[par, c, 2], nbr['x'])]

    def note(c, k, rho):
        hist_s[...] = jnp.where(jnp.logical_and(lane == k, row8 == c), rho, hist_s[...])

    def product(c, beta):
        b64 = wide(beta, NR)
        hx = rhx[c] + b64 * phx[c]
        hy = rhy[c] + wide(beta, 32) * phy[c]
        phx[c] = hx
        phy[c] = hy
        PB[pl.ds(c * PSYS + hrow, 32, stride=PR)] = hy
        lo = splits(NR)

        def direction(x):
            at = pl.ds(c * PSYS + x * PR + 8, NR)
            val = R[pl.ds(c * SYS + x * NR, NR)] + b64 * PB[at]
            PB[at] = val
            return val

        def turn(x, p):
            return roll(KZ[pl.ds(c * SYS + x * NR, NR)] * p, fro_z)

        def load_p(x):
            return PB[pl.ds(c * PSYS + x * PR + 8, NR)]

        p_last = direction(NP - 1)
        p_first = direction(0)
        above = roll(jnp.where(lo, hx, p_first), 64)
        below = roll(jnp.where(lo, p_last, hx), 64)
        turned = {0: turn(0, p_first)}
        for x in range(1, AHEAD):
            turned[x] = turn(x, direction(x))
        cur, kxp_prev = p_first, KXM[c] * below
        acc = jnp.zeros((8, LN), F32)
        for x in range(NP):
            w = x + AHEAD
            if w < NP:
                turned[w] = turn(w, direction(w) if w < NP - 1 else load_p(w))
            nxt = load_p(x + 1) if x + 1 < NP else above
            base = c * PSYS + x * PR
            at = pl.ds(c * SYS + x * NR, NR)
            kbase = c * KSYS + x * KR
            kxv = KX[at]
            kxp = kxv * cur
            q = D[at] * cur - kxp_prev - kxv * nxt
            q = q - KY[pl.ds(kbase + 8, NR)] * PB[pl.ds(base + 9, NR)]
            q = q - KY[pl.ds(kbase + 7, NR)] * PB[pl.ds(base + 7, NR)]
            pz_new = RZ[at] + b64 * PZ[at]
            PZ[at] = pz_new
            q = q - KZF[at] * pz_new - turned.pop(x)
            Q[at] = q
            acc = acc + fold(cur * q)
            cur, kxp_prev = nxt, kxp
        return acc

    def halo_r(c, par):
        for cp in q_copies(c, par):
            cp.wait_recv()
        alpha = alpha_s[c]
        rhx[c] = rhx[c] - wide(alpha, NR) * qhx[par, c]
        rhy[c] = rhy[c] - wide(alpha, 32) * qhy[par, c]
        rhz[c] = rhz[c] - wide(alpha, 32) * qhz[par, c]

    def q_sent(c, par):
        for cp in q_copies(c, par):
            cp.wait_send()

    def first_half(c, k, par):
        rho = reduce_end(0, c)
        note(c, k, rho)
        beta = jnp.where(k == 0, 0.0, rho / rho_s[c])
        rho_s[c] = rho
        reduce_start(1, c, product(c, beta))
        reduce_sent(0, c)
        z_face(Q, c, sz, sy)
        for cp in q_copies(c, par):
            cp.start()

    def second_half(c, k):
        alpha = rho_s[c] / reduce_end(1, c)
        alpha_s[c] = alpha
        a_pl = wide(alpha, NR)
        acc = jnp.zeros((8, LN), F32)
        for x in range(NP):
            at = pl.ds(c * SYS + x * NR, NR)
            r = R[at] - a_pl * Q[at]
            R[at] = r
            acc = acc + fold(r * r)
        reduce_start(0, c, acc)

        def step_x(x, carry):
            X[rows(x, c)] = X[rows(x, c)] + a_pl * PB[pl.ds(pl.multiple_of(c * PSYS + x * PR + 8, 8), NR)]
            return carry
        lax.fori_loop(0, NP, step_x, 0, unroll=4)
        reduce_sent(1, c)

    def body(k, carry):
        par = k % 2
        first_half(0, k, par)

        @pl.when(k == 0)
        def _():
            for cp in r_copies(1):
                cp.wait_recv()

        @pl.when(k > 0)
        def _():
            halo_r(1, 1 - par)
            q_sent(1, 1 - par)
        turn_r(1)
        first_half(1, k, par)

        @pl.when(k == 0)
        def _():
            for c in range(2):
                for cp in r_copies(c):
                    cp.wait_send()
        second_half(0, k)
        halo_r(0, par)
        turn_r(0)
        second_half(1, k)
        q_sent(0, par)
        return carry

    lax.fori_loop(0, ITERS, body, 0)
    for c in range(2):
        note(c, ITERS, reduce_end(0, c))
        reduce_sent(0, c)
    for cp in q_copies(1, (ITERS - 1) % 2):
        cp.wait()
    hist_out[...] = jnp.sqrt(hist_s[...] * (1.0 / (128 * 128 * 128)))


CHUNKS = 4
VMEM_MAIN = 54 * 1024 * 1024


def unpack(buf, hist, x_out, hist_out, st, ho, out_sem, h_sem):
    planes = NP // CHUNKS
    ho[...] = hist[:2, :ITERS + 1]
    stores = [pltpu.make_async_copy(ho, hist_out, h_sem)]
    stores[0].start()
    for n in range(2 * CHUNKS):
        c, x0 = n // CHUNKS, n % CHUNKS * planes

        def plane(x, carry):
            val = buf[pl.ds(pl.multiple_of(n * planes * NR + x * NR, 8), NR)]
            st[c, x0 + x] = val[:, :64]
            st[c, x0 + x + NP] = roll(val, 64)[:, :64]
            return carry
        lax.fori_loop(0, planes, plane, 0, unroll=8)
        for h in range(2):
            at = pl.ds(x0 + NP * h, planes)
            stores.append(pltpu.make_async_copy(st.at[c, at], x_out.at[c, at], out_sem.at[n, h]))
            stores[-1].start()
    for cp in stores:
        cp.wait()


def run(s, b, x0, kx, ky, kz):
    v = lambda *shape: pltpu.VMEM(shape, F32)
    sem = lambda *shape: pltpu.SemaphoreType.DMA(shape)
    scratch = [v(2, 64, 64, 64)] * 6
    full = v(2 * SYS, LN)
    scratch += [full, full, v(2 * PSYS, LN), full, full, full, v(2, NR, LN), v(2 * KSYS, LN), full, full, full, v(2, 32, LN)]
    scratch += [v(2, NR, LN), v(2, 32, LN), v(2, 32, LN)] * 2
    scratch += [v(2, 32, LN)] * 8
    scratch += [v(2, NR, LN), v(2, 32, LN), v(2, 32, LN), v(2, NR, LN), v(2, 32, LN)]
    scratch += [v(2, 2, NR, LN), v(2, 2, 32, LN), v(2, 2, 32, LN)]
    scratch += [v(2, 2, 8, 1, LN), v(2, 8, LN), v(2, 8, LN), v(8, LN)]
    scratch += [sem(6, 2), sem(2, 6), sem(2, 6), sem(2, 3), sem(2, 3), sem(2, 3), sem(2, 2, 3), sem(2, 2, 8), sem(2, 2, 8)]
    xp, hist = pl.pallas_call(
        kernel,
        out_shape=(pltpu.VMEM((2 * SYS, LN), F32), pltpu.VMEM((8, LN), F32)),
        in_specs=[pl.BlockSpec(memory_space=pl.ANY)] * 6,
        out_specs=(pl.BlockSpec(memory_space=pltpu.VMEM), pl.BlockSpec(memory_space=pltpu.VMEM)),
        scratch_shapes=scratch,
        compiler_params=pltpu.CompilerParams(collective_id=0, has_side_effects=True, vmem_limit_bytes=VMEM_MAIN),
        name='cg',
    )(s, b, x0, kx, ky, kz)
    return pl.pallas_call(
        unpack,
        out_shape=(jax.ShapeDtypeStruct((2, 64, 64, 64), F32), jax.ShapeDtypeStruct((2, ITERS + 1), F32)),
        in_specs=[pl.BlockSpec(memory_space=pltpu.VMEM)] * 2,
        out_specs=[pl.BlockSpec(memory_space=pl.ANY)] * 2,
        scratch_shapes=[v(2, 64, 64, 64), v(2, ITERS + 1), sem(2 * CHUNKS, 2), pltpu.SemaphoreType.DMA],
        compiler_params=pltpu.CompilerParams(vmem_limit_bytes=12 * 1024 * 1024),
        name='unpack',
    )(xp, hist)


def solution(mesh):
    field = P(None, 'px', 'py', 'pz')
    return jax.shard_map(run, mesh=mesh, in_specs=(field,) * 6, out_specs=(field, P(None, None)), check_vma=False)
```

```python
import jax
import jax.numpy as jnp
from jax import lax
from jax.experimental import pallas as pl
from jax.experimental.pallas import tpu as pltpu
from jax.sharding import PartitionSpec as P

ITERS = 20
F32 = jnp.float32
MESH = pl.DeviceIdType.MESH

NP = 32
NR = 64
LN = 128
PR = 80
KR = 72
SYS = NP * NR
PSYS = (NP + 1) * PR
KSYS = NP * KR
IN_FLIGHT = 7
AHEAD = 3


def roll(val, shift):
    if isinstance(shift, int):
        shift = shift % LN
    return pltpu.roll(val, shift, 1)


def kernel(s_hbm, b_hbm, x0_hbm, kx_hbm, ky_hbm, kz_hbm, X, hist_out,
           st_s, st_b, st_x, st_kx, st_ky, st_kz,
           R, Q, PB, PZ, RZ, KX, KXM, KY, KZ, KZF, D, KF,
           ix, iy, iz, jx, jy, jz, sxy, sxz, sky, skz, sy, sz, sry, srz,
           rhx, rhy, rhz, phx, phy, qhx, qhy, qhz,
           red, rho_s, alpha_s, hist_s,
           ld_sem, isend, irecv, rsend, rrecv, qsend, qrecv, dsend, drecv):
    pz, py, px = lax.axis_index('pz'), lax.axis_index('py'), lax.axis_index('px')
    nbr = {'x': (pz, py, 1 - px), 'y': (pz, 1 - py, px), 'z': (1 - pz, py, px)}
    others = {}
    for m in range(1, 8):
        others[m] = (1 - pz if m & 4 else pz, 1 - py if m & 2 else py, 1 - px if m & 1 else px)

    lane = lax.broadcasted_iota(jnp.int32, (8, LN), 1)
    row8 = lax.broadcasted_iota(jnp.int32, (8, LN), 0)

    def lanes(n):
        return lax.broadcasted_iota(jnp.int32, (n, LN), 1)

    zf = 63 * (1 - pz)
    xf = 31 * (1 - px)
    yf = 63 * (1 - py)
    hrow = 72 - 65 * py
    to_z = 127 - 126 * pz
    fro_z = 1 + 126 * pz

    def face_mask(n):
        return (lanes(n) % 64) == zf

    def splits(n):
        return lanes(n) < 64

    order = [(num, c) for c in range(2) for num in range(6)]
    pairs = ((x0_hbm, st_x), (kz_hbm, st_kz), (ky_hbm, st_ky), (kx_hbm, st_kx), (s_hbm, st_s), (b_hbm, st_b))
    loads = [pltpu.make_async_copy(pairs[num][0].at[c], pairs[num][1].at[c], ld_sem.at[num, c]) for num, c in order]
    for cp in loads[:IN_FLIGHT]:
        cp.start()

    def loaded(num, c):
        n = c * 6 + num
        loads[n].wait()
        if n + IN_FLIGHT < len(loads):
            loads[n + IN_FLIGHT].start()

    barrier = pltpu.get_barrier_semaphore()
    for m in range(1, 8):
        pl.semaphore_signal(barrier, inc=1, device_id=others[m], device_id_type=MESH)

    def packed(st, c, x):
        return jnp.concatenate([st[c, x], st[c, x + NP]], axis=1)

    def pick(T, val, x, f):
        l64 = lanes(32) % 64
        T = jnp.where(l64 == x, roll(val[:32], lax.rem(x - f + LN, LN)), T)
        return jnp.where(l64 == x + 32, roll(val[32:], lax.rem(x + 32 - f + LN, LN)), T)

    def spread(G, x, f):
        return jnp.concatenate([roll(G, lax.rem(f - x + LN, LN)), roll(G, lax.rem(f - x - 32 + LN, LN))], axis=0)

    zero32 = jnp.zeros((32, LN), F32)

    def remote(src, dst, send_sem, recv_sem, dev):
        return pltpu.make_async_remote_copy(src_ref=src, dst_ref=dst, send_sem=send_sem, recv_sem=recv_sem, device_id=dev, device_id_type=MESH)

    def x_plane(ref, c):
        return ref.at[pl.ds(pl.multiple_of(c * SYS + xf * NR, 8), NR)]

    def rows(x, c):
        return pl.ds(pl.multiple_of(c * SYS + x * NR, 8), NR)

    first = []
    for c in range(2):
        first.append([
            remote(sxz.at[c], iz.at[c], isend.at[c, 0], irecv.at[c, 0], nbr['z']),
            remote(sxy.at[c], iy.at[c], isend.at[c, 1], irecv.at[c, 1], nbr['y']),
            remote(x_plane(X, c), ix.at[c], isend.at[c, 2], irecv.at[c, 2], nbr['x']),
            remote(skz.at[c], jz.at[c], isend.at[c, 3], irecv.at[c, 3], nbr['z']),
            remote(sky.at[c], jy.at[c], isend.at[c, 4], irecv.at[c, 4], nbr['y']),
            remote(KX.at[pl.ds(c * SYS + 31 * NR, NR)], jx.at[c], isend.at[c, 5], irecv.at[c, 5], nbr['x'])])

    def prepare_x0(c):
        loaded(0, c)

        def pack_x(x, T):
            u = packed(st_x, c, x)
            X[rows(x, c)] = u
            base = pl.multiple_of(c * PSYS + x * PR, 8)
            PB[pl.ds(base, 8)] = jnp.zeros((8, LN), F32)
            PB[pl.ds(base + 72, 8)] = jnp.zeros((8, LN), F32)
            PB[pl.ds(base + 8, NR)] = u
            return pick(T, u, x, zf)
        sxz[c] = lax.fori_loop(0, NP, pack_x, zero32, unroll=8)
        sxy[c] = X[pl.ds(c * SYS + yf, 32, stride=NR)]

    def prepare_kz(c):
        loaded(1, c)

        def pack_z(x, T):
            u = packed(st_kz, c, x)
            inner = jnp.where(lanes(NR) % 64 == 63, 0.0, u)
            moved = roll(inner, 1)
            KZ[rows(x, c)] = jnp.where(pz == 1, moved, inner)
            KZF[rows(x, c)] = jnp.where(pz == 1, inner, moved)
            return pick(T, u, x, 63)
        skz[c] = lax.fori_loop(0, NP, pack_z, zero32, unroll=8)

    def prepare_ky(c):
        loaded(2, c)

        def pack_ky(x, carry):
            u = packed(st_ky, c, x)
            row = lax.broadcasted_iota(jnp.int32, (NR, LN), 0)
            u = jnp.where(jnp.logical_and(row == NR - 1, py == 1), 0.0, u)
            KY[pl.ds(pl.multiple_of(c * KSYS + x * KR + 8, 8), NR)] = u
            return carry
        lax.fori_loop(0, NP, pack_ky, 0, unroll=8)
        sky[c] = KY[pl.ds(c * KSYS + 71, 32, stride=KR)]

    def prepare_kx(c):
        loaded(3, c)

        def pack_kx(x, carry):
            KX[rows(x, c)] = packed(st_kx, c, x)
            return carry
        lax.fori_loop(0, NP, pack_kx, 0, unroll=8)
        last = KX[pl.ds(c * SYS + 31 * NR, NR)]
        edge = jnp.logical_and(lanes(NR) >= 64, px == 1)
        KX[pl.ds(c * SYS + 31 * NR, NR)] = jnp.where(edge, 0.0, last)

    def prepare_sb(c):
        loaded(4, c)
        loaded(5, c)

        def pack_sb(x, carry):
            D[rows(x, c)] = packed(st_s, c, x)
            R[rows(x, c)] = packed(st_b, c, x)
            return carry
        lax.fori_loop(0, NP, pack_sb, 0, unroll=8)

    prepare_x0(0)
    pl.semaphore_wait(barrier, 7)
    for cp in first[0][:3]:
        cp.start()
    prepare_kz(0)
    first[0][3].start()
    prepare_ky(0)
    first[0][4].start()
    prepare_kx(0)
    first[0][5].start()
    prepare_sb(0)
    prepare_x0(1)
    for cp in first[1][:3]:
        cp.start()
    prepare_kz(1)
    first[1][3].start()
    prepare_ky(1)
    first[1][4].start()

    def reduce_copies(kind, c):
        return [remote(red.at[kind, c, 0], red.at[kind, c, m], dsend.at[kind, c, m], drecv.at[kind, c, m], others[m]) for m in (7, 6, 5, 4, 3, 2, 1)]

    def reduce_start(kind, c, part):
        red[kind, c, 0] = jnp.sum(part, axis=0, keepdims=True)
        for cp in reduce_copies(kind, c):
            cp.start()

    def reduce_end(kind, c):
        for cp in reduce_copies(kind, c):
            cp.wait_recv()
        v = [red[kind, c, m] for m in range(8)]
        total = ((v[0] + v[1]) + (v[2] + v[3])) + ((v[4] + v[5]) + (v[6] + v[7]))
        total = jnp.broadcast_to(total, (8, LN))
        return jnp.broadcast_to(jnp.sum(total, axis=1, keepdims=True), (8, LN))

    def reduce_sent(kind, c):
        for cp in reduce_copies(kind, c):
            cp.wait_send()

    def fold(val):
        return jnp.sum(val.reshape(-1, 8, LN), axis=0)

    def wide(vec, n):
        return jnp.broadcast_to(vec[None], (n // 8, 8, LN)).reshape(n, LN)

    def z_face(ref, c, to_sz, to_sy):
        def plane(x, T):
            return pick(T, ref[rows(x, c)], x, zf)
        to_sz[c] = lax.fori_loop(0, NP, plane, zero32, unroll=32)
        to_sy[c] = ref[pl.ds(c * SYS + yf, 32, stride=NR)]

    def turn_r(c):
        G = rhz[c]
        mask = face_mask(NR)

        def plane(x, carry):
            RZ[rows(x, c)] = jnp.where(mask, spread(G, x, zf), roll(R[rows(x, c)], to_z))
            return carry
        lax.fori_loop(0, NP, plane, 0, unroll=32)

    def r_copies(c):
        return [
            remote(srz.at[c], rhz.at[c], rsend.at[c, 0], rrecv.at[c, 0], nbr['z']),
            remote(sry.at[c], rhy.at[c], rsend.at[c, 1], rrecv.at[c, 1], nbr['y']),
            remote(x_plane(R, c), rhx.at[c], rsend.at[c, 2], rrecv.at[c, 2], nbr['x'])]

    def start(c):
        for cp in first[c]:
            cp.wait_recv()
        lo = splits(NR)
        kx_last = KX[pl.ds(c * SYS + 31 * NR, NR)]
        KXM[c] = roll(jnp.where(lo, kx_last, jnp.where(px == 1, jx[c], 0.0)), 64)
        KY[pl.ds(c * KSYS + 7, 32, stride=KR)] = jnp.where(py == 1, jy[c], 0.0)
        KF[c] = jnp.where(pz == 1, jz[c], skz[c])
        PB[pl.ds(c * PSYS + hrow, 32, stride=PR)] = iy[c]
        u_first = PB[pl.ds(c * PSYS + 8, NR)]
        u_last = PB[pl.ds(c * PSYS + 31 * PR + 8, NR)]
        PB[pl.ds(c * PSYS + 32 * PR + 8, NR)] = roll(jnp.where(lo, ix[c], u_first), 64)
        low = roll(jnp.where(lo, u_last, ix[c]), 64)
        kf, uf = KF[c], iz[c]
        mask = face_mask(NR)

        def start_plane(x, carry):
            acc, fx_prev, kx_prev, u = carry
            base = pl.multiple_of(c * PSYS + x * PR, 8)
            at = rows(x, c)
            kbase = pl.multiple_of(c * KSYS + x * KR, 8)
            nxt = PB[pl.ds(base + PR + 8, NR)]
            yu = PB[pl.ds(base + 9, NR)]
            yl = PB[pl.ds(base + 7, NR)]
            s = D[at]
            kxv = KX[at]
            kyv = KY[pl.ds(kbase + 8, NR)]
            kyl = KY[pl.ds(kbase + 7, NR)]
            kzf = jnp.where(mask, spread(kf, x, zf), KZ[at])
            uz = jnp.where(mask, spread(uf, x, zf), roll(u, to_z))
            fx = kxv * (u - nxt)
            fz = kzf * (u - uz)
            fz_away = roll(jnp.where(mask, 0.0, fz), fro_z)
            D[at] = s + (kxv + kx_prev) + (kyv + kyl) + (kzf + KZF[at])
            KZF[at] = kzf
            PZ[at] = uz
            r = R[at] - (s * u + (fx - fx_prev) + (kyv * (u - yu) - kyl * (yl - u)) + (fz - fz_away))
            R[at] = r
            return acc + fold(r * r), fx, kxv, nxt
        init = (jnp.zeros((8, LN), F32), KXM[c] * (low - u_first), KXM[c], u_first)
        acc = lax.fori_loop(0, NP, start_plane, init, unroll=4)[0]
        reduce_start(0, c, acc)
        z_face(R, c, srz, sry)
        for cp in r_copies(c):
            cp.start()

    prepare_kx(1)
    first[1][5].start()
    start(0)
    prepare_sb(1)
    start(1)
    hist_s[...] = jnp.zeros((8, LN), F32)
    for c in range(2):
        phx[c] = jnp.zeros((NR, LN), F32)
        phy[c] = zero32
        for cp in first[c]:
            cp.wait_send()
    for cp in r_copies(0):
        cp.wait_recv()
    turn_r(0)

    def q_copies(c, par):
        return [
            remote(sz.at[c], qhz.at[par, c], qsend.at[c, 0], qrecv.at[par, c, 0], nbr['z']),
            remote(sy.at[c], qhy.at[par, c], qsend.at[c, 1], qrecv.at[par, c, 1], nbr['y']),
            remote(x_plane(Q, c), qhx.at[par, c], qsend.at[c, 2], qrecv.at[par, c, 2], nbr['x'])]

    def note(c, k, rho):
        hist_s[...] = jnp.where(jnp.logical_and(lane == k, row8 == c), rho, hist_s[...])

    def product(c, beta):
        b64 = wide(beta, NR)
        hx = rhx[c] + b64 * phx[c]
        hy = rhy[c] + wide(beta, 32) * phy[c]
        phx[c] = hx
        phy[c] = hy
        PB[pl.ds(c * PSYS + hrow, 32, stride=PR)] = hy
        lo = splits(NR)

        def direction(x):
            at = pl.ds(c * PSYS + x * PR + 8, NR)
            val = R[pl.ds(c * SYS + x * NR, NR)] + b64 * PB[at]
            PB[at] = val
            return val

        def turn(x, p):
            return roll(KZ[pl.ds(c * SYS + x * NR, NR)] * p, fro_z)

        def load_p(x):
            return PB[pl.ds(c * PSYS + x * PR + 8, NR)]

        p_last = direction(NP - 1)
        p_first = direction(0)
        above = roll(jnp.where(lo, hx, p_first), 64)
        below = roll(jnp.where(lo, p_last, hx), 64)
        turned = {0: turn(0, p_first)}
        for x in range(1, AHEAD):
            turned[x] = turn(x, direction(x))
        cur, kxp_prev = p_first, KXM[c] * below
        acc = jnp.zeros((8, LN), F32)
        for x in range(NP):
            w = x + AHEAD
            if w < NP:
                turned[w] = turn(w, direction(w) if w < NP - 1 else load_p(w))
            nxt = load_p(x + 1) if x + 1 < NP else above
            base = c * PSYS + x * PR
            at = pl.ds(c * SYS + x * NR, NR)
            kbase = c * KSYS + x * KR
            kxv = KX[at]
            kxp = kxv * cur
            q = D[at] * cur - kxp_prev - kxv * nxt
            q = q - KY[pl.ds(kbase + 8, NR)] * PB[pl.ds(base + 9, NR)]
            q = q - KY[pl.ds(kbase + 7, NR)] * PB[pl.ds(base + 7, NR)]
            pz_new = RZ[at] + b64 * PZ[at]
            PZ[at] = pz_new
            q = q - KZF[at] * pz_new - turned.pop(x)
            Q[at] = q
            acc = acc + fold(cur * q)
            cur, kxp_prev = nxt, kxp
        return acc

    def halo_r(c, par):
        for cp in q_copies(c, par):
            cp.wait_recv()
        alpha = alpha_s[c]
        rhx[c] = rhx[c] - wide(alpha, NR) * qhx[par, c]
        rhy[c] = rhy[c] - wide(alpha, 32) * qhy[par, c]
        rhz[c] = rhz[c] - wide(alpha, 32) * qhz[par, c]

    def q_sent(c, par):
        for cp in q_copies(c, par):
            cp.wait_send()

    def first_half(c, k, par):
        rho = reduce_end(0, c)
        note(c, k, rho)
        beta = jnp.where(k == 0, 0.0, rho / rho_s[c])
        rho_s[c] = rho
        reduce_start(1, c, product(c, beta))
        reduce_sent(0, c)
        z_face(Q, c, sz, sy)
        for cp in q_copies(c, par):
            cp.start()

    def second_half(c, k):
        alpha = rho_s[c] / reduce_end(1, c)
        alpha_s[c] = alpha
        a_pl = wide(alpha, NR)
        acc = jnp.zeros((8, LN), F32)
        for x in range(NP):
            at = pl.ds(c * SYS + x * NR, NR)
            r = R[at] - a_pl * Q[at]
            R[at] = r
            acc = acc + fold(r * r)
        reduce_start(0, c, acc)

        def step_x(x, carry):
            X[rows(x, c)] = X[rows(x, c)] + a_pl * PB[pl.ds(pl.multiple_of(c * PSYS + x * PR + 8, 8), NR)]
            return carry
        lax.fori_loop(0, NP, step_x, 0, unroll=8)
        reduce_sent(1, c)

    def body(k, carry):
        par = k % 2
        first_half(0, k, par)

        @pl.when(k == 0)
        def _():
            for cp in r_copies(1):
                cp.wait_recv()

        @pl.when(k > 0)
        def _():
            halo_r(1, 1 - par)
            q_sent(1, 1 - par)
        turn_r(1)
        first_half(1, k, par)

        @pl.when(k == 0)
        def _():
            for c in range(2):
                for cp in r_copies(c):
                    cp.wait_send()
        second_half(0, k)
        halo_r(0, par)
        turn_r(0)
        second_half(1, k)
        q_sent(0, par)
        return carry

    lax.fori_loop(0, ITERS, body, 0)
    for c in range(2):
        note(c, ITERS, reduce_end(0, c))
        reduce_sent(0, c)
    for cp in q_copies(1, (ITERS - 1) % 2):
        cp.wait()
    hist_out[...] = jnp.sqrt(hist_s[...] * (1.0 / (128 * 128 * 128)))


CHUNKS = 4
VMEM_MAIN = 54 * 1024 * 1024


def unpack(buf, hist, x_out, hist_out, st, ho, out_sem, h_sem):
    planes = NP // CHUNKS
    ho[...] = hist[:2, :ITERS + 1]
    stores = [pltpu.make_async_copy(ho, hist_out, h_sem)]
    stores[0].start()
    for n in range(2 * CHUNKS):
        c, x0 = n // CHUNKS, n % CHUNKS * planes

        def plane(x, carry):
            val = buf[pl.ds(pl.multiple_of(n * planes * NR + x * NR, 8), NR)]
            st[c, x0 + x] = val[:, :64]
            st[c, x0 + x + NP] = roll(val, 64)[:, :64]
            return carry
        lax.fori_loop(0, planes, plane, 0, unroll=8)
        for h in range(2):
            at = pl.ds(x0 + NP * h, planes)
            stores.append(pltpu.make_async_copy(st.at[c, at], x_out.at[c, at], out_sem.at[n, h]))
            stores[-1].start()
    for cp in stores:
        cp.wait()


def run(s, b, x0, kx, ky, kz):
    v = lambda *shape: pltpu.VMEM(shape, F32)
    sem = lambda *shape: pltpu.SemaphoreType.DMA(shape)
    scratch = [v(2, 64, 64, 64)] * 6
    full = v(2 * SYS, LN)
    scratch += [full, full, v(2 * PSYS, LN), full, full, full, v(2, NR, LN), v(2 * KSYS, LN), full, full, full, v(2, 32, LN)]
    scratch += [v(2, NR, LN), v(2, 32, LN), v(2, 32, LN)] * 2
    scratch += [v(2, 32, LN)] * 8
    scratch += [v(2, NR, LN), v(2, 32, LN), v(2, 32, LN), v(2, NR, LN), v(2, 32, LN)]
    scratch += [v(2, 2, NR, LN), v(2, 2, 32, LN), v(2, 2, 32, LN)]
    scratch += [v(2, 2, 8, 1, LN), v(2, 8, LN), v(2, 8, LN), v(8, LN)]
    scratch += [sem(6, 2), sem(2, 6), sem(2, 6), sem(2, 3), sem(2, 3), sem(2, 3), sem(2, 2, 3), sem(2, 2, 8), sem(2, 2, 8)]
    xp, hist = pl.pallas_call(
        kernel,
        out_shape=(pltpu.VMEM((2 * SYS, LN), F32), pltpu.VMEM((8, LN), F32)),
        in_specs=[pl.BlockSpec(memory_space=pl.ANY)] * 6,
        out_specs=(pl.BlockSpec(memory_space=pltpu.VMEM), pl.BlockSpec(memory_space=pltpu.VMEM)),
        scratch_shapes=scratch,
        compiler_params=pltpu.CompilerParams(collective_id=0, has_side_effects=True, vmem_limit_bytes=VMEM_MAIN),
        name='cg',
    )(s, b, x0, kx, ky, kz)
    return pl.pallas_call(
        unpack,
        out_shape=(jax.ShapeDtypeStruct((2, 64, 64, 64), F32), jax.ShapeDtypeStruct((2, ITERS + 1), F32)),
        in_specs=[pl.BlockSpec(memory_space=pltpu.VMEM)] * 2,
        out_specs=[pl.BlockSpec(memory_space=pl.ANY)] * 2,
        scratch_shapes=[v(2, 64, 64, 64), v(2, ITERS + 1), sem(2 * CHUNKS, 2), pltpu.SemaphoreType.DMA],
        compiler_params=pltpu.CompilerParams(vmem_limit_bytes=12 * 1024 * 1024),
        name='unpack',
    )(xp, hist)


def solution(mesh):
    field = P(None, 'px', 'py', 'pz')
    return jax.shard_map(run, mesh=mesh, in_specs=(field,) * 6, out_specs=(field, P(None, None)), check_vma=False)
```

```python
import jax
import jax.numpy as jnp
from jax import lax
from jax.experimental import pallas as pl
from jax.experimental.pallas import tpu as pltpu
from jax.sharding import PartitionSpec as P

ITERS = 20
F32 = jnp.float32
MESH = pl.DeviceIdType.MESH

NP = 32
NR = 64
LN = 128
PR = 80
KR = 72
SYS = NP * NR
PSYS = (NP + 1) * PR
KSYS = NP * KR
IN_FLIGHT = 7
AHEAD = 3


def roll(val, shift):
    if isinstance(shift, int):
        shift = shift % LN
    return pltpu.roll(val, shift, 1)


def kernel(s_hbm, b_hbm, x0_hbm, kx_hbm, ky_hbm, kz_hbm, X, hist_out,
           st_s, st_b, st_x, st_kx, st_ky, st_kz,
           R, Q, PB, PZ, RZ, KX, KXM, KY, KZ, KZF, D, KF,
           ix, iy, iz, jx, jy, jz, sxy, sxz, sky, skz, sy, sz, sry, srz,
           rhx, rhy, rhz, phx, phy, qhx, qhy, qhz,
           red, rho_s, alpha_s, hist_s,
           ld_sem, isend, irecv, rsend, rrecv, qsend, qrecv, dsend, drecv):
    pz, py, px = lax.axis_index('pz'), lax.axis_index('py'), lax.axis_index('px')
    nbr = {'x': (pz, py, 1 - px), 'y': (pz, 1 - py, px), 'z': (1 - pz, py, px)}
    others = {}
    for m in range(1, 8):
        others[m] = (1 - pz if m & 4 else pz, 1 - py if m & 2 else py, 1 - px if m & 1 else px)

    lane = lax.broadcasted_iota(jnp.int32, (8, LN), 1)
    row8 = lax.broadcasted_iota(jnp.int32, (8, LN), 0)

    def lanes(n):
        return lax.broadcasted_iota(jnp.int32, (n, LN), 1)

    zf = 63 * (1 - pz)
    xf = 31 * (1 - px)
    yf = 63 * (1 - py)
    hrow = 72 - 65 * py
    to_z = 127 - 126 * pz
    fro_z = 1 + 126 * pz

    def face_mask(n):
        return (lanes(n) % 64) == zf

    def splits(n):
        return lanes(n) < 64

    order = [(num, c) for c in range(2) for num in range(6)]
    pairs = ((x0_hbm, st_x), (kz_hbm, st_kz), (ky_hbm, st_ky), (kx_hbm, st_kx), (s_hbm, st_s), (b_hbm, st_b))
    loads = [pltpu.make_async_copy(pairs[num][0].at[c], pairs[num][1].at[c], ld_sem.at[num, c]) for num, c in order]
    for cp in loads[:IN_FLIGHT]:
        cp.start()

    def loaded(num, c):
        n = c * 6 + num
        loads[n].wait()
        if n + IN_FLIGHT < len(loads):
            loads[n + IN_FLIGHT].start()

    barrier = pltpu.get_barrier_semaphore()
    for m in range(1, 8):
        pl.semaphore_signal(barrier, inc=1, device_id=others[m], device_id_type=MESH)

    def packed(st, c, x):
        return jnp.concatenate([st[c, x], st[c, x + NP]], axis=1)

    def pick(T, val, x, f):
        l64 = lanes(32) % 64
        T = jnp.where(l64 == x, roll(val[:32], lax.rem(x - f + LN, LN)), T)
        return jnp.where(l64 == x + 32, roll(val[32:], lax.rem(x + 32 - f + LN, LN)), T)

    def spread(G, x, f):
        return jnp.concatenate([roll(G, lax.rem(f - x + LN, LN)), roll(G, lax.rem(f - x - 32 + LN, LN))], axis=0)

    zero32 = jnp.zeros((32, LN), F32)

    def remote(src, dst, send_sem, recv_sem, dev):
        return pltpu.make_async_remote_copy(src_ref=src, dst_ref=dst, send_sem=send_sem, recv_sem=recv_sem, device_id=dev, device_id_type=MESH)

    def x_plane(ref, c):
        return ref.at[pl.ds(pl.multiple_of(c * SYS + xf * NR, 8), NR)]

    def rows(x, c):
        return pl.ds(pl.multiple_of(c * SYS + x * NR, 8), NR)

    first = []
    for c in range(2):
        first.append([
            remote(sxz.at[c], iz.at[c], isend.at[c, 0], irecv.at[c, 0], nbr['z']),
            remote(sxy.at[c], iy.at[c], isend.at[c, 1], irecv.at[c, 1], nbr['y']),
            remote(x_plane(X, c), ix.at[c], isend.at[c, 2], irecv.at[c, 2], nbr['x']),
            remote(skz.at[c], jz.at[c], isend.at[c, 3], irecv.at[c, 3], nbr['z']),
            remote(sky.at[c], jy.at[c], isend.at[c, 4], irecv.at[c, 4], nbr['y']),
            remote(KX.at[pl.ds(c * SYS + 31 * NR, NR)], jx.at[c], isend.at[c, 5], irecv.at[c, 5], nbr['x'])])

    def prepare_x0(c):
        loaded(0, c)

        def pack_x(x, T):
            u = packed(st_x, c, x)
            X[rows(x, c)] = u
            base = pl.multiple_of(c * PSYS + x * PR, 8)
            PB[pl.ds(base, 8)] = jnp.zeros((8, LN), F32)
            PB[pl.ds(base + 72, 8)] = jnp.zeros((8, LN), F32)
            PB[pl.ds(base + 8, NR)] = u
            return pick(T, u, x, zf)
        sxz[c] = lax.fori_loop(0, NP, pack_x, zero32, unroll=8)
        sxy[c] = X[pl.ds(c * SYS + yf, 32, stride=NR)]

    def prepare_kz(c):
        loaded(1, c)

        def pack_z(x, T):
            u = packed(st_kz, c, x)
            inner = jnp.where(lanes(NR) % 64 == 63, 0.0, u)
            moved = roll(inner, 1)
            KZ[rows(x, c)] = jnp.where(pz == 1, moved, inner)
            KZF[rows(x, c)] = jnp.where(pz == 1, inner, moved)
            return pick(T, u, x, 63)
        skz[c] = lax.fori_loop(0, NP, pack_z, zero32, unroll=8)

    def prepare_ky(c):
        loaded(2, c)

        def pack_ky(x, carry):
            u = packed(st_ky, c, x)
            row = lax.broadcasted_iota(jnp.int32, (NR, LN), 0)
            u = jnp.where(jnp.logical_and(row == NR - 1, py == 1), 0.0, u)
            KY[pl.ds(pl.multiple_of(c * KSYS + x * KR + 8, 8), NR)] = u
            return carry
        lax.fori_loop(0, NP, pack_ky, 0, unroll=8)
        sky[c] = KY[pl.ds(c * KSYS + 71, 32, stride=KR)]

    def prepare_kx(c):
        loaded(3, c)

        def pack_kx(x, carry):
            KX[rows(x, c)] = packed(st_kx, c, x)
            return carry
        lax.fori_loop(0, NP, pack_kx, 0, unroll=8)
        last = KX[pl.ds(c * SYS + 31 * NR, NR)]
        edge = jnp.logical_and(lanes(NR) >= 64, px == 1)
        KX[pl.ds(c * SYS + 31 * NR, NR)] = jnp.where(edge, 0.0, last)

    def prepare_sb(c):
        loaded(4, c)
        loaded(5, c)

        def pack_sb(x, carry):
            D[rows(x, c)] = packed(st_s, c, x)
            R[rows(x, c)] = packed(st_b, c, x)
            return carry
        lax.fori_loop(0, NP, pack_sb, 0, unroll=8)

    prepare_x0(0)
    pl.semaphore_wait(barrier, 7)
    for cp in first[0][:3]:
        cp.start()
    prepare_kz(0)
    first[0][3].start()
    prepare_ky(0)
    first[0][4].start()
    prepare_kx(0)
    first[0][5].start()
    prepare_sb(0)
    prepare_x0(1)
    for cp in first[1][:3]:
        cp.start()
    prepare_kz(1)
    first[1][3].start()
    prepare_ky(1)
    first[1][4].start()

    def reduce_copies(kind, c):
        return [remote(red.at[kind, c, 0], red.at[kind, c, m], dsend.at[kind, c, m], drecv.at[kind, c, m], others[m]) for m in (7, 6, 5, 4, 3, 2, 1)]

    def reduce_start(kind, c, part):
        red[kind, c, 0] = jnp.sum(part, axis=0, keepdims=True)
        for cp in reduce_copies(kind, c):
            cp.start()

    def reduce_end(kind, c):
        for cp in reduce_copies(kind, c):
            cp.wait_recv()
        v = [red[kind, c, m] for m in range(8)]
        total = ((v[0] + v[1]) + (v[2] + v[3])) + ((v[4] + v[5]) + (v[6] + v[7]))
        total = jnp.broadcast_to(total, (8, LN))
        return jnp.broadcast_to(jnp.sum(total, axis=1, keepdims=True), (8, LN))

    def reduce_sent(kind, c):
        for cp in reduce_copies(kind, c):
            cp.wait_send()

    def fold(val):
        return jnp.sum(val.reshape(-1, 8, LN), axis=0)

    def wide(vec, n):
        return jnp.broadcast_to(vec[None], (n // 8, 8, LN)).reshape(n, LN)

    def z_face(ref, c, to_sz, to_sy):
        def plane(x, T):
            return pick(T, ref[rows(x, c)], x, zf)
        to_sz[c] = lax.fori_loop(0, NP, plane, zero32, unroll=32)
        to_sy[c] = ref[pl.ds(c * SYS + yf, 32, stride=NR)]

    def turn_r(c):
        G = rhz[c]
        mask = face_mask(NR)

        def plane(x, carry):
            RZ[rows(x, c)] = jnp.where(mask, spread(G, x, zf), roll(R[rows(x, c)], to_z))
            return carry
        lax.fori_loop(0, NP, plane, 0, unroll=32)

    def r_copies(c):
        return [
            remote(srz.at[c], rhz.at[c], rsend.at[c, 0], rrecv.at[c, 0], nbr['z']),
            remote(sry.at[c], rhy.at[c], rsend.at[c, 1], rrecv.at[c, 1], nbr['y']),
            remote(x_plane(R, c), rhx.at[c], rsend.at[c, 2], rrecv.at[c, 2], nbr['x'])]

    def start(c):
        for cp in first[c]:
            cp.wait_recv()
        lo = splits(NR)
        kx_last = KX[pl.ds(c * SYS + 31 * NR, NR)]
        KXM[c] = roll(jnp.where(lo, kx_last, jnp.where(px == 1, jx[c], 0.0)), 64)
        KY[pl.ds(c * KSYS + 7, 32, stride=KR)] = jnp.where(py == 1, jy[c], 0.0)
        KF[c] = jnp.where(pz == 1, jz[c], skz[c])
        PB[pl.ds(c * PSYS + hrow, 32, stride=PR)] = iy[c]
        u_first = PB[pl.ds(c * PSYS + 8, NR)]
        u_last = PB[pl.ds(c * PSYS + 31 * PR + 8, NR)]
        PB[pl.ds(c * PSYS + 32 * PR + 8, NR)] = roll(jnp.where(lo, ix[c], u_first), 64)
        low = roll(jnp.where(lo, u_last, ix[c]), 64)
        kf, uf = KF[c], iz[c]
        mask = face_mask(NR)

        def start_plane(x, carry):
            acc, fx_prev, kx_prev, u, T = carry
            base = pl.multiple_of(c * PSYS + x * PR, 8)
            at = rows(x, c)
            kbase = pl.multiple_of(c * KSYS + x * KR, 8)
            nxt = PB[pl.ds(base + PR + 8, NR)]
            yu = PB[pl.ds(base + 9, NR)]
            yl = PB[pl.ds(base + 7, NR)]
            s = D[at]
            kxv = KX[at]
            kyv = KY[pl.ds(kbase + 8, NR)]
            kyl = KY[pl.ds(kbase + 7, NR)]
            kzf = jnp.where(mask, spread(kf, x, zf), KZ[at])
            uz = jnp.where(mask, spread(uf, x, zf), roll(u, to_z))
            fx = kxv * (u - nxt)
            fz = kzf * (u - uz)
            fz_away = roll(jnp.where(mask, 0.0, fz), fro_z)
            D[at] = s + (kxv + kx_prev) + (kyv + kyl) + (kzf + KZF[at])
            KZF[at] = kzf
            PZ[at] = uz
            r = R[at] - (s * u + (fx - fx_prev) + (kyv * (u - yu) - kyl * (yl - u)) + (fz - fz_away))
            R[at] = r
            return acc + fold(r * r), fx, kxv, nxt, pick(T, r, x, zf)
        init = (jnp.zeros((8, LN), F32), KXM[c] * (low - u_first), KXM[c], u_first, zero32)
        acc, _, _, _, T = lax.fori_loop(0, NP, start_plane, init, unroll=4)
        reduce_start(0, c, acc)
        srz[c] = T
        sry[c] = R[pl.ds(c * SYS + yf, 32, stride=NR)]
        for cp in r_copies(c):
            cp.start()

    prepare_kx(1)
    first[1][5].start()
    start(0)
    prepare_sb(1)
    start(1)
    hist_s[...] = jnp.zeros((8, LN), F32)
    for c in range(2):
        phx[c] = jnp.zeros((NR, LN), F32)
        phy[c] = zero32
        for cp in first[c]:
            cp.wait_send()
    for cp in r_copies(0):
        cp.wait_recv()
    turn_r(0)

    def q_copies(c, par):
        return [
            remote(sz.at[c], qhz.at[par, c], qsend.at[c, 0], qrecv.at[par, c, 0], nbr['z']),
            remote(sy.at[c], qhy.at[par, c], qsend.at[c, 1], qrecv.at[par, c, 1], nbr['y']),
            remote(x_plane(Q, c), qhx.at[par, c], qsend.at[c, 2], qrecv.at[par, c, 2], nbr['x'])]

    def note(c, k, rho):
        hist_s[...] = jnp.where(jnp.logical_and(lane == k, row8 == c), rho, hist_s[...])

    def product(c, beta):
        b64 = wide(beta, NR)
        hx = rhx[c] + b64 * phx[c]
        hy = rhy[c] + wide(beta, 32) * phy[c]
        phx[c] = hx
        phy[c] = hy
        PB[pl.ds(c * PSYS + hrow, 32, stride=PR)] = hy
        lo = splits(NR)

        def direction(x):
            at = pl.ds(c * PSYS + x * PR + 8, NR)
            val = R[pl.ds(c * SYS + x * NR, NR)] + b64 * PB[at]
            PB[at] = val
            return val

        def turn(x, p):
            return roll(KZ[pl.ds(c * SYS + x * NR, NR)] * p, fro_z)

        def load_p(x):
            return PB[pl.ds(c * PSYS + x * PR + 8, NR)]

        p_last = direction(NP - 1)
        p_first = direction(0)
        above = roll(jnp.where(lo, hx, p_first), 64)
        below = roll(jnp.where(lo, p_last, hx), 64)
        turned = {0: turn(0, p_first)}
        for x in range(1, AHEAD):
            turned[x] = turn(x, direction(x))
        cur, kxp_prev = p_first, KXM[c] * below
        acc = jnp.zeros((8, LN), F32)
        for x in range(NP):
            w = x + AHEAD
            if w < NP:
                turned[w] = turn(w, direction(w) if w < NP - 1 else load_p(w))
            nxt = load_p(x + 1) if x + 1 < NP else above
            base = c * PSYS + x * PR
            at = pl.ds(c * SYS + x * NR, NR)
            kbase = c * KSYS + x * KR
            kxv = KX[at]
            kxp = kxv * cur
            q = D[at] * cur - kxp_prev - kxv * nxt
            q = q - KY[pl.ds(kbase + 8, NR)] * PB[pl.ds(base + 9, NR)]
            q = q - KY[pl.ds(kbase + 7, NR)] * PB[pl.ds(base + 7, NR)]
            pz_new = RZ[at] + b64 * PZ[at]
            PZ[at] = pz_new
            q = q - KZF[at] * pz_new - turned.pop(x)
            Q[at] = q
            acc = acc + fold(cur * q)
            cur, kxp_prev = nxt, kxp
        return acc

    def halo_r(c, par):
        for cp in q_copies(c, par):
            cp.wait_recv()
        alpha = alpha_s[c]
        rhx[c] = rhx[c] - wide(alpha, NR) * qhx[par, c]
        rhy[c] = rhy[c] - wide(alpha, 32) * qhy[par, c]
        rhz[c] = rhz[c] - wide(alpha, 32) * qhz[par, c]

    def q_sent(c, par):
        for cp in q_copies(c, par):
            cp.wait_send()

    def first_half(c, k, par):
        rho = reduce_end(0, c)
        note(c, k, rho)
        beta = jnp.where(k == 0, 0.0, rho / rho_s[c])
        rho_s[c] = rho
        reduce_start(1, c, product(c, beta))
        reduce_sent(0, c)
        z_face(Q, c, sz, sy)
        for cp in q_copies(c, par):
            cp.start()

    def second_half(c, k):
        alpha = rho_s[c] / reduce_end(1, c)
        alpha_s[c] = alpha
        a_pl = wide(alpha, NR)
        acc = jnp.zeros((8, LN), F32)
        for x in range(NP):
            at = pl.ds(c * SYS + x * NR, NR)
            r = R[at] - a_pl * Q[at]
            R[at] = r
            acc = acc + fold(r * r)
        reduce_start(0, c, acc)

        def step_x(x, carry):
            X[rows(x, c)] = X[rows(x, c)] + a_pl * PB[pl.ds(pl.multiple_of(c * PSYS + x * PR + 8, 8), NR)]
            return carry
        lax.fori_loop(0, NP, step_x, 0, unroll=8)
        reduce_sent(1, c)

    def body(k, carry):
        par = k % 2
        first_half(0, k, par)

        @pl.when(k == 0)
        def _():
            for cp in r_copies(1):
                cp.wait_recv()

        @pl.when(k > 0)
        def _():
            halo_r(1, 1 - par)
            q_sent(1, 1 - par)
        turn_r(1)
        first_half(1, k, par)

        @pl.when(k == 0)
        def _():
            for c in range(2):
                for cp in r_copies(c):
                    cp.wait_send()
        second_half(0, k)
        halo_r(0, par)
        turn_r(0)
        second_half(1, k)
        q_sent(0, par)
        return carry

    lax.fori_loop(0, ITERS, body, 0)
    for c in range(2):
        note(c, ITERS, reduce_end(0, c))
        reduce_sent(0, c)
    for cp in q_copies(1, (ITERS - 1) % 2):
        cp.wait()
    hist_out[...] = jnp.sqrt(hist_s[...] * (1.0 / (128 * 128 * 128)))


CHUNKS = 4
VMEM_MAIN = 54 * 1024 * 1024


def unpack(buf, hist, x_out, hist_out, st, ho, out_sem, h_sem):
    planes = NP // CHUNKS
    ho[...] = hist[:2, :ITERS + 1]
    stores = [pltpu.make_async_copy(ho, hist_out, h_sem)]
    stores[0].start()
    for n in range(2 * CHUNKS):
        c, x0 = n // CHUNKS, n % CHUNKS * planes

        def plane(x, carry):
            val = buf[pl.ds(pl.multiple_of(n * planes * NR + x * NR, 8), NR)]
            st[c, x0 + x] = val[:, :64]
            st[c, x0 + x + NP] = roll(val, 64)[:, :64]
            return carry
        lax.fori_loop(0, planes, plane, 0, unroll=8)
        for h in range(2):
            at = pl.ds(x0 + NP * h, planes)
            stores.append(pltpu.make_async_copy(st.at[c, at], x_out.at[c, at], out_sem.at[n, h]))
            stores[-1].start()
    for cp in stores:
        cp.wait()


def run(s, b, x0, kx, ky, kz):
    v = lambda *shape: pltpu.VMEM(shape, F32)
    sem = lambda *shape: pltpu.SemaphoreType.DMA(shape)
    scratch = [v(2, 64, 64, 64)] * 6
    full = v(2 * SYS, LN)
    scratch += [full, full, v(2 * PSYS, LN), full, full, full, v(2, NR, LN), v(2 * KSYS, LN), full, full, full, v(2, 32, LN)]
    scratch += [v(2, NR, LN), v(2, 32, LN), v(2, 32, LN)] * 2
    scratch += [v(2, 32, LN)] * 8
    scratch += [v(2, NR, LN), v(2, 32, LN), v(2, 32, LN), v(2, NR, LN), v(2, 32, LN)]
    scratch += [v(2, 2, NR, LN), v(2, 2, 32, LN), v(2, 2, 32, LN)]
    scratch += [v(2, 2, 8, 1, LN), v(2, 8, LN), v(2, 8, LN), v(8, LN)]
    scratch += [sem(6, 2), sem(2, 6), sem(2, 6), sem(2, 3), sem(2, 3), sem(2, 3), sem(2, 2, 3), sem(2, 2, 8), sem(2, 2, 8)]
    xp, hist = pl.pallas_call(
        kernel,
        out_shape=(pltpu.VMEM((2 * SYS, LN), F32), pltpu.VMEM((8, LN), F32)),
        in_specs=[pl.BlockSpec(memory_space=pl.ANY)] * 6,
        out_specs=(pl.BlockSpec(memory_space=pltpu.VMEM), pl.BlockSpec(memory_space=pltpu.VMEM)),
        scratch_shapes=scratch,
        compiler_params=pltpu.CompilerParams(collective_id=0, has_side_effects=True, vmem_limit_bytes=VMEM_MAIN),
        name='cg',
    )(s, b, x0, kx, ky, kz)
    return pl.pallas_call(
        unpack,
        out_shape=(jax.ShapeDtypeStruct((2, 64, 64, 64), F32), jax.ShapeDtypeStruct((2, ITERS + 1), F32)),
        in_specs=[pl.BlockSpec(memory_space=pltpu.VMEM)] * 2,
        out_specs=[pl.BlockSpec(memory_space=pl.ANY)] * 2,
        scratch_shapes=[v(2, 64, 64, 64), v(2, ITERS + 1), sem(2 * CHUNKS, 2), pltpu.SemaphoreType.DMA],
        compiler_params=pltpu.CompilerParams(vmem_limit_bytes=12 * 1024 * 1024),
        name='unpack',
    )(xp, hist)


def solution(mesh):
    field = P(None, 'px', 'py', 'pz')
    return jax.shard_map(run, mesh=mesh, in_specs=(field,) * 6, out_specs=(field, P(None, None)), check_vma=False)
```
